32 devices in a mesh: rep: 8 (over y, x, core), shard: 4 (over z).
Axes of the slice: x: 2, y: 2, z: 4, core: 2. Of those that a mesh axis runs over, the one named last changes fastest.
Arguments:
- activations: bfloat16 [6, 4096, 2048], P(None, ('rep', 'shard')), may hold values from -50 to 50
- cotangents: bfloat16 [6, 4096, 512], P(None, ('rep', 'shard')), may hold values from -120 to 120
- momentum: float32 [12, 256, 2048], P(None, None, 'shard'), may hold values from -6 to 6
- owners: int32 [12], replicated, may hold values from 0 to 3, as said below
- bucket_starts: int32 [2], replicated, may hold values from 1 to 11, as said below
Outputs:
- momentum_out: float32 [12, 256, 2048], P(None, None, 'shard')
- update: float32 [12, 256, 2048], P(None, None, 'shard')
- owned: bfloat16 [16, 256, 2048], P('shard')
The draws below stay inside these ranges and needn't reach their ends.
Inputs may be any that keep to these rules, and one draw needn't show every extreme that they name: `owners`: no owner is named more than 4 times, and some owner exactly 4 times. `bucket_starts`: strictly increasing.
All inputs are finite; a program needn't handle non-finite values.
Results may differ from the reference program's by a relative error of at most 0.033.
Values may be sent and summed in bfloat16 or wider, within the bound.
A program may use at most 128 MiB of HBM per device.

```python
import math
import jax
import jax.numpy as jnp
from jax import lax

D = 2048
KV = 256
LAYERS = 6
ITERS = 5
BUCKETS = 3
MATS = 12
SLOTS = 4
TOKENS = 4096
N_SHARD = 4


def bucket_layout(key):
    key_starts = jax.random.fold_in(key, 31)
    chosen = jax.random.permutation(key_starts, MATS - 2)[:BUCKETS - 2] + 1
    last_start = jnp.full((1,), MATS - 1, dtype=jnp.int32)
    return jnp.sort(jnp.concatenate([chosen.astype(jnp.int32), last_start])).astype(jnp.int32)


def draw_activations(key, part):
    key_values = jax.random.fold_in(key, 41)
    shape_full = (LAYERS, TOKENS, D)
    values = jnp.clip(jax.random.normal(key_values, shape_full, jnp.float32), -4.5, 4.5)
    ratio = 6.0
    position = jnp.arange(D, dtype=jnp.float32) / D
    rising = jnp.exp(math.log(ratio) * position)
    mean_energy = (ratio * ratio - 1.0) / (2.0 * math.log(ratio))
    column_scale = rising / math.sqrt(mean_energy)
    return (values * column_scale[None, None, :]).astype(jnp.bfloat16)


def draw_cotangents(key, part):
    key_normal = jax.random.fold_in(key, 11)
    key_quiet_scale = jax.random.fold_in(key, 12)
    key_column = jax.random.fold_in(key, 13)
    key_quiet = jax.random.fold_in(key, 14)
    key_loud_scale = jax.random.fold_in(key, 15)
    shape_full = (LAYERS, TOKENS, 2 * KV)
    normal_part = jnp.clip(jax.random.normal(key_normal, shape_full, jnp.float32), -5.0, 5.0)
    starts = bucket_layout(key)
    indices = jnp.arange(MATS, dtype=jnp.int32)
    buckets = jnp.sum((indices[:, None] >= starts[None, :]).astype(jnp.int32), axis=1)
    quiet_bucket = jax.random.randint(key_quiet, (), 0, BUCKETS, dtype=jnp.int32)
    quiet_log = jax.random.uniform(key_quiet_scale, (MATS,), jnp.float32, math.log(0.03), math.log(0.1))
    loud_log = jax.random.uniform(key_loud_scale, (MATS,), jnp.float32, 0.0, math.log(8.0))
    matrix_scale = jnp.exp(jnp.where(buckets == quiet_bucket, quiet_log, loud_log))
    matrix_scale = jnp.repeat(matrix_scale.reshape(LAYERS, 1, 2), KV, axis=2)
    column_scale = jnp.exp(jax.random.uniform(key_column, (LAYERS, 1, 2 * KV), jnp.float32, 0.0, math.log(3.0)))
    return (normal_part * matrix_scale * column_scale).astype(jnp.bfloat16)


def draw_owners(key, part):
    key_first = jax.random.fold_in(key, 21)
    key_second = jax.random.fold_in(key, 22)
    key_third = jax.random.fold_in(key, 23)
    shuffled = jax.random.permutation(key_first, N_SHARD).astype(jnp.int32)
    filled = jnp.full((SLOTS,), shuffled[0], dtype=jnp.int32)
    others = jax.random.permutation(key_second, jnp.repeat(shuffled[1:], SLOTS))
    candidates = jnp.concatenate([filled, others])[:MATS]
    return jax.random.permutation(key_third, candidates).astype(jnp.int32)


def draw_bucket_starts(key, part):
    return bucket_layout(key)


def block_scale(rng, shape, pieces, smallest, largest):
    level = 1.0
    for axis_at, shards_of in pieces:
        steps = jax.random.uniform(jax.random.fold_in(jax.random.fold_in(rng, 6), axis_at), (shards_of,), jnp.float32, smallest / len(pieces), largest / len(pieces))
        level = level * jnp.repeat(jnp.exp(steps), shape[axis_at] // shards_of).reshape((-1,) + (1,) * (len(shape) - 1 - axis_at))
    return level


def bell_draw(stream_key, extent, deviation, limit, shards=(), kind=jnp.bfloat16):
    drawn = jax.random.normal(stream_key, extent, jnp.float32) * deviation
    if len(shards) > 0:
        drawn = block_scale(stream_key, extent, shards, -0.22, 0.18) * drawn
    return jnp.clip(drawn, min=-limit, max=limit).astype(kind)


def setup_inputs(seed: int = 0) -> dict:
    key_list = jax.random.split(jax.random.key(seed), 6)
    activations = draw_activations(jax.random.fold_in(key_list[5], 71), 0)
    cotangents = draw_cotangents(jax.random.fold_in(key_list[5], 71), 0)
    momentum = bell_draw(key_list[2], (MATS, KV, D), 1.0, 6.0, ((2, 4),), jnp.float32)
    owners = draw_owners(jax.random.fold_in(key_list[5], 71), 0)
    bucket_starts = draw_bucket_starts(jax.random.fold_in(key_list[5], 71), 0)
    return {"activations": activations, "cotangents": cotangents, "momentum": momentum, "owners": owners, "bucket_starts": bucket_starts}


coef_a = 3.4445
coef_b = -4.775
coef_c = 2.0315
momentum_rate = 0.95
clip_level = 0.5
epsilon = 1e-06

def orthogonal(update_in):
    values = update_in.astype(jnp.float32)
    frobenius = jnp.sqrt(jnp.sum(values * values))
    matrix = (values / (frobenius + epsilon)).astype(jnp.bfloat16)
    for iteration in range(ITERS):
        gram_matrix = jnp.dot(matrix, matrix.T, preferred_element_type=jnp.float32).astype(jnp.bfloat16)
        square = jnp.dot(gram_matrix, gram_matrix, preferred_element_type=jnp.float32)
        mixing = (coef_b * gram_matrix.astype(jnp.float32) + coef_c * square).astype(jnp.bfloat16)
        matrix = (coef_a * matrix.astype(jnp.float32) + jnp.dot(mixing, matrix, preferred_element_type=jnp.float32)).astype(jnp.bfloat16)
    return matrix

def clip_factors(square_sums, bucket_starts):
    indices = jnp.arange(MATS, dtype=jnp.int32)
    buckets = lax.optimization_barrier(jnp.sum((indices[:, None] >= bucket_starts[None, :]).astype(jnp.int32), axis=1))
    together = (buckets[:, None] == buckets[None, :]).astype(jnp.float32)
    totals = lax.optimization_barrier(jnp.sum(together * square_sums[None, :], axis=1))
    members = lax.optimization_barrier(jnp.sum(together, axis=1))
    root_mean = jnp.sqrt(totals / (members * KV * D) + epsilon)
    return jnp.minimum(1.0, clip_level / root_mean)

def slot_numbers(owners):
    indices = jnp.arange(MATS, dtype=jnp.int32)
    earlier = (indices[None, :] < indices[:, None]) & (owners[None, :] == owners[:, None])
    return lax.optimization_barrier(jnp.sum(earlier.astype(jnp.int32), axis=1)).astype(jnp.int32)

def reference(activations, cotangents, momentum, owners, bucket_starts):
    layer_grads = []
    for layer_index in range(LAYERS):
        layer_grads.append(lax.dot_general(cotangents[layer_index], activations[layer_index], (((0,), (0,)), ((), ())), preferred_element_type=jnp.float32))
    gradient = jnp.stack(layer_grads).reshape(MATS, KV, D) / jnp.sqrt(jnp.float32(TOKENS))
    square_sums = lax.optimization_barrier(jnp.sum(gradient * gradient, axis=(1, 2)))
    factors = clip_factors(square_sums, bucket_starts)
    momentum_out = momentum_rate * momentum + factors[:, None, None] * gradient
    nesterov = (factors[:, None, None] * gradient + momentum_rate * momentum_out).astype(jnp.bfloat16)
    orthogonalized = lax.map(orthogonal, nesterov)
    update_scale = math.sqrt(max(KV, D))
    update = update_scale * orthogonalized.astype(jnp.float32)
    slot_of = slot_numbers(owners)
    positions = owners * SLOTS + slot_of
    select = (jnp.arange(N_SHARD * SLOTS, dtype=jnp.int32)[:, None] == positions[None, :]).astype(jnp.float32)
    holdings = jnp.einsum('pm,mkd->pkd', select, update).astype(jnp.bfloat16)
    return (momentum_out, update, holdings)
```

```python
import functools
import math

import jax
import jax.numpy as jnp
from jax import lax
from jax.experimental import pallas as pl
from jax.experimental.pallas import tpu as pltpu
from jax.sharding import PartitionSpec as P

D = 2048
KV = 256
ITERS = 5
MATS = 12
MESH = pl.DeviceIdType.MESH
VMEM_SPEC = pl.BlockSpec(memory_space=pltpu.VMEM)
SMEM_SPEC = pl.BlockSpec(memory_space=pltpu.SMEM)
ANY_SPEC = pl.BlockSpec(memory_space=pl.ANY)
VMEM_LIMIT = 60 * 1024 * 1024

coef_a = 3.4445
coef_b = -4.775
coef_c = 2.0315
momentum_rate = 0.95
clip_level = 0.5
epsilon = 1e-06


def orthogonal_batch(matrices):
    values = matrices.astype(jnp.float32)
    frobenius = jnp.sqrt(jnp.sum(values * values, axis=(1, 2), keepdims=True))
    matrix = (values / (frobenius + epsilon)).astype(jnp.bfloat16)
    for iteration in range(ITERS):
        gram_matrix = jnp.einsum(
            "skd,sjd->skj", matrix, matrix, preferred_element_type=jnp.float32
        ).astype(jnp.bfloat16)
        square = jnp.einsum(
            "skj,sji->ski", gram_matrix, gram_matrix, preferred_element_type=jnp.float32
        )
        mixing = (coef_b * gram_matrix.astype(jnp.float32) + coef_c * square).astype(jnp.bfloat16)
        product = jnp.einsum("skj,sjd->skd", mixing, matrix, preferred_element_type=jnp.float32)
        matrix = (coef_a * matrix.astype(jnp.float32) + product).astype(jnp.bfloat16)
    return matrix


def clip_factors(square_sums, bucket_starts):
    indices = jnp.arange(MATS, dtype=jnp.int32)
    buckets = jnp.sum((indices[:, None] >= bucket_starts[None, :]).astype(jnp.int32), axis=1)
    together = (buckets[:, None] == buckets[None, :]).astype(jnp.float32)
    totals = jnp.sum(together * square_sums[None, :], axis=1)
    members = jnp.sum(together, axis=1)
    root_mean = jnp.sqrt(totals / (members * KV * D) + epsilon)
    return jnp.minimum(1.0, clip_level / root_mean)


def slot_numbers(owners):
    indices = jnp.arange(MATS, dtype=jnp.int32)
    earlier = (indices[None, :] < indices[:, None]) & (owners[None, :] == owners[:, None])
    return jnp.sum(earlier.astype(jnp.int32), axis=1)


def selector(owner_of, slot_of, shard_count, slot_count):
    holders = lax.broadcasted_iota(jnp.int32, (shard_count, slot_count, 1), 0)
    places = lax.broadcasted_iota(jnp.int32, (shard_count, slot_count, 1), 1)
    chosen = (holders == owner_of[None, None, :]) & (places == slot_of[None, None, :])
    return chosen.astype(jnp.bfloat16)


def pack_slots(shards, chooser):
    return jnp.einsum("psm,mkd->skpd", chooser, shards, preferred_element_type=jnp.float32).astype(
        jnp.bfloat16
    )


def unpack_slots(received, chooser):
    return jnp.einsum("psm,skpd->mkd", chooser, received, preferred_element_type=jnp.float32)


def per_device_general(activations, cotangents, momentum, owners, bucket_starts):
    shard_count = lax.axis_size("shard")
    replica_count = lax.axis_size("rep")
    layers, tok_rows, width = activations.shape
    token_total = tok_rows * shard_count * replica_count
    columns = width // shard_count
    slot_count = -(-MATS // shard_count) + 1
    update_scale = math.sqrt(max(KV, D))
    partial_terms = jnp.einsum(
        "ltk,ltd->lkd", cotangents, activations, preferred_element_type=jnp.float32
    ).reshape(MATS, KV, width)
    shard_part = lax.psum_scatter(
        partial_terms.astype(jnp.bfloat16), "shard", scatter_dimension=2, tiled=True
    )
    summed = lax.psum(shard_part, "rep").astype(jnp.float32)
    gradient = summed / jnp.sqrt(jnp.float32(token_total))
    square_sums = lax.psum(jnp.sum(gradient * gradient, axis=(1, 2)), "shard")
    factors = clip_factors(square_sums, bucket_starts)
    momentum_out = momentum_rate * momentum + factors[:, None, None] * gradient
    nesterov = (factors[:, None, None] * gradient + momentum_rate * momentum_out).astype(
        jnp.bfloat16
    )
    slot_of = slot_numbers(owners)
    chooser = selector(owners, slot_of, shard_count, slot_count)
    received = lax.all_to_all(
        pack_slots(nesterov, chooser), "shard", split_axis=2, concat_axis=2, tiled=True
    )
    item_count = received.shape[0]
    result = orthogonal_batch(received.reshape(item_count, KV, width))
    scaled = (update_scale * result.astype(jnp.float32)).astype(jnp.bfloat16)
    returned_part = lax.all_to_all(
        result.reshape(item_count, KV, shard_count, columns),
        "shard",
        split_axis=2,
        concat_axis=2,
        tiled=True,
    )
    update = update_scale * unpack_slots(returned_part, chooser)
    return (momentum_out, update, scaled)


def lodged(block, member):
    x = lax.rem(block, 2)
    y = lax.div(block, 2)
    whole = 2 * x + y
    paired = 4 + y
    return jnp.where(member < 2, whole, paired), jnp.where(member < 2, member, x)


def lodging(matrix):
    layer = lax.div(matrix, 2)
    side = lax.rem(matrix, 2)
    early = matrix < 8
    x = jnp.where(early, lax.div(layer, 2), side)
    y = jnp.where(early, lax.rem(layer, 2), layer - 4)
    return 2 * y + x, jnp.where(early, side, 2)


def place():
    me = lax.axis_index("rep")
    core = lax.rem(me, 2)
    x = lax.rem(lax.div(me, 2), 2)
    y = lax.div(me, 4)
    to_core = me + 1 - 2 * core
    to_x = me + 2 - 4 * x
    to_y = me + 4 - 8 * y
    to_xy = me + 6 - 4 * x - 8 * y
    return me, core, x, y, to_core, to_x, to_y, to_xy


def greet(peers):
    barrier = pltpu.get_barrier_semaphore()
    for peer in peers:
        pl.semaphore_signal(barrier, inc=1, device_id=peer, device_id_type=MESH)
    pl.semaphore_wait(barrier, len(peers))


def remote(src, dst, send, recv, peer):
    return pltpu.make_async_remote_copy(
        src_ref=src, dst_ref=dst, send_sem=send, recv_sem=recv, device_id=peer, device_id_type=MESH
    )


def plane_gather_start(z, at, send, recv):
    me, core, x, y, to_core, to_x, to_y, to_xy = place()
    plan = ((0, to_x, 0), (2, to_y, 1), (1, to_x, 1), (3, to_y, 0), (4, to_core, None))
    copies = {}
    for k, peer, half in plan:
        copies[k] = remote(at(me, half), at(me, half), send.at[k], recv.at[k], (peer, z))
        copies[k].start()
    return copies


def plane_gather_turn(z, at, send, recv, copies):
    me, core, x, y, to_core, to_x, to_y, to_xy = place()

    def forward(k, block, half, peer):
        copies[k] = remote(
            at(block, half), at(block, half), send.at[k], recv.at[k], (peer, z)
        )
        copies[k].start()

    copies[0].wait_recv()
    forward(5, to_x, 0, to_y)
    copies[2].wait_recv()
    forward(6, to_y, 1, to_x)
    copies[1].wait_recv()
    forward(7, to_x, None, to_core)
    copies[3].wait_recv()
    forward(8, to_y, None, to_core)


def plane_gather_finish(z, at, send, recv, copies, last=(4, 7, 8, 9)):
    me, core, x, y, to_core, to_x, to_y, to_xy = place()
    copies[5].wait_recv()
    copies[6].wait_recv()
    copies[9] = remote(
        at(to_xy, None), at(to_xy, None), send.at[9], recv.at[9], (to_core, z)
    )
    copies[9].start()
    for k in last:
        copies[k].wait_recv()
    for k in range(10):
        copies[k].wait_send()


def reduce_kernel(
    n_shard, inverse, act_ref, cot_ref, gown_ref, sq_ref,
    act, cot, part, recv1, turn, recv2, plane, zrecv,
    local_sem, in_send, in_recv, s1, r1, s2, r2, s3, r3,
):
    me, core, x, y, to_core, to_x, to_y, to_xy = place()
    z = lax.axis_index("shard")
    tokens = act_ref.shape[1]
    rows, cols = part.shape[-2:]
    members = part.shape[2 + 1]
    steps = [d for d in (2, 1, 3) if d < n_shard] + list(range(4, n_shard)) + [0]
    peers = [(p, z) for p in (to_core, to_x, to_y)]
    peers += [(me, lax.rem(z + d, n_shard)) for d in range(1, n_shard)]
    cut = [
        pl.ds(pl.multiple_of(lax.rem(z + d, n_shard) * cols, cols), cols) for d in steps
    ]
    own = [
        pltpu.make_async_copy(
            act_ref.at[:, :, cut[k]], act[k].at[:, pl.ds(0, tokens)], local_sem.at[k]
        )
        for k in range(n_shard)
    ]
    own.append(
        pltpu.make_async_copy(cot_ref, cot.at[:, pl.ds(0, tokens)], local_sem.at[n_shard])
    )
    for c in own:
        c.start()
    greet(peers)
    theirs = pl.ds(tokens, tokens)
    swap = [
        remote(
            act_ref.at[:, :, cut[k]], act[k].at[:, theirs],
            in_send.at[k], in_recv.at[k], (to_core, z),
        )
        for k in range(n_shard)
    ]
    swap.append(
        remote(cot_ref, cot.at[:, theirs], in_send.at[n_shard], in_recv.at[n_shard], (to_core, z))
    )
    for c in swap[-1:] + swap[:-1]:
        c.start()
    for c in own:
        c.wait()
    swap[n_shard].wait()
    first = []
    second = []
    third = []

    def launch(k):
        swap[k].wait()

        def one(q, carry):
            group = lax.div(q, members)
            member = lax.rem(q, members)
            layer, side = lodged(group, member)
            block = cot[layer]
            low = jnp.where(core == 0, block[:, :rows], block[:, rows : 2 * rows])
            high = jnp.where(core == 0, block[:, 2 * rows : 3 * rows], block[:, 3 * rows :])
            left = jnp.where(side == 0, low, high)
            right = act[k][layer]
            value = lax.dot_general(
                left, right, (((0,), (0,)), ((), ())), preferred_element_type=jnp.float32
            )
            part[k, lax.div(group, 2), lax.rem(group, 2), member] = value.astype(part.dtype)
            return carry

        lax.fori_loop(0, 4 * members, one, 0)

    def send_first(k):
        if k % 2 == 0:
            c = remote(part.at[k, :, 1 - x], recv1.at[k], s1.at[k], r1.at[k], (to_x, z))
        else:
            c = remote(part.at[k, 1 - y], recv1.at[k], s1.at[k], r1.at[k], (to_y, z))
        c.start()
        first.append(c)

    def send_second(k):
        first[k].wait_recv()

        def add_out(j, carry):
            if k % 2 == 0:
                mine = part[k, 1 - y, x, j]
                came = recv1[k, 1 - y, j]
            else:
                mine = part[k, y, 1 - x, j]
                came = recv1[k, 1 - x, j]
            turn[k, j] = (mine.astype(jnp.float32) + came.astype(jnp.float32)).astype(turn.dtype)
            return carry

        lax.fori_loop(0, members, add_out, 0)
        c = remote(
            turn.at[k], recv2.at[k], s2.at[k], r2.at[k], (to_y if k % 2 == 0 else to_x, z)
        )
        c.start()
        second.append(c)

    def send_third(k):
        second[k].wait_recv()

        def add_in(j, carry):
            came = recv1[k, y, j] if k % 2 == 0 else recv1[k, x, j]
            value = part[k, y, x, j].astype(jnp.float32) + came.astype(jnp.float32)
            value = value + recv2[k, j].astype(jnp.float32)
            plane[k, j] = value.astype(plane.dtype)
            return carry

        lax.fori_loop(0, members, add_in, 0)
        if steps[k]:
            c = remote(
                plane.at[k], zrecv.at[k], s3.at[k], r3.at[k],
                (me, lax.rem(z + steps[k], n_shard)),
            )
            c.start()
            third.append(c)

    launch(0)
    send_first(0)
    launch(1)
    send_first(1)
    for k in range(2, n_shard):
        launch(k)
    for k in range(0, n_shard, 2):
        pair = [i for i in (k, k + 1) if i < n_shard]
        for i in pair:
            send_second(i)
        for i in (k + 2, k + 3):
            if i < n_shard:
                send_first(i)
        for i in pair:
            send_third(i)
    for c in third:
        c.wait_recv()

    def add_last(j, carry):
        value = plane[n_shard - 1, j].astype(jnp.float32)
        for k in range(n_shard - 1):
            value = value + zrecv[k, j].astype(jnp.float32)
        value = (value * inverse).astype(gown_ref.dtype)
        gown_ref[j] = value
        value = value.astype(jnp.float32)
        line = jnp.sum(value * value, axis=0, keepdims=True)
        lanes = sq_ref.shape[-1]
        fold = line[:, :lanes]
        for i in range(1, cols // lanes):
            fold = fold + line[:, i * lanes : (i + 1) * lanes]
        sq_ref[j] = fold
        return carry

    lax.fori_loop(0, members, add_last, 0)
    for c in first + second + third:
        c.wait_send()


HOMES = ((1, 0), (2, 0), (2, 1))


def block_at(ref, axis, rows):
    def at(r, half):
        count = rows if half is None else rows // 2
        start = lax.rem(r, 2) * rows + (0 if half is None else half * count)
        cut = pl.ds(pl.multiple_of(start, count), count)
        block = lax.div(r, 2)
        return ref.at[block, cut] if axis == 1 else ref.at[block, :, cut]

    return at


def split(value):
    high = value.astype(jnp.bfloat16)
    return high, (value - high.astype(jnp.float32)).astype(jnp.bfloat16)


def times(left, right):
    dot = functools.partial(jnp.dot, preferred_element_type=jnp.float32)
    return dot(left[0], right[0]) + (dot(left[0], right[1]) + dot(left[1], right[0]))


def gram_iteration(gram, scale, gram_scr, root_scr):
    n = gram.shape[0]
    row = lax.broadcasted_iota(jnp.int32, (n, n), 0)
    col = lax.broadcasted_iota(jnp.int32, (n, n), 1)
    eye = (row == col).astype(jnp.float32)
    trace = jnp.sum(jnp.sum(gram * eye, axis=0, keepdims=True), axis=1, keepdims=True)
    inverse = 1.0 / (jnp.sqrt(trace) + epsilon)
    gram_scr[...] = gram * inverse * inverse
    for iteration in range(ITERS):
        a = split(gram_scr[...])
        mixing = coef_b * gram_scr[...] + coef_c * times(a, a)
        b = split(mixing)
        if iteration == 0:
            root_scr[...] = coef_a * eye + mixing
        else:
            root_scr[...] = coef_a * root_scr[...] + times(b, split(root_scr[...]))
        if iteration < ITERS - 1:
            half = coef_a * gram_scr[...] + times(b, a)
            gram_scr[...] = coef_a * half + times(b, split(half))
    return root_scr[...] * (inverse * scale)


def settle_kernel(
    n_shard, scale, owner_ref, start_ref, momentum_hbm, gown_ref, sq_ref,
    mout_ref, u_ref, wall_ref, qall_ref,
    momentum, gall, sqall, table, factor, uown, held, gram_out, gram_in, gram_scr, root_scr, root,
    load, ps, pr, qs, qr, gs, gr, as_, ar, ws, wr, os_, or_, rs, rr, hs, hr,
):
    f32, bf16 = jnp.float32, jnp.bfloat16
    me, core, x, y, to_core, to_x, to_y, to_xy = place()
    z = lax.axis_index("shard")
    base = me - core
    block = lax.div(me, 2)
    members, rows, cols = gown_ref.shape
    lanes = sq_ref.shape[-1]
    other = 1 - 2 * core
    near = (to_core, to_x, to_y, to_xy, to_x + other, to_y + other, to_xy + other)
    mine = pl.ds(pl.multiple_of(core * rows, rows), rows)

    fetch = pltpu.make_async_copy(momentum_hbm, momentum, load)
    fetch.start()
    column = [(base + c, lax.rem(z + d, n_shard)) for d in range(1, n_shard) for c in range(2)]
    greet([(p, z) for p in near] + column)

    sqall[0, me] = sq_ref[...]
    squares = []
    for k, peer in enumerate(near):
        c = remote(sqall.at[0, me], sqall.at[0, me], ps.at[k], pr.at[k], (peer, z))
        c.start()
        squares.append(c)
    gall[block, :, mine] = gown_ref[...]
    at_g = block_at(gall, 2, rows)
    gathers = plane_gather_start(z, at_g, gs, gr)
    for c in squares:
        c.wait_recv()
    lines = []
    for d in range(1, n_shard):
        c = remote(sqall.at[0], sqall.at[d], qs.at[d - 1], qr.at[d - 1], (me, lax.rem(z + d, n_shard)))
        c.start()
        lines.append(c)
    fetch.wait()
    for c in lines:
        c.wait_recv()

    table[...] = jnp.zeros_like(table)
    for m in range(MATS):
        layer, side = divmod(m, 2)
        bx, by = divmod(layer, 2) if m < 8 else (side, layer - 4)
        j, i = 2 * by + bx, side if m < 8 else 2
        line = sqall[0, 2 * j, i] + sqall[0, 2 * j + 1, i]
        for d in range(1, n_shard):
            line = line + sqall[d, 2 * j, i] + sqall[d, 2 * j + 1, i]
        table[pl.ds(m, 1)] = line
    index = lax.broadcasted_iota(jnp.int32, table.shape, 0)
    bucket = jnp.zeros(table.shape, jnp.int32)
    for k in range(start_ref.shape[0]):
        bucket = bucket + (index >= start_ref[k]).astype(jnp.int32)
    sums = table[...]
    clip = jnp.zeros(table.shape, f32)
    for k in range(start_ref.shape[0] + 1):
        inside = (bucket == k) & (index < MATS)
        total = jnp.sum(jnp.where(inside, sums, 0.0), axis=(0, 1), keepdims=True)
        count = jnp.sum(inside.astype(f32), axis=(0, 1), keepdims=True) / lanes
        mean = total / (jnp.maximum(count, 1.0) * (2 * rows) * (n_shard * cols))
        clip = jnp.where(inside, jnp.minimum(1.0, clip_level / jnp.sqrt(mean + epsilon)), clip)
    for m in range(MATS):
        factor[m] = jnp.concatenate([clip[m : m + 1, :]] * (cols // lanes), axis=1)

    def advance(matrix, gradient, past):
        step = factor[matrix] * gradient.astype(f32)
        new = momentum_rate * past + step
        return new, (step + momentum_rate * new).astype(bf16)

    gathers[4].wait_recv()
    for i in range(members):
        layer, side = lodged(block, i)
        matrix = 2 * layer + side
        uown[i] = advance(matrix, gall[block, i], momentum[matrix])[1]
    over = (((1,), (1,)), ((), ()))
    parts = []
    for i, (hz, hc) in enumerate(HOMES):
        here = (z == hz) & (core == hc)
        owner = (base + hc, hz)
        low = uown[i, :rows]
        high = uown[i, rows:]
        own = jnp.where(core == 0, low, high)
        diag = lax.dot_general(own, own, over, preferred_element_type=f32)
        gram_out[i, 0] = diag
        part = remote(gram_out.at[i, 0], gram_in.at[z, core], as_.at[i, 0], ar.at[z, core], owner)
        cross = remote(gram_out.at[i, 1], gram_in.at[z, 2], as_.at[i, 1], ar.at[z, 2], owner)
        parts.append((here, part, cross))

        @pl.when(here)
        def _():
            gram_in[z, core] = diag

        @pl.when(jnp.logical_not(here))
        def _():
            part.start()

        @pl.when(core == 0)
        def _():
            off = lax.dot_general(low, high, over, preferred_element_type=f32)
            gram_out[i, 1] = off

            @pl.when(here)
            def _():
                gram_in[z, 2] = off

            @pl.when(jnp.logical_not(here))
            def _():
                cross.start()

    plane_gather_turn(z, at_g, gs, gr, gathers)
    plane_gather_finish(z, at_g, gs, gr, gathers, last=(7, 8, 9))

    def slot_matrix(shard, slot):
        found = jnp.int32(0)
        count = jnp.int32(0)
        for m in range(MATS):
            yes = owner_ref[m] == shard
            found = jnp.where(yes & (count == slot), m, found)
            count = count + yes.astype(jnp.int32)
        return found

    sends = []
    for d in (1, 3, 2):
        shard = lax.rem(z + d, n_shard)
        matrix = slot_matrix(shard, block)
        home, member = lodging(matrix)
        held[d - 1] = advance(matrix, gall[home, member, mine], momentum[matrix, mine])[1]
        c = remote(
            held.at[d - 1], wall_ref.at[n_shard - d - 1, block, mine],
            ws.at[d - 1], wr.at[d - 1], (me, shard),
        )
        c.start()
        sends.append((d, c))

    def all_one(m, carry):
        home, member = lodging(m)
        new, turned = advance(m, gall[home, member], momentum[m])
        mout_ref[m] = new
        u_ref[m] = turned
        return carry

    lax.fori_loop(0, MATS, all_one, 0)

    is_home = functools.reduce(jnp.logical_or, [here for here, _, _ in parts])
    member = jnp.where(z == HOMES[0][0], 0, 1 + core)
    roots = []
    for d in range(n_shard):
        for c in range(2):
            if d == 0 and c == 1:
                continue
            peer = (to_core, z) if d == 0 else (base + c, lax.rem(z + d, n_shard))
            half = 1 - core if d == 0 else c
            cut = pl.ds(pl.multiple_of(half * rows, rows), rows)
            k = len(roots)
            roots.append(remote(root.at[cut], qall_ref.at[block, member, cut], rs.at[k], rr.at[member], peer))

    @pl.when(is_home)
    def _():
        for d in range(n_shard):
            for k in range(3):
                source = remote(gram_out.at[0, 0], gram_in.at[d, k], as_.at[0, 0], ar.at[d, k], (to_core, z))
                local = (z == d) & ((core == k) if k < 2 else (core == 0))

                @pl.when(jnp.logical_not(local))
                def _():
                    source.wait_recv()

        blocks = []
        for k in range(3):
            value = gram_in[0, k]
            for d in range(1, n_shard):
                value = value + gram_in[d, k]
            blocks.append(value)
        top = jnp.concatenate([blocks[0], blocks[2]], axis=1)
        bottom = jnp.concatenate([blocks[2].T, blocks[1]], axis=1)
        result = gram_iteration(jnp.concatenate([top, bottom], axis=0), scale, gram_scr, root_scr)
        root[...] = result.astype(bf16)
        for c in roots:
            c.start()
        qall_ref[block, member, mine] = root[mine]

    at_w = {d: block_at(wall_ref.at[n_shard - d - 1], 1, rows) for d, _ in sends}
    walls = {}
    for d, c in sends:
        c.wait_recv()
        walls[d] = plane_gather_start(z, at_w[d], os_.at[d - 1], or_.at[d - 1])
    order = [d for d, _ in sends]
    plane_gather_turn(z, at_w[order[0]], os_.at[order[0] - 1], or_.at[order[0] - 1], walls[order[0]])
    for i, (here, _, _) in enumerate(parts):
        arrival = remote(root.at[mine], qall_ref.at[block, i, mine], rs.at[0], rr.at[i], (to_core, z))

        @pl.when(jnp.logical_not(here))
        def _():
            arrival.wait_recv()

    at_q = block_at(qall_ref, 2, rows)
    gathers_q = plane_gather_start(z, at_q, hs, hr)
    for d in order[1:]:
        plane_gather_turn(z, at_w[d], os_.at[d - 1], or_.at[d - 1], walls[d])
    plane_gather_turn(z, at_q, hs, hr, gathers_q)
    for d in order:
        plane_gather_finish(z, at_w[d], os_.at[d - 1], or_.at[d - 1], walls[d])
    plane_gather_finish(z, at_q, hs, hr, gathers_q)

    @pl.when(is_home)
    def _():
        for c in roots:
            c.wait_send()

    for here, part, cross in parts:

        @pl.when(jnp.logical_not(here))
        def _():
            part.wait_send()

            @pl.when(core == 0)
            def _():
                cross.wait_send()

    for _, c in sends:
        c.wait_send()
    for c in squares + lines:
        c.wait_send()


def finish_kernel(
    owner_ref, mout_ref, u_ref, wall_ref, qall_ref, mom_out, update_out, owned_out,
    ubuf, wbuf, msem, usem, wsem,
):
    f32 = jnp.float32
    slots, _, width = wbuf.shape
    mats, _, cols = ubuf.shape
    n_shard = width // cols
    z = lax.axis_index("shard")
    whole = pltpu.make_async_copy(mout_ref, mom_out, msem)
    whole.start()

    def put(buf, out, sem, m):
        return pltpu.make_async_copy(buf.at[m], out.at[m], sem.at[m])

    def update_one(m, carry):
        home, member = lodging(m)
        ubuf[m] = jnp.dot(qall_ref[home, member], u_ref[m], preferred_element_type=f32)
        put(ubuf, update_out, usem, m).start()
        return carry

    lax.fori_loop(0, mats, update_one, 0)

    def owned_one(s, carry):
        matrix = jnp.int32(0)
        count = jnp.int32(0)
        for m in range(mats):
            yes = owner_ref[m] == z
            matrix = jnp.where(yes & (count == s), m, matrix)
            count = count + yes.astype(jnp.int32)
        keep = (count > s).astype(f32)
        home, member = lodging(matrix)
        q = qall_ref[home, member]
        for d in range(n_shard):
            right = u_ref[matrix] if d == 0 else wall_ref[d - 1, s]
            value = jnp.dot(q, right, preferred_element_type=f32) * keep
            at = lax.rem(z + d, n_shard)
            wbuf[s, :, pl.ds(pl.multiple_of(at * cols, cols), cols)] = value.astype(wbuf.dtype)
        put(wbuf, owned_out, wsem, s).start()
        return carry

    lax.fori_loop(0, slots, owned_one, 0)

    def each(count, buf, out, sem):
        def step(m, carry):
            put(buf, out, sem, m).wait()
            return carry

        lax.fori_loop(0, count, step, 0)

    whole.wait()
    each(mats, ubuf, update_out, usem)
    each(slots, wbuf, owned_out, wsem)


def per_device_planes(activations, cotangents, momentum, owners, bucket_starts):
    n_shard = lax.axis_size("shard")
    n_rep = lax.axis_size("rep")
    layers, tok_rows, width = activations.shape
    token_total = tok_rows * n_shard * n_rep
    cols = width // n_shard
    rows = KV // 2
    lanes = math.gcd(cols, 128)
    groups = n_rep // 2
    members = MATS // groups
    slots = -(-MATS // n_shard) + 1
    update_scale = math.sqrt(max(KV, D))
    bf16, f32 = jnp.bfloat16, jnp.float32

    def params(limit, **rest):
        return pltpu.CompilerParams(vmem_limit_bytes=limit * 1024 * 1024, **rest)

    dma = pltpu.SemaphoreType.DMA
    gown, sq = pl.pallas_call(
        functools.partial(reduce_kernel, n_shard, 1.0 / math.sqrt(token_total)),
        out_shape=(
            pltpu.VMEM((members, rows, cols), bf16),
            pltpu.VMEM((members, 1, lanes), f32),
        ),
        in_specs=[ANY_SPEC, ANY_SPEC],
        out_specs=(VMEM_SPEC, VMEM_SPEC),
        scratch_shapes=[
            [pltpu.VMEM((layers, 2 * tok_rows, cols), bf16) for _ in range(n_shard)],
            pltpu.VMEM((layers, 2 * tok_rows, 2 * KV), bf16),
            pltpu.VMEM((n_shard, 2, 2, members, rows, cols), bf16),
            pltpu.VMEM((n_shard, 2, members, rows, cols), bf16),
            pltpu.VMEM((n_shard, members, rows, cols), bf16),
            pltpu.VMEM((n_shard, members, rows, cols), bf16),
            pltpu.VMEM((n_shard, members, rows, cols), bf16),
            pltpu.VMEM((n_shard - 1, members, rows, cols), bf16),
            dma((n_shard + 1,)), dma((n_shard + 1,)), dma((n_shard + 1,)),
            dma((n_shard,)), dma((n_shard,)), dma((n_shard,)), dma((n_shard,)),
            dma((n_shard,)), dma((n_shard,)),
        ],
        compiler_params=params(44, has_side_effects=True, collective_id=0),
        name="reduce",
    )(activations, cotangents)

    mout, turned, wall, qall = pl.pallas_call(
        functools.partial(settle_kernel, n_shard, update_scale),
        out_shape=(
            pltpu.VMEM((MATS, KV, cols), f32),
            pltpu.VMEM((MATS, KV, cols), bf16),
            pltpu.VMEM((n_shard - 1, slots, KV, cols), bf16),
            pltpu.VMEM((groups, members, KV, KV), bf16),
        ),
        in_specs=[SMEM_SPEC, SMEM_SPEC, ANY_SPEC, VMEM_SPEC, VMEM_SPEC],
        out_specs=(VMEM_SPEC,) * 4,
        scratch_shapes=[
            pltpu.VMEM((MATS, KV, cols), f32),
            pltpu.VMEM((groups, members, KV, cols), bf16),
            pltpu.VMEM((n_shard, n_rep, members, 1, lanes), f32),
            pltpu.VMEM((16, lanes), f32),
            pltpu.VMEM((MATS, 1, cols), f32),
            pltpu.VMEM((members, KV, cols), bf16),
            pltpu.VMEM((n_shard - 1, rows, cols), bf16),
            pltpu.VMEM((members, 2, rows, rows), f32),
            pltpu.VMEM((n_shard, 3, rows, rows), f32),
            pltpu.VMEM((KV, KV), f32),
            pltpu.VMEM((KV, KV), f32),
            pltpu.VMEM((KV, KV), bf16),
            dma(()),
            dma((7,)), dma((7,)), dma((n_shard - 1,)), dma((n_shard - 1,)),
            dma((10,)), dma((10,)),
            dma((members, 2)), dma((n_shard, 3)),
            dma((n_shard - 1,)), dma((n_shard - 1,)),
            dma((n_shard - 1, 10)), dma((n_shard - 1, 10)),
            dma((2 * n_shard - 1,)), dma((members,)),
            dma((10,)), dma((10,)),
        ],
        compiler_params=params(32, has_side_effects=True, collective_id=1),
        name="settle",
    )(owners, bucket_starts, momentum, gown, sq)

    return pl.pallas_call(
        finish_kernel,
        out_shape=(
            jax.ShapeDtypeStruct(momentum.shape, f32),
            jax.ShapeDtypeStruct(momentum.shape, f32),
            jax.ShapeDtypeStruct((slots, KV, width), bf16),
        ),
        in_specs=[SMEM_SPEC] + [VMEM_SPEC] * 4,
        out_specs=(ANY_SPEC,) * 3,
        scratch_shapes=[
            pltpu.VMEM(momentum.shape, f32),
            pltpu.VMEM((slots, KV, width), bf16),
            dma(()), dma((MATS,)), dma((slots,)),
        ],
        compiler_params=params(20),
        name="finish",
    )(owners, mout, turned, wall, qall)


def solution(mesh):
    groups = mesh.shape["rep"] // 2
    slots = -(-MATS // mesh.shape["shard"]) + 1
    fits = mesh.shape["rep"] == 8 and mesh.shape["shard"] == 4 and slots <= groups
    placed = (
        P(None, ("rep", "shard"), None),
        P(None, ("rep", "shard"), None),
        P(None, None, "shard"),
        P(),
        P(),
    )
    return jax.shard_map(
        per_device_planes if fits else per_device_general,
        mesh=mesh,
        in_specs=placed,
        out_specs=(P(None, None, "shard"), P(None, None, "shard"), P("shard", None, None)),
        check_vma=False,
    )
```

```python
import functools
import math

import jax
import jax.numpy as jnp
from jax import lax
from jax.experimental import pallas as pl
from jax.experimental.pallas import tpu as pltpu
from jax.sharding import PartitionSpec as P

D = 2048
KV = 256
ITERS = 5
MATS = 12
MESH = pl.DeviceIdType.MESH
VMEM_SPEC = pl.BlockSpec(memory_space=pltpu.VMEM)
SMEM_SPEC = pl.BlockSpec(memory_space=pltpu.SMEM)
ANY_SPEC = pl.BlockSpec(memory_space=pl.ANY)
VMEM_LIMIT = 60 * 1024 * 1024

coef_a = 3.4445
coef_b = -4.775
coef_c = 2.0315
momentum_rate = 0.95
clip_level = 0.5
epsilon = 1e-06


def orthogonal_batch(matrices):
    values = matrices.astype(jnp.float32)
    frobenius = jnp.sqrt(jnp.sum(values * values, axis=(1, 2), keepdims=True))
    matrix = (values / (frobenius + epsilon)).astype(jnp.bfloat16)
    for iteration in range(ITERS):
        gram_matrix = jnp.einsum(
            "skd,sjd->skj", matrix, matrix, preferred_element_type=jnp.float32
        ).astype(jnp.bfloat16)
        square = jnp.einsum(
            "skj,sji->ski", gram_matrix, gram_matrix, preferred_element_type=jnp.float32
        )
        mixing = (coef_b * gram_matrix.astype(jnp.float32) + coef_c * square).astype(jnp.bfloat16)
        product = jnp.einsum("skj,sjd->skd", mixing, matrix, preferred_element_type=jnp.float32)
        matrix = (coef_a * matrix.astype(jnp.float32) + product).astype(jnp.bfloat16)
    return matrix


def clip_factors(square_sums, bucket_starts):
    indices = jnp.arange(MATS, dtype=jnp.int32)
    buckets = jnp.sum((indices[:, None] >= bucket_starts[None, :]).astype(jnp.int32), axis=1)
    together = (buckets[:, None] == buckets[None, :]).astype(jnp.float32)
    totals = jnp.sum(together * square_sums[None, :], axis=1)
    members = jnp.sum(together, axis=1)
    root_mean = jnp.sqrt(totals / (members * KV * D) + epsilon)
    return jnp.minimum(1.0, clip_level / root_mean)


def slot_numbers(owners):
    indices = jnp.arange(MATS, dtype=jnp.int32)
    earlier = (indices[None, :] < indices[:, None]) & (owners[None, :] == owners[:, None])
    return jnp.sum(earlier.astype(jnp.int32), axis=1)


def selector(owner_of, slot_of, shard_count, slot_count):
    holders = lax.broadcasted_iota(jnp.int32, (shard_count, slot_count, 1), 0)
    places = lax.broadcasted_iota(jnp.int32, (shard_count, slot_count, 1), 1)
    chosen = (holders == owner_of[None, None, :]) & (places == slot_of[None, None, :])
    return chosen.astype(jnp.bfloat16)


def pack_slots(shards, chooser):
    return jnp.einsum("psm,mkd->skpd", chooser, shards, preferred_element_type=jnp.float32).astype(
        jnp.bfloat16
    )


def unpack_slots(received, chooser):
    return jnp.einsum("psm,skpd->mkd", chooser, received, preferred_element_type=jnp.float32)


def per_device_general(activations, cotangents, momentum, owners, bucket_starts):
    shard_count = lax.axis_size("shard")
    replica_count = lax.axis_size("rep")
    layers, tok_rows, width = activations.shape
    token_total = tok_rows * shard_count * replica_count
    columns = width // shard_count
    slot_count = -(-MATS // shard_count) + 1
    update_scale = math.sqrt(max(KV, D))
    partial_terms = jnp.einsum(
        "ltk,ltd->lkd", cotangents, activations, preferred_element_type=jnp.float32
    ).reshape(MATS, KV, width)
    shard_part = lax.psum_scatter(
        partial_terms.astype(jnp.bfloat16), "shard", scatter_dimension=2, tiled=True
    )
    summed = lax.psum(shard_part, "rep").astype(jnp.float32)
    gradient = summed / jnp.sqrt(jnp.float32(token_total))
    square_sums = lax.psum(jnp.sum(gradient * gradient, axis=(1, 2)), "shard")
    factors = clip_factors(square_sums, bucket_starts)
    momentum_out = momentum_rate * momentum + factors[:, None, None] * gradient
    nesterov = (factors[:, None, None] * gradient + momentum_rate * momentum_out).astype(
        jnp.bfloat16
    )
    slot_of = slot_numbers(owners)
    chooser = selector(owners, slot_of, shard_count, slot_count)
    received = lax.all_to_all(
        pack_slots(nesterov, chooser), "shard", split_axis=2, concat_axis=2, tiled=True
    )
    item_count = received.shape[0]
    result = orthogonal_batch(received.reshape(item_count, KV, width))
    scaled = (update_scale * result.astype(jnp.float32)).astype(jnp.bfloat16)
    returned_part = lax.all_to_all(
        result.reshape(item_count, KV, shard_count, columns),
        "shard",
        split_axis=2,
        concat_axis=2,
        tiled=True,
    )
    update = update_scale * unpack_slots(returned_part, chooser)
    return (momentum_out, update, scaled)


def lodged(block, member):
    x = lax.rem(block, 2)
    y = lax.div(block, 2)
    whole = 2 * x + y
    paired = 4 + y
    return jnp.where(member < 2, whole, paired), jnp.where(member < 2, member, x)


def lodging(matrix):
    layer = lax.div(matrix, 2)
    side = lax.rem(matrix, 2)
    early = matrix < 8
    x = jnp.where(early, lax.div(layer, 2), side)
    y = jnp.where(early, lax.rem(layer, 2), layer - 4)
    return 2 * y + x, jnp.where(early, side, 2)


def place():
    me = lax.axis_index("rep")
    core = lax.rem(me, 2)
    x = lax.rem(lax.div(me, 2), 2)
    y = lax.div(me, 4)
    to_core = me + 1 - 2 * core
    to_x = me + 2 - 4 * x
    to_y = me + 4 - 8 * y
    to_xy = me + 6 - 4 * x - 8 * y
    return me, core, x, y, to_core, to_x, to_y, to_xy


def greet(peers):
    barrier = pltpu.get_barrier_semaphore()
    for peer in peers:
        pl.semaphore_signal(barrier, inc=1, device_id=peer, device_id_type=MESH)
    pl.semaphore_wait(barrier, len(peers))


def remote(src, dst, send, recv, peer):
    return pltpu.make_async_remote_copy(
        src_ref=src, dst_ref=dst, send_sem=send, recv_sem=recv, device_id=peer, device_id_type=MESH
    )


def plane_gather_start(z, at, send, recv):
    me, core, x, y, to_core, to_x, to_y, to_xy = place()
    plan = ((0, to_x, 0), (2, to_y, 1), (1, to_x, 1), (3, to_y, 0), (4, to_core, None))
    copies = {}
    for k, peer, half in plan:
        copies[k] = remote(at(me, half), at(me, half), send.at[k], recv.at[k], (peer, z))
        copies[k].start()
    return copies


def plane_gather_turn(z, at, send, recv, copies):
    me, core, x, y, to_core, to_x, to_y, to_xy = place()

    def forward(k, block, half, peer):
        copies[k] = remote(
            at(block, half), at(block, half), send.at[k], recv.at[k], (peer, z)
        )
        copies[k].start()

    copies[0].wait_recv()
    forward(5, to_x, 0, to_y)
    copies[2].wait_recv()
    forward(6, to_y, 1, to_x)
    copies[1].wait_recv()
    forward(7, to_x, None, to_core)
    copies[3].wait_recv()
    forward(8, to_y, None, to_core)


def plane_gather_finish(z, at, send, recv, copies, last=(4, 7, 8, 9)):
    me, core, x, y, to_core, to_x, to_y, to_xy = place()
    copies[5].wait_recv()
    copies[6].wait_recv()
    copies[9] = remote(
        at(to_xy, None), at(to_xy, None), send.at[9], recv.at[9], (to_core, z)
    )
    copies[9].start()
    for k in last:
        copies[k].wait_recv()
    for k in range(10):
        copies[k].wait_send()


def gather_reduce(
    n_shard, inverse, act_ref, cot_ref, gall, sqall, act, cot, turned, part, recv, plane, far, zrecv,
    own_sem, swap_s, swap_r, hop_s, hop_r, pass_s, pass_r, sum_s, sum_r, line_s, line_r,
):
    f32 = jnp.float32
    me, core, x, y, to_core, to_x, to_y, to_xy = place()
    z = lax.axis_index("shard")
    tokens = act_ref.shape[1]
    members, rows, cols = plane.shape[1:]
    near = z + 1 - 2 * lax.rem(z, 2)
    across = z + 2 - 4 * lax.div(z, 2)
    targets = (n_shard - 1 - z, across, near, z)
    cut = [pl.ds(pl.multiple_of(t * cols, cols), cols) for t in targets]
    counts = [c.shape[0] for c in cot]
    shared = counts[0] * 2
    mine = (counts[0] * x, shared + counts[1] * y)
    yours = (counts[0] * (1 - x), shared + counts[1] * (1 - y))
    peers = (to_x, to_y)
    waits = []

    def source(kind, k, layer):
        span = pl.ds(layer, counts[kind])
        return cot_ref.at[span] if k == n_shard else act_ref.at[span, :, cut[k]]

    def slot(kind, k, s):
        buffer = cot[kind] if k == n_shard else act[kind].at[k]
        return buffer.at[:, pl.ds(s * tokens, tokens)]

    order = [(1, n_shard), (0, n_shard)] + [(kind, k) for k in range(n_shard) for kind in (1, 0)]
    own = {
        (kind, k): pltpu.make_async_copy(
            source(kind, k, mine[kind]), slot(kind, k, 0), own_sem.at[kind, k]
        )
        for kind, k in order
    }
    swap = {
        (kind, k): remote(
            source(kind, k, mine[kind]), slot(kind, k, 1),
            swap_s.at[kind, k], swap_r.at[kind, k], (to_core, z),
        )
        for kind, k in order
    }
    hop = {
        (kind, k): remote(
            source(kind, k, yours[kind]), slot(kind, k, 2),
            hop_s.at[kind, k], hop_r.at[kind, k], (peers[kind], z),
        )
        for kind, k in order
    }
    onward = {
        (kind, k): remote(
            slot(kind, k, 2), slot(kind, k, 3),
            pass_s.at[kind, k], pass_r.at[kind, k], (to_core, z),
        )
        for kind, k in order
    }
    sums = [
        [
            remote(
                part[0].at[k, 1 - y], recv[0].at[k],
                sum_s.at[0, k], sum_r.at[0, k], (to_y, z),
            ),
            remote(
                part[1].at[k, 1 - x], recv[1].at[k],
                sum_s.at[1, k], sum_r.at[1, k], (to_x, z),
            ),
        ]
        for k in range(n_shard)
    ]
    spans = (pl.ds(0, members - 1), pl.ds(members - 1, 1))
    lines = [
        [
            remote(
                (far if m == 1 else plane.at[m]).at[spans[kind]], zrecv.at[m, spans[kind]],
                line_s.at[m, kind], line_r.at[m, kind], (me, across if m == 1 else near),
            )
            for kind in range(2)
        ]
        for m in range(n_shard - 1)
    ]

    def enter():
        for key in order:
            own[key].start()

    def begin():
        for key in order:
            if key != (0, n_shard - 1):
                hop[key].start()
        for key in order:
            swap[key].start()

    def take(kind, k):
        hop[kind, k].wait_recv()
        onward[kind, k].start()

    def ready(kind, k):
        own[kind, k].wait()
        swap[kind, k].wait_recv()
        onward[kind, k].wait_recv()

    def turn(kind):
        ready(kind, n_shard)
        for layer in range(counts[kind]):
            for side in range(2):
                at = pl.ds(pl.multiple_of((2 * side + core) * rows, rows), rows)
                turned[kind][layer, side] = cot[kind][layer, :, at].T

    def product(kind, k):
        ready(kind, k)

        def one(q, carry):
            layer = lax.div(q, 2)
            side = lax.rem(q, 2)
            value = jnp.dot(turned[kind][layer, side], act[kind][k, layer], preferred_element_type=f32)
            if kind == 0:
                part[0][k, layer, side] = value.astype(part[0].dtype)
            else:
                part[1][k, side, 0] = value.astype(part[1].dtype)
            return carry

        lax.fori_loop(0, 2 * counts[kind], one, 0)
        sums[k][kind].start()

    def gather(kind, k):
        sums[k][kind].wait_recv()
        for i in range(members - 1 if kind == 0 else 1):
            kept = part[0][k, y, i] if kind == 0 else part[1][k, x, i]
            value = kept.astype(f32) + recv[kind][k, i].astype(f32)
            plane[k, i if kind == 0 else members - 1] = value.astype(plane.dtype)

    def cross(kind):
        lines[0][kind].wait_recv()
        for i in range(members - 1) if kind == 0 else (members - 1,):
            value = plane[1, i].astype(f32) + zrecv[0, i].astype(f32)
            far[i] = value.astype(far.dtype)
        lines[1][kind].start()

    def run():
        take(1, n_shard)
        take(1, 0)
        take(0, n_shard)
        turn(1)
        product(1, 0)
        take(1, 1)
        turn(0)
        product(1, 1)
        hop[0, n_shard - 1].start()
        take(0, 0)
        take(1, 2)
        product(0, 0)
        product(1, 2)
        take(1, 3)
        product(1, 3)
        take(0, 1)
        product(0, 1)
        gather(0, 0)
        lines[0][0].start()
        take(0, 2)
        product(0, 2)
        gather(1, 0)
        lines[0][1].start()
        gather(0, 1)
        gather(1, 1)
        cross(0)
        cross(1)
        gather(0, 2)
        lines[2][0].start()
        take(0, 3)
        product(0, 3)
        gather(1, 2)
        lines[2][1].start()
        gather(1, 3)
        gather(0, 3)
        for m in (2, 1):
            for c in lines[m]:
                c.wait_recv()
        home = lax.div(me, 2)
        half = pl.ds(pl.multiple_of(core * rows, rows), rows)

        def add_last(j, carry):
            value = plane[n_shard - 1, j].astype(f32)
            for m in (1, 2):
                value = value + zrecv[m, j].astype(f32)
            value = (value * inverse).astype(gall.dtype)
            gall[home, j, half] = value
            value = value.astype(f32)
            line = jnp.sum(value * value, axis=0, keepdims=True)
            lanes = sqall.shape[-1]
            fold = line[:, :lanes]
            for i in range(1, cols // lanes):
                fold = fold + line[:, i * lanes : (i + 1) * lanes]
            sqall[0, me, j] = fold
            return carry

        lax.fori_loop(0, members, add_last, 0)

    def leave():
        for key in order:
            swap[key].wait_send()
            hop[key].wait_send()
            onward[key].wait_send()
        for pair in sums + lines:
            for c in pair:
                c.wait_send()

    return enter, begin, run, leave


HOMES = ((1, 0), (2, 0), (2, 1))


def block_at(ref, axis, rows):
    def at(r, half):
        count = rows if half is None else rows // 2
        start = lax.rem(r, 2) * rows + (0 if half is None else half * count)
        cut = pl.ds(pl.multiple_of(start, count), count)
        block = lax.div(r, 2)
        return ref.at[block, cut] if axis == 1 else ref.at[block, :, cut]

    return at


def split(value):
    high = value.astype(jnp.bfloat16)
    return high, (value - high.astype(jnp.float32)).astype(jnp.bfloat16)


def times(left, right):
    dot = functools.partial(jnp.dot, preferred_element_type=jnp.float32)
    return dot(left[0], right[0]) + (dot(left[0], right[1]) + dot(left[1], right[0]))


def gram_iteration(gram, scale, gram_scr, root_scr):
    n = gram.shape[0]
    row = lax.broadcasted_iota(jnp.int32, (n, n), 0)
    col = lax.broadcasted_iota(jnp.int32, (n, n), 1)
    eye = (row == col).astype(jnp.float32)
    trace = jnp.sum(jnp.sum(gram * eye, axis=0, keepdims=True), axis=1, keepdims=True)
    inverse = 1.0 / (jnp.sqrt(trace) + epsilon)
    gram_scr[...] = gram * inverse * inverse
    for iteration in range(ITERS):
        a = split(gram_scr[...])
        mixing = coef_b * gram_scr[...] + coef_c * times(a, a)
        b = split(mixing)
        if iteration == 0:
            root_scr[...] = coef_a * eye + mixing
        else:
            root_scr[...] = coef_a * root_scr[...] + times(b, split(root_scr[...]))
        if iteration < ITERS - 1:
            half = coef_a * gram_scr[...] + times(b, a)
            gram_scr[...] = coef_a * half + times(b, split(half))
    return root_scr[...] * (inverse * scale)


def muon_kernel(
    n_shard, inverse, scale, owner_ref, start_ref, act_ref, cot_ref, momentum_hbm,
    mout_ref, u_ref, wall_ref, qall_ref,
    momentum, gall, sqall, table, factor, uown, held, gram_out, gram_in, gram_scr, root_scr, root,
    act, cot, turned, part, recv, plane, far, zrecv, reduce_sems,
    load, ps, pr, qs, qr, gs, gr, as_, ar, ws, wr, os_, or_, rs, rr, hs, hr,
):
    f32, bf16 = jnp.float32, jnp.bfloat16
    me, core, x, y, to_core, to_x, to_y, to_xy = place()
    z = lax.axis_index("shard")
    base = me - core
    block = lax.div(me, 2)
    members = gall.shape[1]
    rows, cols = held.shape[1:]
    lanes = sqall.shape[-1]
    other = 1 - 2 * core
    near = (to_core, to_x, to_y, to_xy, to_x + other, to_y + other, to_xy + other)
    mine = pl.ds(pl.multiple_of(core * rows, rows), rows)

    fetch = pltpu.make_async_copy(momentum_hbm, momentum, load)
    enter, begin, run, leave = gather_reduce(
        n_shard, inverse, act_ref, cot_ref, gall, sqall, act, cot, turned, part, recv,
        plane, far, zrecv, *reduce_sems,
    )
    enter()
    column = [(base + c, lax.rem(z + d, n_shard)) for d in range(1, n_shard) for c in range(2)]
    greet([(p, z) for p in near] + column)

    begin()
    fetch.start()
    run()

    squares = []
    for k, peer in enumerate(near):
        c = remote(sqall.at[0, me], sqall.at[0, me], ps.at[k], pr.at[k], (peer, z))
        c.start()
        squares.append(c)
    at_g = block_at(gall, 2, rows)
    gathers = plane_gather_start(z, at_g, gs, gr)
    for c in squares:
        c.wait_recv()
    lines = []
    for d in range(1, n_shard):
        c = remote(sqall.at[0], sqall.at[d], qs.at[d - 1], qr.at[d - 1], (me, lax.rem(z + d, n_shard)))
        c.start()
        lines.append(c)
    fetch.wait()
    for c in lines:
        c.wait_recv()

    table[...] = jnp.zeros_like(table)
    for m in range(MATS):
        layer, side = divmod(m, 2)
        bx, by = divmod(layer, 2) if m < 8 else (side, layer - 4)
        j, i = 2 * by + bx, side if m < 8 else 2
        line = sqall[0, 2 * j, i] + sqall[0, 2 * j + 1, i]
        for d in range(1, n_shard):
            line = line + sqall[d, 2 * j, i] + sqall[d, 2 * j + 1, i]
        table[pl.ds(m, 1)] = line
    index = lax.broadcasted_iota(jnp.int32, table.shape, 0)
    bucket = jnp.zeros(table.shape, jnp.int32)
    for k in range(start_ref.shape[0]):
        bucket = bucket + (index >= start_ref[k]).astype(jnp.int32)
    sums = table[...]
    clip = jnp.zeros(table.shape, f32)
    for k in range(start_ref.shape[0] + 1):
        inside = (bucket == k) & (index < MATS)
        total = jnp.sum(jnp.where(inside, sums, 0.0), axis=(0, 1), keepdims=True)
        count = jnp.sum(inside.astype(f32), axis=(0, 1), keepdims=True) / lanes
        mean = total / (jnp.maximum(count, 1.0) * (2 * rows) * (n_shard * cols))
        clip = jnp.where(inside, jnp.minimum(1.0, clip_level / jnp.sqrt(mean + epsilon)), clip)
    for m in range(MATS):
        factor[m] = jnp.concatenate([clip[m : m + 1, :]] * (cols // lanes), axis=1)

    def advance(matrix, gradient, past):
        step = factor[matrix] * gradient.astype(f32)
        new = momentum_rate * past + step
        return new, (step + momentum_rate * new).astype(bf16)

    gathers[4].wait_recv()
    for i in range(members):
        layer, side = lodged(block, i)
        matrix = 2 * layer + side
        uown[i] = advance(matrix, gall[block, i], momentum[matrix])[1]
    over = (((1,), (1,)), ((), ()))
    parts = []
    for i, (hz, hc) in enumerate(HOMES):
        here = (z == hz) & (core == hc)
        owner = (base + hc, hz)
        low = uown[i, :rows]
        high = uown[i, rows:]
        own = jnp.where(core == 0, low, high)
        diag = lax.dot_general(own, own, over, preferred_element_type=f32)
        gram_out[i, 0] = diag
        part = remote(gram_out.at[i, 0], gram_in.at[z, core], as_.at[i, 0], ar.at[z, core], owner)
        cross = remote(gram_out.at[i, 1], gram_in.at[z, 2], as_.at[i, 1], ar.at[z, 2], owner)
        parts.append((here, part, cross))

        @pl.when(here)
        def _():
            gram_in[z, core] = diag

        @pl.when(jnp.logical_not(here))
        def _():
            part.start()

        @pl.when(core == 0)
        def _():
            off = lax.dot_general(low, high, over, preferred_element_type=f32)
            gram_out[i, 1] = off

            @pl.when(here)
            def _():
                gram_in[z, 2] = off

            @pl.when(jnp.logical_not(here))
            def _():
                cross.start()

    plane_gather_turn(z, at_g, gs, gr, gathers)
    plane_gather_finish(z, at_g, gs, gr, gathers, last=(7, 8, 9))

    def slot_matrix(shard, slot):
        found = jnp.int32(0)
        count = jnp.int32(0)
        for m in range(MATS):
            yes = owner_ref[m] == shard
            found = jnp.where(yes & (count == slot), m, found)
            count = count + yes.astype(jnp.int32)
        return found

    sends = []
    for d in (1, 3, 2):
        shard = lax.rem(z + d, n_shard)
        matrix = slot_matrix(shard, block)
        home, member = lodging(matrix)
        held[d - 1] = advance(matrix, gall[home, member, mine], momentum[matrix, mine])[1]
        c = remote(
            held.at[d - 1], wall_ref.at[n_shard - d - 1, block, mine],
            ws.at[d - 1], wr.at[d - 1], (me, shard),
        )
        c.start()
        sends.append((d, c))

    def all_one(m, carry):
        home, member = lodging(m)
        new, turned = advance(m, gall[home, member], momentum[m])
        mout_ref[m] = new
        u_ref[m] = turned
        return carry

    lax.fori_loop(0, MATS, all_one, 0)

    is_home = functools.reduce(jnp.logical_or, [here for here, _, _ in parts])
    member = jnp.where(z == HOMES[0][0], 0, 1 + core)
    roots = []
    for d in range(n_shard):
        for c in range(2):
            if d == 0 and c == 1:
                continue
            peer = (to_core, z) if d == 0 else (base + c, lax.rem(z + d, n_shard))
            half = 1 - core if d == 0 else c
            cut = pl.ds(pl.multiple_of(half * rows, rows), rows)
            k = len(roots)
            roots.append(remote(root.at[cut], qall_ref.at[block, member, cut], rs.at[k], rr.at[member], peer))

    @pl.when(is_home)
    def _():
        for d in range(n_shard):
            for k in range(3):
                source = remote(gram_out.at[0, 0], gram_in.at[d, k], as_.at[0, 0], ar.at[d, k], (to_core, z))
                local = (z == d) & ((core == k) if k < 2 else (core == 0))

                @pl.when(jnp.logical_not(local))
                def _():
                    source.wait_recv()

        blocks = []
        for k in range(3):
            value = gram_in[0, k]
            for d in range(1, n_shard):
                value = value + gram_in[d, k]
            blocks.append(value)
        top = jnp.concatenate([blocks[0], blocks[2]], axis=1)
        bottom = jnp.concatenate([blocks[2].T, blocks[1]], axis=1)
        result = gram_iteration(jnp.concatenate([top, bottom], axis=0), scale, gram_scr, root_scr)
        root[...] = result.astype(bf16)
        for c in roots:
            c.start()
        qall_ref[block, member, mine] = root[mine]

    at_w = {d: block_at(wall_ref.at[n_shard - d - 1], 1, rows) for d, _ in sends}
    walls = {}
    for d, c in sends:
        c.wait_recv()
        walls[d] = plane_gather_start(z, at_w[d], os_.at[d - 1], or_.at[d - 1])
    order = [d for d, _ in sends]
    plane_gather_turn(z, at_w[order[0]], os_.at[order[0] - 1], or_.at[order[0] - 1], walls[order[0]])
    for i, (here, _, _) in enumerate(parts):
        arrival = remote(root.at[mine], qall_ref.at[block, i, mine], rs.at[0], rr.at[i], (to_core, z))

        @pl.when(jnp.logical_not(here))
        def _():
            arrival.wait_recv()

    at_q = block_at(qall_ref, 2, rows)
    gathers_q = plane_gather_start(z, at_q, hs, hr)
    for d in order[1:]:
        plane_gather_turn(z, at_w[d], os_.at[d - 1], or_.at[d - 1], walls[d])
    plane_gather_turn(z, at_q, hs, hr, gathers_q)
    for d in order:
        plane_gather_finish(z, at_w[d], os_.at[d - 1], or_.at[d - 1], walls[d])
    plane_gather_finish(z, at_q, hs, hr, gathers_q)

    @pl.when(is_home)
    def _():
        for c in roots:
            c.wait_send()

    for here, part, cross in parts:

        @pl.when(jnp.logical_not(here))
        def _():
            part.wait_send()

            @pl.when(core == 0)
            def _():
                cross.wait_send()

    for _, c in sends:
        c.wait_send()
    for c in squares + lines:
        c.wait_send()
    leave()


def finish_kernel(
    owner_ref, mout_ref, u_ref, wall_ref, qall_ref, mom_out, update_out, owned_out,
    ubuf, wbuf, msem, usem, wsem,
):
    f32 = jnp.float32
    slots, _, width = wbuf.shape
    mats, _, cols = ubuf.shape
    n_shard = width // cols
    z = lax.axis_index("shard")
    whole = pltpu.make_async_copy(mout_ref, mom_out, msem)
    whole.start()

    def put(buf, out, sem, m):
        return pltpu.make_async_copy(buf.at[m], out.at[m], sem.at[m])

    def update_one(m, carry):
        home, member = lodging(m)
        ubuf[m] = jnp.dot(qall_ref[home, member], u_ref[m], preferred_element_type=f32)
        put(ubuf, update_out, usem, m).start()
        return carry

    lax.fori_loop(0, mats, update_one, 0)

    def owned_one(s, carry):
        matrix = jnp.int32(0)
        count = jnp.int32(0)
        for m in range(mats):
            yes = owner_ref[m] == z
            matrix = jnp.where(yes & (count == s), m, matrix)
            count = count + yes.astype(jnp.int32)
        keep = (count > s).astype(f32)
        home, member = lodging(matrix)
        q = qall_ref[home, member]
        for d in range(n_shard):
            right = u_ref[matrix] if d == 0 else wall_ref[d - 1, s]
            value = jnp.dot(q, right, preferred_element_type=f32) * keep
            at = lax.rem(z + d, n_shard)
            wbuf[s, :, pl.ds(pl.multiple_of(at * cols, cols), cols)] = value.astype(wbuf.dtype)
        put(wbuf, owned_out, wsem, s).start()
        return carry

    lax.fori_loop(0, slots, owned_one, 0)

    def each(count, buf, out, sem):
        def step(m, carry):
            put(buf, out, sem, m).wait()
            return carry

        lax.fori_loop(0, count, step, 0)

    whole.wait()
    each(mats, ubuf, update_out, usem)
    each(slots, wbuf, owned_out, wsem)


def per_device_planes(activations, cotangents, momentum, owners, bucket_starts):
    n_shard = lax.axis_size("shard")
    n_rep = lax.axis_size("rep")
    layers, tok_rows, width = activations.shape
    token_total = tok_rows * n_shard * n_rep
    cols = width // n_shard
    rows = KV // 2
    lanes = math.gcd(cols, 128)
    groups = n_rep // 2
    members = MATS // groups
    slots = -(-MATS // n_shard) + 1
    update_scale = math.sqrt(max(KV, D))
    bf16, f32 = jnp.bfloat16, jnp.float32

    def params(limit, **rest):
        return pltpu.CompilerParams(vmem_limit_bytes=limit * 1024 * 1024, **rest)

    dma = pltpu.SemaphoreType.DMA
    tokens = 4 * tok_rows
    shares = (layers // 3, layers // 6)
    hbm = functools.partial(pltpu.with_memory_space_constraint, memory_space=pltpu.HBM)
    mout, turned, wall, qall = pl.pallas_call(
        functools.partial(muon_kernel, n_shard, 1.0 / math.sqrt(token_total), update_scale),
        out_shape=(
            pltpu.VMEM((MATS, KV, cols), f32),
            pltpu.VMEM((MATS, KV, cols), bf16),
            pltpu.VMEM((n_shard - 1, slots, KV, cols), bf16),
            pltpu.VMEM((groups, members, KV, KV), bf16),
        ),
        in_specs=[SMEM_SPEC, SMEM_SPEC, ANY_SPEC, ANY_SPEC, ANY_SPEC],
        out_specs=(VMEM_SPEC,) * 4,
        scratch_shapes=[
            pltpu.VMEM((MATS, KV, cols), f32),
            pltpu.VMEM((groups, members, KV, cols), bf16),
            pltpu.VMEM((n_shard, n_rep, members, 1, lanes), f32),
            pltpu.VMEM((16, lanes), f32),
            pltpu.VMEM((MATS, 1, cols), f32),
            pltpu.VMEM((members, KV, cols), bf16),
            pltpu.VMEM((n_shard - 1, rows, cols), bf16),
            pltpu.VMEM((members, 2, rows, rows), f32),
            pltpu.VMEM((n_shard, 3, rows, rows), f32),
            pltpu.VMEM((KV, KV), f32),
            pltpu.VMEM((KV, KV), f32),
            pltpu.VMEM((KV, KV), bf16),
            [pltpu.VMEM((n_shard, n, tokens, cols), bf16) for n in shares],
            [pltpu.VMEM((n, tokens, 2 * KV), bf16) for n in shares],
            [pltpu.VMEM((n, 2, rows, tokens), bf16) for n in shares],
            [pltpu.VMEM((n_shard, 2, n, rows, cols), bf16) for n in shares],
            [pltpu.VMEM((n_shard, n, rows, cols), bf16) for n in shares],
            pltpu.VMEM((n_shard, members, rows, cols), bf16),
            pltpu.VMEM((members, rows, cols), bf16),
            pltpu.VMEM((n_shard - 1, members, rows, cols), bf16),
            [dma((2, n_shard + 1)) for _ in range(7)]
            + [dma((2, n_shard)) for _ in range(2)]
            + [dma((n_shard - 1, 2)) for _ in range(2)],
            dma(()),
            dma((7,)), dma((7,)), dma((n_shard - 1,)), dma((n_shard - 1,)),
            dma((10,)), dma((10,)),
            dma((members, 2)), dma((n_shard, 3)),
            dma((n_shard - 1,)), dma((n_shard - 1,)),
            dma((n_shard - 1, 10)), dma((n_shard - 1, 10)),
            dma((2 * n_shard - 1,)), dma((members,)),
            dma((10,)), dma((10,)),
        ],
        compiler_params=params(48, has_side_effects=True, collective_id=0),
        name="muon",
    )(owners, bucket_starts, hbm(activations), hbm(cotangents), hbm(momentum))

    return pl.pallas_call(
        finish_kernel,
        out_shape=(
            jax.ShapeDtypeStruct(momentum.shape, f32),
            jax.ShapeDtypeStruct(momentum.shape, f32),
            jax.ShapeDtypeStruct((slots, KV, width), bf16),
        ),
        in_specs=[SMEM_SPEC] + [VMEM_SPEC] * 4,
        out_specs=(ANY_SPEC,) * 3,
        scratch_shapes=[
            pltpu.VMEM(momentum.shape, f32),
            pltpu.VMEM((slots, KV, width), bf16),
            dma(()), dma((MATS,)), dma((slots,)),
        ],
        compiler_params=params(20),
        name="finish",
    )(owners, mout, turned, wall, qall)


def solution(mesh):
    groups = mesh.shape["rep"] // 2
    slots = -(-MATS // mesh.shape["shard"]) + 1
    fits = mesh.shape["rep"] == 8 and mesh.shape["shard"] == 4 and slots <= groups
    placed = (
        P(None, ("rep", "shard"), None),
        P(None, ("rep", "shard"), None),
        P(None, None, "shard"),
        P(),
        P(),
    )
    return jax.shard_map(
        per_device_planes if fits else per_device_general,
        mesh=mesh,
        in_specs=placed,
        out_specs=(P(None, None, "shard"), P(None, None, "shard"), P("shard", None, None)),
        check_vma=False,
    )
```

```python
import functools
import math

import jax
import jax.numpy as jnp
from jax import lax
from jax.experimental import pallas as pl
from jax.experimental.pallas import tpu as pltpu
from jax.sharding import PartitionSpec as P

D = 2048
KV = 256
ITERS = 5
MATS = 12
MESH = pl.DeviceIdType.MESH
VMEM_SPEC = pl.BlockSpec(memory_space=pltpu.VMEM)
SMEM_SPEC = pl.BlockSpec(memory_space=pltpu.SMEM)
ANY_SPEC = pl.BlockSpec(memory_space=pl.ANY)
VMEM_LIMIT = 60 * 1024 * 1024

coef_a = 3.4445
coef_b = -4.775
coef_c = 2.0315
momentum_rate = 0.95
clip_level = 0.5
epsilon = 1e-06


def orthogonal_batch(matrices):
    values = matrices.astype(jnp.float32)
    frobenius = jnp.sqrt(jnp.sum(values * values, axis=(1, 2), keepdims=True))
    matrix = (values / (frobenius + epsilon)).astype(jnp.bfloat16)
    for iteration in range(ITERS):
        gram_matrix = jnp.einsum(
            "skd,sjd->skj", matrix, matrix, preferred_element_type=jnp.float32
        ).astype(jnp.bfloat16)
        square = jnp.einsum(
            "skj,sji->ski", gram_matrix, gram_matrix, preferred_element_type=jnp.float32
        )
        mixing = (coef_b * gram_matrix.astype(jnp.float32) + coef_c * square).astype(jnp.bfloat16)
        product = jnp.einsum("skj,sjd->skd", mixing, matrix, preferred_element_type=jnp.float32)
        matrix = (coef_a * matrix.astype(jnp.float32) + product).astype(jnp.bfloat16)
    return matrix


def clip_factors(square_sums, bucket_starts):
    indices = jnp.arange(MATS, dtype=jnp.int32)
    buckets = jnp.sum((indices[:, None] >= bucket_starts[None, :]).astype(jnp.int32), axis=1)
    together = (buckets[:, None] == buckets[None, :]).astype(jnp.float32)
    totals = jnp.sum(together * square_sums[None, :], axis=1)
    members = jnp.sum(together, axis=1)
    root_mean = jnp.sqrt(totals / (members * KV * D) + epsilon)
    return jnp.minimum(1.0, clip_level / root_mean)


def slot_numbers(owners):
    indices = jnp.arange(MATS, dtype=jnp.int32)
    earlier = (indices[None, :] < indices[:, None]) & (owners[None, :] == owners[:, None])
    return jnp.sum(earlier.astype(jnp.int32), axis=1)


def selector(owner_of, slot_of, shard_count, slot_count):
    holders = lax.broadcasted_iota(jnp.int32, (shard_count, slot_count, 1), 0)
    places = lax.broadcasted_iota(jnp.int32, (shard_count, slot_count, 1), 1)
    chosen = (holders == owner_of[None, None, :]) & (places == slot_of[None, None, :])
    return chosen.astype(jnp.bfloat16)


def pack_slots(shards, chooser):
    return jnp.einsum("psm,mkd->skpd", chooser, shards, preferred_element_type=jnp.float32).astype(
        jnp.bfloat16
    )


def unpack_slots(received, chooser):
    return jnp.einsum("psm,skpd->mkd", chooser, received, preferred_element_type=jnp.float32)


def per_device_general(activations, cotangents, momentum, owners, bucket_starts):
    shard_count = lax.axis_size("shard")
    replica_count = lax.axis_size("rep")
    layers, tok_rows, width = activations.shape
    token_total = tok_rows * shard_count * replica_count
    columns = width // shard_count
    slot_count = -(-MATS // shard_count) + 1
    update_scale = math.sqrt(max(KV, D))
    partial_terms = jnp.einsum(
        "ltk,ltd->lkd", cotangents, activations, preferred_element_type=jnp.float32
    ).reshape(MATS, KV, width)
    shard_part = lax.psum_scatter(
        partial_terms.astype(jnp.bfloat16), "shard", scatter_dimension=2, tiled=True
    )
    summed = lax.psum(shard_part, "rep").astype(jnp.float32)
    gradient = summed / jnp.sqrt(jnp.float32(token_total))
    square_sums = lax.psum(jnp.sum(gradient * gradient, axis=(1, 2)), "shard")
    factors = clip_factors(square_sums, bucket_starts)
    momentum_out = momentum_rate * momentum + factors[:, None, None] * gradient
    nesterov = (factors[:, None, None] * gradient + momentum_rate * momentum_out).astype(
        jnp.bfloat16
    )
    slot_of = slot_numbers(owners)
    chooser = selector(owners, slot_of, shard_count, slot_count)
    received = lax.all_to_all(
        pack_slots(nesterov, chooser), "shard", split_axis=2, concat_axis=2, tiled=True
    )
    item_count = received.shape[0]
    result = orthogonal_batch(received.reshape(item_count, KV, width))
    scaled = (update_scale * result.astype(jnp.float32)).astype(jnp.bfloat16)
    returned_part = lax.all_to_all(
        result.reshape(item_count, KV, shard_count, columns),
        "shard",
        split_axis=2,
        concat_axis=2,
        tiled=True,
    )
    update = update_scale * unpack_slots(returned_part, chooser)
    return (momentum_out, update, scaled)


def lodged(block, member):
    x = lax.rem(block, 2)
    y = lax.div(block, 2)
    whole = 2 * x + y
    paired = 4 + y
    return jnp.where(member < 2, whole, paired), jnp.where(member < 2, member, x)


def lodging(matrix):
    layer = lax.div(matrix, 2)
    side = lax.rem(matrix, 2)
    early = matrix < 8
    x = jnp.where(early, lax.div(layer, 2), side)
    y = jnp.where(early, lax.rem(layer, 2), layer - 4)
    return 2 * y + x, jnp.where(early, side, 2)


def place():
    me = lax.axis_index("rep")
    core = lax.rem(me, 2)
    x = lax.rem(lax.div(me, 2), 2)
    y = lax.div(me, 4)
    to_core = me + 1 - 2 * core
    to_x = me + 2 - 4 * x
    to_y = me + 4 - 8 * y
    to_xy = me + 6 - 4 * x - 8 * y
    return me, core, x, y, to_core, to_x, to_y, to_xy


def greet(peers):
    barrier = pltpu.get_barrier_semaphore()
    for peer in peers:
        pl.semaphore_signal(barrier, inc=1, device_id=peer, device_id_type=MESH)
    pl.semaphore_wait(barrier, len(peers))


def remote(src, dst, send, recv, peer):
    return pltpu.make_async_remote_copy(
        src_ref=src, dst_ref=dst, send_sem=send, recv_sem=recv, device_id=peer, device_id_type=MESH
    )


def plane_gather_start(z, at, send, recv):
    me, core, x, y, to_core, to_x, to_y, to_xy = place()
    plan = ((0, to_x, 0), (2, to_y, 1), (1, to_x, 1), (3, to_y, 0), (4, to_core, None))
    copies = {}
    for k, peer, half in plan:
        copies[k] = remote(at(me, half), at(me, half), send, recv.at[k], (peer, z))
        copies[k].start()
    return copies


def plane_gather_turn(z, at, send, recv, copies):
    me, core, x, y, to_core, to_x, to_y, to_xy = place()

    def forward(k, block, half, peer):
        copies[k] = remote(
            at(block, half), at(block, half), send, recv.at[k], (peer, z)
        )
        copies[k].start()

    copies[0].wait_recv()
    forward(5, to_x, 0, to_y)
    copies[2].wait_recv()
    forward(6, to_y, 1, to_x)
    copies[1].wait_recv()
    forward(7, to_x, None, to_core)
    copies[3].wait_recv()
    forward(8, to_y, None, to_core)


def plane_gather_finish(z, at, send, recv, copies, last=(4, 7, 8, 9)):
    me, core, x, y, to_core, to_x, to_y, to_xy = place()
    copies[5].wait_recv()
    copies[6].wait_recv()
    copies[9] = remote(
        at(to_xy, None), at(to_xy, None), send, recv.at[9], (to_core, z)
    )
    copies[9].start()
    for k in last:
        copies[k].wait_recv()


def drain(ref, semaphore):
    pltpu.make_async_copy(ref, ref, semaphore).wait()


def gather_reduce(
    n_shard, inverse, act_ref, cot_ref, gall, sqall, act, cot, turned, part, recv, plane, far, zrecv,
    in_sem, hop_r, swap_s, hop_s, pass_s, sum_s, sum_r, line_s, line_r,
):
    f32 = jnp.float32
    me, core, x, y, to_core, to_x, to_y, to_xy = place()
    z = lax.axis_index("shard")
    tokens = act_ref.shape[1]
    members, rows, cols = plane.shape[1:]
    near = z + 1 - 2 * lax.rem(z, 2)
    across = z + 2 - 4 * lax.div(z, 2)
    targets = (n_shard - 1 - z, across, near, z)
    cut = [pl.ds(pl.multiple_of(t * cols, cols), cols) for t in targets]
    counts = [c.shape[0] for c in cot]
    shared = counts[0] * 2
    mine = (counts[0] * x, shared + counts[1] * y)
    yours = (counts[0] * (1 - x), shared + counts[1] * (1 - y))
    peers = (to_x, to_y)
    layer_of = ((1 - y, y), (0,))
    keys = [(1, n_shard, 0), (0, n_shard, 0), (1, 0, 0), (0, 0, 0), (0, n_shard, 1), (0, 0, 1)]
    keys += [(kind, k, j) for k in range(1, n_shard) for kind, j in ((1, 0), (0, 0), (0, 1))]

    def index(kind, k, j):
        return 2 * k + j if kind == 0 else 2 * (n_shard + 1) + k

    def source(kind, k, layer):
        return cot_ref.at[layer] if k == n_shard else act_ref.at[layer, :, cut[k]]

    def slots(kind, k, j, first, count):
        layer = layer_of[kind][j]
        buffer = cot[kind].at[layer] if k == n_shard else act[kind].at[k, layer]
        return buffer.at[pl.ds(first * tokens, count * tokens)]

    own, swap, hop, onward = {}, {}, {}, {}
    for key in keys:
        kind, k, j = key
        at = in_sem.at[index(*key)]
        group = 2 * kind + (1 if k == n_shard else 0)
        layer = layer_of[kind][j]
        here = source(kind, k, mine[kind] + layer)
        own[key] = pltpu.make_async_copy(here, slots(*key, 0, 1), at)
        swap[key] = remote(here, slots(*key, 1, 1), swap_s.at[group], at, (to_core, z))
        hop[key] = remote(
            source(kind, k, yours[kind] + layer), slots(*key, 3, 1),
            hop_s.at[group], hop_r.at[index(*key)], (peers[kind], z),
        )
        onward[key] = remote(slots(*key, 3, 1), slots(*key, 2, 1), pass_s.at[group], at, (to_core, z))
    sums = [
        [
            remote(
                part[0].at[k, 1 - y], recv[0].at[k], sum_s.at[0], sum_r.at[0, k], (to_y, z)
            ),
            remote(
                part[1].at[k, 1 - x], recv[1].at[k], sum_s.at[1], sum_r.at[1, k], (to_x, z)
            ),
        ]
        for k in range(n_shard)
    ]
    spans = (pl.ds(0, members - 1), pl.ds(members - 1, 1))
    lines = [
        [
            remote(
                (far if m == 1 else plane.at[m]).at[spans[kind]], zrecv.at[m, spans[kind]],
                line_s.at[kind], line_r.at[m, kind], (me, across if m == 1 else near),
            )
            for kind in range(2)
        ]
        for m in range(n_shard - 1)
    ]

    def enter():
        for key in keys:
            own[key].start()

    def send(kind, k):
        for j in range(counts[kind]):
            hop[kind, k, j].start()

    def begin():
        for key in keys[:6]:
            hop[key].start()
        send(1, 1)
        send(0, 1)
        for key in keys:
            swap[key].start()

    def take(kind, k, j=0):
        hop[kind, k, j].wait_recv()
        onward[kind, k, j].start()

    def ready(kind, k, j):
        drain(slots(kind, k, j, 0, 3), in_sem.at[index(kind, k, j)])

    def turn(kind, j=0):
        ready(kind, n_shard, j)
        layer = layer_of[kind][j]
        for side in range(2):
            at = pl.ds(pl.multiple_of((2 * side + core) * rows, rows), rows)
            turned[kind][layer, side] = cot[kind][layer, :, at].T

    def product(kind, k, j=0):
        ready(kind, k, j)
        layer = layer_of[kind][j]

        def one(side, carry):
            value = jnp.dot(turned[kind][layer, side], act[kind][k, layer], preferred_element_type=f32)
            if kind == 0:
                part[0][k, layer, side] = value.astype(part[0].dtype)
            else:
                part[1][k, side, 0] = value.astype(part[1].dtype)
            return carry

        lax.fori_loop(0, 2, one, 0)
        if j == 0:
            sums[k][kind].start()

    def gather(kind, k):
        sums[k][kind].wait_recv()
        for i in range(members - 1 if kind == 0 else 1):
            kept = part[0][k, y, i] if kind == 0 else part[1][k, x, i]
            value = kept.astype(f32) + recv[kind][k, i].astype(f32)
            plane[k, i if kind == 0 else members - 1] = value.astype(plane.dtype)

    def cross(kind):
        lines[0][kind].wait_recv()
        for i in range(members - 1) if kind == 0 else (members - 1,):
            value = plane[1, i].astype(f32) + zrecv[0, i].astype(f32)
            far[i] = value.astype(far.dtype)
        lines[1][kind].start()

    def run():
        take(1, n_shard)
        take(0, n_shard, 0)
        turn(1)
        take(1, 0)
        take(0, 0, 0)
        turn(0, 0)
        product(1, 0)
        product(0, 0, 0)
        send(1, 2)
        take(1, 1)
        take(0, n_shard, 1)
        product(1, 1)
        send(0, 2)
        turn(0, 1)
        take(0, 0, 1)
        product(0, 0, 1)
        take(0, 1, 0)
        product(0, 1, 0)
        send(1, 3)
        gather(0, 0)
        lines[0][0].start()
        take(0, 1, 1)
        product(0, 1, 1)
        take(1, 2)
        product(1, 2)
        send(0, 3)
        gather(1, 0)
        lines[0][1].start()
        gather(0, 1)
        gather(1, 1)
        cross(0)
        take(0, 2, 0)
        product(0, 2, 0)
        cross(1)
        take(1, 3)
        product(1, 3)
        take(0, 2, 1)
        product(0, 2, 1)
        gather(1, 2)
        lines[2][1].start()
        gather(0, 2)
        lines[2][0].start()
        take(0, 3, 0)
        product(0, 3, 0)
        take(0, 3, 1)
        product(0, 3, 1)
        gather(1, 3)
        gather(0, 3)
        for m in (2, 1):
            for c in lines[m]:
                c.wait_recv()
        home = lax.div(me, 2)
        half = pl.ds(pl.multiple_of(core * rows, rows), rows)

        def add_last(j, carry):
            value = plane[n_shard - 1, j].astype(f32)
            for m in (1, 2):
                value = value + zrecv[m, j].astype(f32)
            value = (value * inverse).astype(gall.dtype)
            gall[home, j, half] = value
            value = value.astype(f32)
            line = jnp.sum(value * value, axis=0, keepdims=True)
            lanes = sqall.shape[-1]
            fold = line[:, :lanes]
            for i in range(1, cols // lanes):
                fold = fold + line[:, i * lanes : (i + 1) * lanes]
            sqall[me * n_shard + z, j] = fold
            return carry

        lax.fori_loop(0, members, add_last, 0)

    def leave():
        for kind in range(2):
            for pool in (swap_s, hop_s, pass_s):
                drain(act[kind].at[:, :, pl.ds(0, tokens)], pool.at[2 * kind])
                drain(cot[kind].at[:, pl.ds(0, tokens)], pool.at[2 * kind + 1])
            drain(recv[kind], sum_s.at[kind])
            drain(zrecv.at[:, spans[kind]], line_s.at[kind])

    return enter, begin, run, leave


HOMES = ((1, 0), (2, 0), (2, 1))


def block_at(ref, axis, rows):
    def at(r, half):
        count = rows if half is None else rows // 2
        start = lax.rem(r, 2) * rows + (0 if half is None else half * count)
        cut = pl.ds(pl.multiple_of(start, count), count)
        block = lax.div(r, 2)
        return ref.at[block, cut] if axis == 1 else ref.at[block, :, cut]

    return at


def split(value):
    high = value.astype(jnp.bfloat16)
    return high, (value - high.astype(jnp.float32)).astype(jnp.bfloat16)


def times(left, right):
    dot = functools.partial(jnp.dot, preferred_element_type=jnp.float32)
    return dot(left[0], right[0]) + (dot(left[0], right[1]) + dot(left[1], right[0]))


def gram_iteration(gram, scale, gram_scr, root_scr):
    n = gram.shape[0]
    row = lax.broadcasted_iota(jnp.int32, (n, n), 0)
    col = lax.broadcasted_iota(jnp.int32, (n, n), 1)
    eye = (row == col).astype(jnp.float32)
    trace = jnp.sum(jnp.sum(gram * eye, axis=0, keepdims=True), axis=1, keepdims=True)
    inverse = 1.0 / (jnp.sqrt(trace) + epsilon)
    gram_scr[...] = gram * inverse * inverse
    for iteration in range(ITERS):
        a = split(gram_scr[...])
        mixing = coef_b * gram_scr[...] + coef_c * times(a, a)
        b = split(mixing)
        if iteration == 0:
            root_scr[...] = coef_a * eye + mixing
        else:
            root_scr[...] = coef_a * root_scr[...] + times(b, split(root_scr[...]))
        if iteration < ITERS - 1:
            half = coef_a * gram_scr[...] + times(b, a)
            gram_scr[...] = coef_a * half + times(b, split(half))
    return root_scr[...] * (inverse * scale)


def muon_kernel(
    n_shard, inverse, scale, owner_ref, start_ref, act_ref, cot_ref, momentum_hbm,
    mout_ref, u_ref, wall_ref, qall_ref,
    momentum, gall, sqall, table, factor, uown, held, gram_out, gram_in, gram_scr, root_scr, root,
    act, cot, turned, part, recv, plane, far, zrecv, reduce_sems,
    load, ps, pr, gs, gr, as_, ar, ws, wr, os_, or_, rs, rr, hs, hr,
):
    f32, bf16 = jnp.float32, jnp.bfloat16
    me, core, x, y, to_core, to_x, to_y, to_xy = place()
    z = lax.axis_index("shard")
    base = me - core
    block = lax.div(me, 2)
    members = gall.shape[1]
    rows, cols = held.shape[1:]
    lanes = sqall.shape[-1]
    mine = pl.ds(pl.multiple_of(core * rows, rows), rows)

    fetch = pltpu.make_async_copy(momentum_hbm, momentum, load)
    enter, begin, run, leave = gather_reduce(
        n_shard, inverse, act_ref, cot_ref, gall, sqall, act, cot, turned, part, recv,
        plane, far, zrecv, *reduce_sems,
    )
    enter()
    everyone = n_shard * 2 * gall.shape[0]
    here = me * n_shard + z
    others = [lax.rem(here + t, everyone) for t in range(1, everyone)]
    others = [(lax.div(to, n_shard), lax.rem(to, n_shard)) for to in others]
    greet(others)

    begin()
    fetch.start()
    run()

    for peer in others:
        remote(sqall.at[here], sqall.at[here], ps, pr, peer).start()
    at_g = block_at(gall, 2, rows)
    gathers = plane_gather_start(z, at_g, gs, gr)
    fetch.wait()
    drain(sqall.at[pl.ds(0, everyone - 1)], pr)

    table[...] = jnp.zeros_like(table)
    for m in range(MATS):
        layer, side = divmod(m, 2)
        bx, by = divmod(layer, 2) if m < 8 else (side, layer - 4)
        j, i = 2 * by + bx, side if m < 8 else 2
        line = sqall[2 * j * n_shard, i]
        for d in range(1, 2 * n_shard):
            line = line + sqall[2 * j * n_shard + d, i]
        table[pl.ds(m, 1)] = line
    index = lax.broadcasted_iota(jnp.int32, table.shape, 0)
    bucket = jnp.zeros(table.shape, jnp.int32)
    for k in range(start_ref.shape[0]):
        bucket = bucket + (index >= start_ref[k]).astype(jnp.int32)
    sums = table[...]
    clip = jnp.zeros(table.shape, f32)
    for k in range(start_ref.shape[0] + 1):
        inside = (bucket == k) & (index < MATS)
        total = jnp.sum(jnp.where(inside, sums, 0.0), axis=(0, 1), keepdims=True)
        count = jnp.sum(inside.astype(f32), axis=(0, 1), keepdims=True) / lanes
        mean = total / (jnp.maximum(count, 1.0) * (2 * rows) * (n_shard * cols))
        clip = jnp.where(inside, jnp.minimum(1.0, clip_level / jnp.sqrt(mean + epsilon)), clip)
    for m in range(MATS):
        factor[m] = jnp.concatenate([clip[m : m + 1, :]] * (cols // lanes), axis=1)

    def advance(matrix, gradient, past):
        step = factor[matrix] * gradient.astype(f32)
        new = momentum_rate * past + step
        return new, (step + momentum_rate * new).astype(bf16)

    gathers[4].wait_recv()
    for i in range(members):
        layer, side = lodged(block, i)
        matrix = 2 * layer + side
        uown[i] = advance(matrix, gall[block, i], momentum[matrix])[1]
    over = (((1,), (1,)), ((), ()))
    parts = []
    for i, (hz, hc) in enumerate(HOMES):
        here = (z == hz) & (core == hc)
        owner = (base + hc, hz)
        low = uown[i, :rows]
        high = uown[i, rows:]
        own = jnp.where(core == 0, low, high)
        diag = lax.dot_general(own, own, over, preferred_element_type=f32)
        gram_out[i, 0] = diag
        part = remote(gram_out.at[i, 0], gram_in.at[z, core], as_.at[i, 0], ar.at[z, core], owner)
        cross = remote(gram_out.at[i, 1], gram_in.at[z, 2], as_.at[i, 1], ar.at[z, 2], owner)
        parts.append((here, part, cross))

        @pl.when(here)
        def _():
            gram_in[z, core] = diag

        @pl.when(jnp.logical_not(here))
        def _():
            part.start()

        @pl.when(core == 0)
        def _():
            off = lax.dot_general(low, high, over, preferred_element_type=f32)
            gram_out[i, 1] = off

            @pl.when(here)
            def _():
                gram_in[z, 2] = off

            @pl.when(jnp.logical_not(here))
            def _():
                cross.start()

    plane_gather_turn(z, at_g, gs, gr, gathers)
    plane_gather_finish(z, at_g, gs, gr, gathers, last=(7, 8, 9))

    def slot_matrix(shard, slot):
        found = jnp.int32(0)
        count = jnp.int32(0)
        for m in range(MATS):
            yes = owner_ref[m] == shard
            found = jnp.where(yes & (count == slot), m, found)
            count = count + yes.astype(jnp.int32)
        return found

    sends = {}

    def send_slice(d):
        shard = lax.rem(z + d, n_shard)
        matrix = slot_matrix(shard, block)
        home, member = lodging(matrix)
        held[d - 1] = advance(matrix, gall[home, member, mine], momentum[matrix, mine])[1]
        sends[d] = remote(
            held.at[d - 1], wall_ref.at[n_shard - d - 1, block, mine], ws, wr.at[d - 1], (me, shard)
        )
        sends[d].start()

    send_slice(1)
    send_slice(3)

    def all_one(m, carry):
        home, member = lodging(m)
        new, turned = advance(m, gall[home, member], momentum[m])
        mout_ref[m] = new
        u_ref[m] = turned
        return carry

    is_home = functools.reduce(jnp.logical_or, [here for here, _, _ in parts])
    member = jnp.where(z == HOMES[0][0], 0, 1 + core)
    roots = []
    for d in range(n_shard):
        for c in range(2):
            if d == 0 and c == 1:
                continue
            peer = (to_core, z) if d == 0 else (base + c, lax.rem(z + d, n_shard))
            half = 1 - core if d == 0 else c
            cut = pl.ds(pl.multiple_of(half * rows, rows), rows)
            roots.append(remote(root.at[cut], qall_ref.at[block, member, cut], rs, rr.at[member], peer))

    @pl.when(is_home)
    def _():
        for d in range(n_shard):
            for k in range(3):
                source = remote(gram_out.at[0, 0], gram_in.at[d, k], as_.at[0, 0], ar.at[d, k], (to_core, z))
                local = (z == d) & ((core == k) if k < 2 else (core == 0))

                @pl.when(jnp.logical_not(local))
                def _():
                    source.wait_recv()

        blocks = []
        for k in range(3):
            value = gram_in[0, k]
            for d in range(1, n_shard):
                value = value + gram_in[d, k]
            blocks.append(value)
        top = jnp.concatenate([blocks[0], blocks[2]], axis=1)
        bottom = jnp.concatenate([blocks[2].T, blocks[1]], axis=1)
        result = gram_iteration(jnp.concatenate([top, bottom], axis=0), scale, gram_scr, root_scr)
        root[...] = result.astype(bf16)
        for c in roots:
            c.start()
        qall_ref[block, member, mine] = root[mine]

    walls = {}

    def at_w(d):
        return block_at(wall_ref.at[n_shard - d - 1], 1, rows)

    for d in (1, 3):
        sends[d].wait_recv()
        walls[d] = plane_gather_start(z, at_w(d), os_.at[d - 1], or_.at[d - 1])
    send_slice(2)
    lax.fori_loop(0, MATS, all_one, 0)
    for d in (1, 3):
        plane_gather_turn(z, at_w(d), os_.at[d - 1], or_.at[d - 1], walls[d])
    for i, (here, _, _) in enumerate(parts):
        arrival = remote(root.at[mine], qall_ref.at[block, i, mine], rs, rr.at[i], (to_core, z))

        @pl.when(jnp.logical_not(here))
        def _():
            arrival.wait_recv()

    at_q = block_at(qall_ref, 2, rows)
    gathers_q = plane_gather_start(z, at_q, hs, hr)
    sends[2].wait_recv()
    walls[2] = plane_gather_start(z, at_w(2), os_.at[1], or_.at[1])
    for d in (1, 3):
        plane_gather_finish(z, at_w(d), os_.at[d - 1], or_.at[d - 1], walls[d])
    plane_gather_turn(z, at_q, hs, hr, gathers_q)
    plane_gather_turn(z, at_w(2), os_.at[1], or_.at[1], walls[2])
    plane_gather_finish(z, at_q, hs, hr, gathers_q)
    plane_gather_finish(z, at_w(2), os_.at[1], or_.at[1], walls[2])
    most = pl.ds(0, 2 * rows - rows // 4)
    drain(gall.at[:, :, most], gs)
    drain(qall_ref.at[:, :, most], hs)
    for d in range(n_shard - 1):
        drain(wall_ref.at[d, :, most], os_.at[d])
    drain(held, ws)
    drain(sqall.at[pl.ds(0, everyone - 1)], ps)

    @pl.when(is_home)
    def _():
        drain(u_ref.at[pl.ds(0, len(roots)), pl.ds(0, rows // 2)], rs)

    for here, part, cross in parts:

        @pl.when(jnp.logical_not(here))
        def _():
            part.wait_send()

            @pl.when(core == 0)
            def _():
                cross.wait_send()

    leave()


def finish_kernel(
    owner_ref, mout_ref, u_ref, wall_ref, qall_ref, mom_out, update_out, owned_out,
    ubuf, wbuf, msem, usem, wsem,
):
    f32 = jnp.float32
    slots, _, width = wbuf.shape
    mats, _, cols = ubuf.shape
    n_shard = width // cols
    z = lax.axis_index("shard")
    whole = pltpu.make_async_copy(mout_ref, mom_out, msem)
    whole.start()

    def put(buf, out, sem, m):
        return pltpu.make_async_copy(buf.at[m], out.at[m], sem.at[m])

    def update_one(m, carry):
        home, member = lodging(m)
        ubuf[m] = jnp.dot(qall_ref[home, member], u_ref[m], preferred_element_type=f32)
        put(ubuf, update_out, usem, m).start()
        return carry

    lax.fori_loop(0, mats, update_one, 0)

    def owned_one(s, carry):
        matrix = jnp.int32(0)
        count = jnp.int32(0)
        for m in range(mats):
            yes = owner_ref[m] == z
            matrix = jnp.where(yes & (count == s), m, matrix)
            count = count + yes.astype(jnp.int32)
        keep = (count > s).astype(f32)
        home, member = lodging(matrix)
        q = qall_ref[home, member]
        for d in range(n_shard):
            right = u_ref[matrix] if d == 0 else wall_ref[d - 1, s]
            value = jnp.dot(q, right, preferred_element_type=f32) * keep
            at = lax.rem(z + d, n_shard)
            wbuf[s, :, pl.ds(pl.multiple_of(at * cols, cols), cols)] = value.astype(wbuf.dtype)
        put(wbuf, owned_out, wsem, s).start()
        return carry

    lax.fori_loop(0, slots, owned_one, 0)

    def each(count, buf, out, sem):
        def step(m, carry):
            put(buf, out, sem, m).wait()
            return carry

        lax.fori_loop(0, count, step, 0)

    whole.wait()
    each(mats, ubuf, update_out, usem)
    each(slots, wbuf, owned_out, wsem)


def per_device_planes(activations, cotangents, momentum, owners, bucket_starts):
    n_shard = lax.axis_size("shard")
    n_rep = lax.axis_size("rep")
    layers, tok_rows, width = activations.shape
    token_total = tok_rows * n_shard * n_rep
    cols = width // n_shard
    rows = KV // 2
    lanes = math.gcd(cols, 128)
    groups = n_rep // 2
    members = MATS // groups
    slots = -(-MATS // n_shard) + 1
    update_scale = math.sqrt(max(KV, D))
    bf16, f32 = jnp.bfloat16, jnp.float32

    def params(limit, **rest):
        return pltpu.CompilerParams(vmem_limit_bytes=limit * 1024 * 1024, **rest)

    dma = pltpu.SemaphoreType.DMA
    tokens = 4 * tok_rows
    shares = (layers // 3, layers // 6)
    hbm = functools.partial(pltpu.with_memory_space_constraint, memory_space=pltpu.HBM)
    mout, turned, wall, qall = pl.pallas_call(
        functools.partial(muon_kernel, n_shard, 1.0 / math.sqrt(token_total), update_scale),
        out_shape=(
            pltpu.VMEM((MATS, KV, cols), f32),
            pltpu.VMEM((MATS, KV, cols), bf16),
            pltpu.VMEM((n_shard - 1, slots, KV, cols), bf16),
            pltpu.VMEM((groups, members, KV, KV), bf16),
        ),
        in_specs=[SMEM_SPEC, SMEM_SPEC, ANY_SPEC, ANY_SPEC, ANY_SPEC],
        out_specs=(VMEM_SPEC,) * 4,
        scratch_shapes=[
            pltpu.VMEM((MATS, KV, cols), f32),
            pltpu.VMEM((groups, members, KV, cols), bf16),
            pltpu.VMEM((n_rep * n_shard, members, 1, lanes), f32),
            pltpu.VMEM((16, lanes), f32),
            pltpu.VMEM((MATS, 1, cols), f32),
            pltpu.VMEM((members, KV, cols), bf16),
            pltpu.VMEM((n_shard - 1, rows, cols), bf16),
            pltpu.VMEM((members, 2, rows, rows), f32),
            pltpu.VMEM((n_shard, 3, rows, rows), f32),
            pltpu.VMEM((KV, KV), f32),
            pltpu.VMEM((KV, KV), f32),
            pltpu.VMEM((KV, KV), bf16),
            [pltpu.VMEM((n_shard, n, tokens, cols), bf16) for n in shares],
            [pltpu.VMEM((n, tokens, 2 * KV), bf16) for n in shares],
            [pltpu.VMEM((n, 2, rows, tokens), bf16) for n in shares],
            [pltpu.VMEM((n_shard, 2, n, rows, cols), bf16) for n in shares],
            [pltpu.VMEM((n_shard, n, rows, cols), bf16) for n in shares],
            pltpu.VMEM((n_shard, members, rows, cols), bf16),
            pltpu.VMEM((members, rows, cols), bf16),
            pltpu.VMEM((n_shard - 1, members, rows, cols), bf16),
            [dma((3 * n_shard + 3,)) for _ in range(2)]
            + [dma((4,)) for _ in range(3)]
            + [dma((2,)), dma((2, n_shard)), dma((2,)), dma((n_shard - 1, 2))],
            dma(()),
            dma(()), dma(()),
            dma(()), dma((10,)),
            dma((members, 2)), dma((n_shard, 3)),
            dma(()), dma((n_shard - 1,)),
            dma((n_shard - 1,)), dma((n_shard - 1, 10)),
            dma(()), dma((members,)),
            dma(()), dma((10,)),
        ],
        compiler_params=params(48, has_side_effects=True, collective_id=0),
        name="muon",
    )(owners, bucket_starts, hbm(activations), hbm(cotangents), hbm(momentum))

    return pl.pallas_call(
        finish_kernel,
        out_shape=(
            jax.ShapeDtypeStruct(momentum.shape, f32),
            jax.ShapeDtypeStruct(momentum.shape, f32),
            jax.ShapeDtypeStruct((slots, KV, width), bf16),
        ),
        in_specs=[SMEM_SPEC] + [VMEM_SPEC] * 4,
        out_specs=(ANY_SPEC,) * 3,
        scratch_shapes=[
            pltpu.VMEM(momentum.shape, f32),
            pltpu.VMEM((slots, KV, width), bf16),
            dma(()), dma((MATS,)), dma((slots,)),
        ],
        compiler_params=params(20),
        name="finish",
    )(owners, mout, turned, wall, qall)


def solution(mesh):
    groups = mesh.shape["rep"] // 2
    slots = -(-MATS // mesh.shape["shard"]) + 1
    fits = mesh.shape["rep"] == 8 and mesh.shape["shard"] == 4 and slots <= groups
    placed = (
        P(None, ("rep", "shard"), None),
        P(None, ("rep", "shard"), None),
        P(None, None, "shard"),
        P(),
        P(),
    )
    return jax.shard_map(
        per_device_planes if fits else per_device_general,
        mesh=mesh,
        in_specs=placed,
        out_specs=(P(None, None, "shard"), P(None, None, "shard"), P("shard", None, None)),
        check_vma=False,
    )
```

```python
import functools
import math

import jax
import jax.numpy as jnp
from jax import lax
from jax.experimental import pallas as pl
from jax.experimental.pallas import tpu as pltpu
from jax.sharding import PartitionSpec as P

D = 2048
KV = 256
ITERS = 5
MATS = 12
MESH = pl.DeviceIdType.MESH
VMEM_SPEC = pl.BlockSpec(memory_space=pltpu.VMEM)
SMEM_SPEC = pl.BlockSpec(memory_space=pltpu.SMEM)
ANY_SPEC = pl.BlockSpec(memory_space=pl.ANY)
VMEM_LIMIT = 60 * 1024 * 1024

coef_a = 3.4445
coef_b = -4.775
coef_c = 2.0315
momentum_rate = 0.95
clip_level = 0.5
epsilon = 1e-06


def orthogonal_batch(matrices):
    values = matrices.astype(jnp.float32)
    frobenius = jnp.sqrt(jnp.sum(values * values, axis=(1, 2), keepdims=True))
    matrix = (values / (frobenius + epsilon)).astype(jnp.bfloat16)
    for iteration in range(ITERS):
        gram_matrix = jnp.einsum(
            "skd,sjd->skj", matrix, matrix, preferred_element_type=jnp.float32
        ).astype(jnp.bfloat16)
        square = jnp.einsum(
            "skj,sji->ski", gram_matrix, gram_matrix, preferred_element_type=jnp.float32
        )
        mixing = (coef_b * gram_matrix.astype(jnp.float32) + coef_c * square).astype(jnp.bfloat16)
        product = jnp.einsum("skj,sjd->skd", mixing, matrix, preferred_element_type=jnp.float32)
        matrix = (coef_a * matrix.astype(jnp.float32) + product).astype(jnp.bfloat16)
    return matrix


def clip_factors(square_sums, bucket_starts):
    indices = jnp.arange(MATS, dtype=jnp.int32)
    buckets = jnp.sum((indices[:, None] >= bucket_starts[None, :]).astype(jnp.int32), axis=1)
    together = (buckets[:, None] == buckets[None, :]).astype(jnp.float32)
    totals = jnp.sum(together * square_sums[None, :], axis=1)
    members = jnp.sum(together, axis=1)
    root_mean = jnp.sqrt(totals / (members * KV * D) + epsilon)
    return jnp.minimum(1.0, clip_level / root_mean)


def slot_numbers(owners):
    indices = jnp.arange(MATS, dtype=jnp.int32)
    earlier = (indices[None, :] < indices[:, None]) & (owners[None, :] == owners[:, None])
    return jnp.sum(earlier.astype(jnp.int32), axis=1)


def selector(owner_of, slot_of, shard_count, slot_count):
    holders = lax.broadcasted_iota(jnp.int32, (shard_count, slot_count, 1), 0)
    places = lax.broadcasted_iota(jnp.int32, (shard_count, slot_count, 1), 1)
    chosen = (holders == owner_of[None, None, :]) & (places == slot_of[None, None, :])
    return chosen.astype(jnp.bfloat16)


def pack_slots(shards, chooser):
    return jnp.einsum("psm,mkd->skpd", chooser, shards, preferred_element_type=jnp.float32).astype(
        jnp.bfloat16
    )


def unpack_slots(received, chooser):
    return jnp.einsum("psm,skpd->mkd", chooser, received, preferred_element_type=jnp.float32)


def per_device_general(activations, cotangents, momentum, owners, bucket_starts):
    shard_count = lax.axis_size("shard")
    replica_count = lax.axis_size("rep")
    layers, tok_rows, width = activations.shape
    token_total = tok_rows * shard_count * replica_count
    columns = width // shard_count
    slot_count = -(-MATS // shard_count) + 1
    update_scale = math.sqrt(max(KV, D))
    partial_terms = jnp.einsum(
        "ltk,ltd->lkd", cotangents, activations, preferred_element_type=jnp.float32
    ).reshape(MATS, KV, width)
    shard_part = lax.psum_scatter(
        partial_terms.astype(jnp.bfloat16), "shard", scatter_dimension=2, tiled=True
    )
    summed = lax.psum(shard_part, "rep").astype(jnp.float32)
    gradient = summed / jnp.sqrt(jnp.float32(token_total))
    square_sums = lax.psum(jnp.sum(gradient * gradient, axis=(1, 2)), "shard")
    factors = clip_factors(square_sums, bucket_starts)
    momentum_out = momentum_rate * momentum + factors[:, None, None] * gradient
    nesterov = (factors[:, None, None] * gradient + momentum_rate * momentum_out).astype(
        jnp.bfloat16
    )
    slot_of = slot_numbers(owners)
    chooser = selector(owners, slot_of, shard_count, slot_count)
    received = lax.all_to_all(
        pack_slots(nesterov, chooser), "shard", split_axis=2, concat_axis=2, tiled=True
    )
    item_count = received.shape[0]
    result = orthogonal_batch(received.reshape(item_count, KV, width))
    scaled = (update_scale * result.astype(jnp.float32)).astype(jnp.bfloat16)
    returned_part = lax.all_to_all(
        result.reshape(item_count, KV, shard_count, columns),
        "shard",
        split_axis=2,
        concat_axis=2,
        tiled=True,
    )
    update = update_scale * unpack_slots(returned_part, chooser)
    return (momentum_out, update, scaled)


def lodged(block, member):
    x = lax.rem(block, 2)
    y = lax.div(block, 2)
    whole = 2 * x + y
    paired = 4 + y
    return jnp.where(member < 2, whole, paired), jnp.where(member < 2, member, x)


def lodging(matrix):
    layer = lax.div(matrix, 2)
    side = lax.rem(matrix, 2)
    early = matrix < 8
    x = jnp.where(early, lax.div(layer, 2), side)
    y = jnp.where(early, lax.rem(layer, 2), layer - 4)
    return 2 * y + x, jnp.where(early, side, 2)


def place():
    me = lax.axis_index("rep")
    core = lax.rem(me, 2)
    x = lax.rem(lax.div(me, 2), 2)
    y = lax.div(me, 4)
    to_core = me + 1 - 2 * core
    to_x = me + 2 - 4 * x
    to_y = me + 4 - 8 * y
    to_xy = me + 6 - 4 * x - 8 * y
    return me, core, x, y, to_core, to_x, to_y, to_xy


def greet(peers):
    barrier = pltpu.get_barrier_semaphore()
    for peer in peers:
        pl.semaphore_signal(barrier, inc=1, device_id=peer, device_id_type=MESH)
    pl.semaphore_wait(barrier, len(peers))


def remote(src, dst, send, recv, peer):
    return pltpu.make_async_remote_copy(
        src_ref=src, dst_ref=dst, send_sem=send, recv_sem=recv, device_id=peer, device_id_type=MESH
    )


def plane_gather_start(z, at, send, recv):
    me, core, x, y, to_core, to_x, to_y, to_xy = place()
    plan = ((0, to_x, 0), (2, to_y, 1), (1, to_x, 1), (3, to_y, 0), (4, to_core, None))
    copies = {}
    for k, peer, half in plan:
        copies[k] = remote(at(me, half), at(me, half), send, recv.at[k], (peer, z))
        copies[k].start()
    return copies


def plane_gather_turn(z, at, send, recv, copies):
    me, core, x, y, to_core, to_x, to_y, to_xy = place()

    def forward(k, block, half, peer):
        copies[k] = remote(
            at(block, half), at(block, half), send, recv.at[k], (peer, z)
        )
        copies[k].start()

    copies[0].wait_recv()
    forward(5, to_x, 0, to_y)
    copies[2].wait_recv()
    forward(6, to_y, 1, to_x)
    copies[1].wait_recv()
    forward(7, to_x, None, to_core)
    copies[3].wait_recv()
    forward(8, to_y, None, to_core)


def plane_gather_finish(z, at, send, recv, copies, last=(4, 7, 8, 9)):
    me, core, x, y, to_core, to_x, to_y, to_xy = place()
    copies[5].wait_recv()
    copies[6].wait_recv()
    copies[9] = remote(
        at(to_xy, None), at(to_xy, None), send, recv.at[9], (to_core, z)
    )
    copies[9].start()
    for k in last:
        copies[k].wait_recv()


def drain(ref, semaphore):
    pltpu.make_async_copy(ref, ref, semaphore).wait()


def gather_reduce(
    n_shard, inverse, act_ref, cot_ref, gall, sqall, act, cot, turned, part, recv, plane, zrecv,
    in_sem, hop_r, swap_s, hop_s, pass_s, sum_s, sum_r, line_s, line_r,
):
    f32 = jnp.float32
    me, core, x, y, to_core, to_x, to_y, to_xy = place()
    z = lax.axis_index("shard")
    tokens = act_ref.shape[1]
    members, rows, cols = plane.shape[1:]
    near = z + 1 - 2 * lax.rem(z, 2)
    low = z < 2
    inner = (z == 1) | (z == 2)
    inward = jnp.where(low, z + 1, z - 1)
    targets = (jnp.where(low, 3, 0), jnp.where(low, 2, 1), near, z)
    cut = [pl.ds(pl.multiple_of(t * cols, cols), cols) for t in targets]
    counts = [c.shape[0] for c in cot]
    shared = counts[0] * 2
    mine = (counts[0] * x, shared + counts[1] * y)
    yours = (counts[0] * (1 - x), shared + counts[1] * (1 - y))
    peers = (to_x, to_y)
    layer_of = ((1 - y, y), (0,))
    keys = [(1, n_shard, 0), (0, n_shard, 0), (1, 0, 0), (0, 0, 0), (0, n_shard, 1), (0, 0, 1)]
    keys += [(kind, k, j) for k in range(1, n_shard) for kind, j in ((1, 0), (0, 0), (0, 1))]

    def index(kind, k, j):
        return 2 * k + j if kind == 0 else 2 * (n_shard + 1) + k

    def source(kind, k, layer):
        return cot_ref.at[layer] if k == n_shard else act_ref.at[layer, :, cut[k]]

    def slots(kind, k, j, first, count):
        layer = layer_of[kind][j]
        buffer = cot[kind].at[layer] if k == n_shard else act[kind].at[k, layer]
        return buffer.at[pl.ds(first * tokens, count * tokens)]

    own, swap, hop, onward = {}, {}, {}, {}
    for key in keys:
        kind, k, j = key
        at = in_sem.at[index(*key)]
        group = 2 * kind + (1 if k == n_shard else 0)
        layer = layer_of[kind][j]
        here = source(kind, k, mine[kind] + layer)
        own[key] = pltpu.make_async_copy(here, slots(*key, 0, 1), at)
        swap[key] = remote(here, slots(*key, 1, 1), swap_s.at[group], at, (to_core, z))
        hop[key] = remote(
            source(kind, k, yours[kind] + layer), slots(*key, 3, 1),
            hop_s.at[group], hop_r.at[index(*key)], (peers[kind], z),
        )
        onward[key] = remote(slots(*key, 3, 1), slots(*key, 2, 1), pass_s.at[group], at, (to_core, z))
    sums = [
        [
            remote(
                part[0].at[k, 1 - y], recv[0].at[k], sum_s.at[0], sum_r.at[0, k], (to_y, z)
            ),
            remote(
                part[1].at[k, 1 - x], recv[1].at[k], sum_s.at[1], sum_r.at[1, k], (to_x, z)
            ),
        ]
        for k in range(n_shard)
    ]
    spans = (pl.ds(0, members - 1), pl.ds(members - 1, 1))
    lines = [
        [
            remote(
                plane.at[k, spans[kind]],
                zrecv.at[k if k == 2 else k + 3 * inner.astype(jnp.int32), spans[kind]],
                line_s.at[kind],
                line_r.at[k if k == 2 else k + 3 * inner.astype(jnp.int32), kind],
                (me, near if k == 2 else inward),
            )
            for kind in range(2)
        ]
        for k in range(n_shard - 1)
    ]

    def arrived(s, kind):
        remote(
            plane.at[0, spans[kind]], zrecv.at[s, spans[kind]], line_s.at[kind], line_r.at[s, kind],
            (me, near),
        ).wait_recv()

    def enter():
        for key in keys:
            own[key].start()

    def send(kind, k):
        for j in range(counts[kind]):
            hop[kind, k, j].start()

    def begin():
        for key in keys[:6]:
            hop[key].start()
        send(1, 1)
        send(0, 1)
        for key in keys:
            swap[key].start()

    def take(kind, k, j=0):
        hop[kind, k, j].wait_recv()
        onward[kind, k, j].start()

    def ready(kind, k, j):
        drain(slots(kind, k, j, 0, 3), in_sem.at[index(kind, k, j)])

    def turn(kind, j=0):
        ready(kind, n_shard, j)
        layer = layer_of[kind][j]
        for side in range(2):
            at = pl.ds(pl.multiple_of((2 * side + core) * rows, rows), rows)
            turned[kind][layer, side] = cot[kind][layer, :, at].T

    def product(kind, k, j=0):
        ready(kind, k, j)
        layer = layer_of[kind][j]

        def one(side, carry):
            value = jnp.dot(turned[kind][layer, side], act[kind][k, layer], preferred_element_type=f32)
            if kind == 0:
                part[0][k, layer, side] = value.astype(part[0].dtype)
            else:
                part[1][k, side, 0] = value.astype(part[1].dtype)
            return carry

        lax.fori_loop(0, 2, one, 0)
        if j == 0:
            sums[k][kind].start()

    def gather(kind, k):
        sums[k][kind].wait_recv()
        for i in range(members - 1 if kind == 0 else 1):
            kept = part[0][k, y, i] if kind == 0 else part[1][k, x, i]
            value = kept.astype(f32) + recv[kind][k, i].astype(f32)
            plane[k, i if kind == 0 else members - 1] = value.astype(plane.dtype)

    def release(kind, k):
        @pl.when(jnp.logical_not(inner))
        def _():
            lines[k][kind].start()

    def forward(kind, k):
        s = 3 if k == 2 else k

        @pl.when(inner)
        def _():
            arrived(s, kind)
            for i in range(members - 1) if kind == 0 else (members - 1,):
                value = plane[k, i].astype(f32) + zrecv[s, i].astype(f32)
                plane[k, i] = value.astype(plane.dtype)
            lines[k][kind].start()

    def run():
        take(1, n_shard)
        take(0, n_shard, 0)
        turn(1)
        take(1, 0)
        take(0, 0, 0)
        turn(0, 0)
        product(1, 0)
        product(0, 0, 0)
        send(1, 2)
        take(1, 1)
        take(0, n_shard, 1)
        product(1, 1)
        send(0, 2)
        turn(0, 1)
        take(0, 0, 1)
        product(0, 0, 1)
        take(0, 1, 0)
        product(0, 1, 0)
        send(1, 3)
        gather(0, 0)
        release(0, 0)
        take(0, 1, 1)
        product(0, 1, 1)
        take(1, 2)
        product(1, 2)
        send(0, 3)
        gather(1, 0)
        release(1, 0)
        gather(0, 1)
        release(0, 1)
        gather(1, 1)
        release(1, 1)
        forward(0, 0)
        take(0, 2, 0)
        product(0, 2, 0)
        forward(1, 0)
        take(1, 3)
        product(1, 3)
        take(0, 2, 1)
        product(0, 2, 1)
        forward(0, 1)
        gather(1, 2)
        release(1, 2)
        gather(0, 2)
        release(0, 2)
        forward(1, 1)
        forward(0, 2)
        forward(1, 2)
        take(0, 3, 0)
        product(0, 3, 0)
        take(0, 3, 1)
        product(0, 3, 1)
        gather(1, 3)
        gather(0, 3)
        for kind in range(2):
            arrived(2, kind)
        home = lax.div(me, 2)
        half = pl.ds(pl.multiple_of(core * rows, rows), rows)

        def add_last(others, j):
            value = plane[n_shard - 1, j].astype(f32)
            for s in others:
                value = value + zrecv[s, j].astype(f32)
            value = (value * inverse).astype(gall.dtype)
            gall[home, j, half] = value
            value = value.astype(f32)
            line = jnp.sum(value * value, axis=0, keepdims=True)
            lanes = sqall.shape[-1]
            fold = line[:, :lanes]
            for i in range(1, cols // lanes):
                fold = fold + line[:, i * lanes : (i + 1) * lanes]
            sqall[me * n_shard + z, j] = fold

        @pl.when(inner)
        def _():
            for kind in range(2):
                arrived(4, kind)
            for j in range(members):
                add_last((2, 4), j)

        @pl.when(jnp.logical_not(inner))
        def _():
            for j in range(members):
                add_last((2,), j)

    def leave():
        for kind in range(2):
            for pool in (swap_s, hop_s, pass_s):
                drain(act[kind].at[:, :, pl.ds(0, tokens)], pool.at[2 * kind])
                drain(cot[kind].at[:, pl.ds(0, tokens)], pool.at[2 * kind + 1])
            drain(recv[kind], sum_s.at[kind])
            drain(plane.at[pl.ds(0, n_shard - 1), spans[kind]], line_s.at[kind])

    return enter, begin, run, leave


HOMES = ((1, 0), (2, 0), (2, 1))


def block_at(ref, axis, rows):
    def at(r, half):
        count = rows if half is None else rows // 2
        start = lax.rem(r, 2) * rows + (0 if half is None else half * count)
        cut = pl.ds(pl.multiple_of(start, count), count)
        block = lax.div(r, 2)
        return ref.at[block, cut] if axis == 1 else ref.at[block, :, cut]

    return at


def split(value):
    high = value.astype(jnp.bfloat16)
    return high, (value - high.astype(jnp.float32)).astype(jnp.bfloat16)


def times(left, right):
    dot = functools.partial(jnp.dot, preferred_element_type=jnp.float32)
    return dot(left[0], right[0]) + (dot(left[0], right[1]) + dot(left[1], right[0]))


def gram_iteration(gram, scale, gram_scr, root_scr):
    n = gram.shape[0]
    row = lax.broadcasted_iota(jnp.int32, (n, n), 0)
    col = lax.broadcasted_iota(jnp.int32, (n, n), 1)
    eye = (row == col).astype(jnp.float32)
    trace = jnp.sum(jnp.sum(gram * eye, axis=0, keepdims=True), axis=1, keepdims=True)
    inverse = 1.0 / (jnp.sqrt(trace) + epsilon)
    gram_scr[...] = gram * inverse * inverse
    for iteration in range(ITERS):
        a = split(gram_scr[...])
        mixing = coef_b * gram_scr[...] + coef_c * times(a, a)
        b = split(mixing)
        if iteration == 0:
            root_scr[...] = coef_a * eye + mixing
        else:
            root_scr[...] = coef_a * root_scr[...] + times(b, split(root_scr[...]))
        if iteration < ITERS - 1:
            half = coef_a * gram_scr[...] + times(b, a)
            gram_scr[...] = coef_a * half + times(b, split(half))
    return root_scr[...] * (inverse * scale)


def muon_kernel(
    n_shard, inverse, scale, owner_ref, start_ref, act_ref, cot_ref, momentum_hbm,
    mout_ref, u_ref, wall_ref, qall_ref,
    momentum, gall, sqall, table, factor, uown, held, gram_out, gram_in, gram_scr, root_scr, root,
    act, cot, turned, part, recv, plane, zrecv, reduce_sems,
    load, ps, pr, gs, gr, as_, ar, ws, wr, os_, or_, rs, rr, hs, hr,
):
    f32, bf16 = jnp.float32, jnp.bfloat16
    me, core, x, y, to_core, to_x, to_y, to_xy = place()
    z = lax.axis_index("shard")
    base = me - core
    block = lax.div(me, 2)
    members = gall.shape[1]
    rows, cols = held.shape[1:]
    lanes = sqall.shape[-1]
    mine = pl.ds(pl.multiple_of(core * rows, rows), rows)

    fetch = pltpu.make_async_copy(momentum_hbm, momentum, load)
    enter, begin, run, leave = gather_reduce(
        n_shard, inverse, act_ref, cot_ref, gall, sqall, act, cot, turned, part, recv,
        plane, zrecv, *reduce_sems,
    )
    enter()
    everyone = n_shard * 2 * gall.shape[0]
    here = me * n_shard + z
    others = [lax.rem(here + t, everyone) for t in range(1, everyone)]
    others = [(lax.div(to, n_shard), lax.rem(to, n_shard)) for to in others]
    greet(others)

    begin()
    fetch.start()
    run()

    for peer in others:
        remote(sqall.at[here], sqall.at[here], ps, pr, peer).start()
    at_g = block_at(gall, 2, rows)
    gathers = plane_gather_start(z, at_g, gs, gr)
    fetch.wait()
    drain(sqall.at[pl.ds(0, everyone - 1)], pr)

    table[...] = jnp.zeros_like(table)
    for m in range(MATS):
        layer, side = divmod(m, 2)
        bx, by = divmod(layer, 2) if m < 8 else (side, layer - 4)
        j, i = 2 * by + bx, side if m < 8 else 2
        line = sqall[2 * j * n_shard, i]
        for d in range(1, 2 * n_shard):
            line = line + sqall[2 * j * n_shard + d, i]
        table[pl.ds(m, 1)] = line
    index = lax.broadcasted_iota(jnp.int32, table.shape, 0)
    bucket = jnp.zeros(table.shape, jnp.int32)
    for k in range(start_ref.shape[0]):
        bucket = bucket + (index >= start_ref[k]).astype(jnp.int32)
    sums = table[...]
    clip = jnp.zeros(table.shape, f32)
    for k in range(start_ref.shape[0] + 1):
        inside = (bucket == k) & (index < MATS)
        total = jnp.sum(jnp.where(inside, sums, 0.0), axis=(0, 1), keepdims=True)
        count = jnp.sum(inside.astype(f32), axis=(0, 1), keepdims=True) / lanes
        mean = total / (jnp.maximum(count, 1.0) * (2 * rows) * (n_shard * cols))
        clip = jnp.where(inside, jnp.minimum(1.0, clip_level / jnp.sqrt(mean + epsilon)), clip)
    for m in range(MATS):
        factor[m] = jnp.concatenate([clip[m : m + 1, :]] * (cols // lanes), axis=1)

    def advance(matrix, gradient, past):
        step = factor[matrix] * gradient.astype(f32)
        new = momentum_rate * past + step
        return new, (step + momentum_rate * new).astype(bf16)

    gathers[4].wait_recv()
    for i in range(members):
        layer, side = lodged(block, i)
        matrix = 2 * layer + side
        uown[i] = advance(matrix, gall[block, i], momentum[matrix])[1]
    over = (((1,), (1,)), ((), ()))
    parts = []
    for i, (hz, hc) in enumerate(HOMES):
        here = (z == hz) & (core == hc)
        owner = (base + hc, hz)
        low = uown[i, :rows]
        high = uown[i, rows:]
        own = jnp.where(core == 0, low, high)
        diag = lax.dot_general(own, own, over, preferred_element_type=f32)
        gram_out[i, 0] = diag
        part = remote(gram_out.at[i, 0], gram_in.at[z, core], as_.at[i, 0], ar.at[z, core], owner)
        cross = remote(gram_out.at[i, 1], gram_in.at[z, 2], as_.at[i, 1], ar.at[z, 2], owner)
        parts.append((here, part, cross))

        @pl.when(here)
        def _():
            gram_in[z, core] = diag

        @pl.when(jnp.logical_not(here))
        def _():
            part.start()

        @pl.when(core == 0)
        def _():
            off = lax.dot_general(low, high, over, preferred_element_type=f32)
            gram_out[i, 1] = off

            @pl.when(here)
            def _():
                gram_in[z, 2] = off

            @pl.when(jnp.logical_not(here))
            def _():
                cross.start()

    plane_gather_turn(z, at_g, gs, gr, gathers)
    plane_gather_finish(z, at_g, gs, gr, gathers, last=(7, 8, 9))

    def slot_matrix(shard, slot):
        found = jnp.int32(0)
        count = jnp.int32(0)
        for m in range(MATS):
            yes = owner_ref[m] == shard
            found = jnp.where(yes & (count == slot), m, found)
            count = count + yes.astype(jnp.int32)
        return found

    sends = {}

    def send_slice(d):
        shard = lax.rem(z + d, n_shard)
        matrix = slot_matrix(shard, block)
        home, member = lodging(matrix)
        held[d - 1] = advance(matrix, gall[home, member, mine], momentum[matrix, mine])[1]
        sends[d] = remote(
            held.at[d - 1], wall_ref.at[n_shard - d - 1, block, mine], ws, wr.at[d - 1], (me, shard)
        )
        sends[d].start()

    send_slice(1)
    send_slice(3)

    def all_one(m, carry):
        home, member = lodging(m)
        new, turned = advance(m, gall[home, member], momentum[m])
        mout_ref[m] = new
        u_ref[m] = turned
        return carry

    is_home = functools.reduce(jnp.logical_or, [here for here, _, _ in parts])
    member = jnp.where(z == HOMES[0][0], 0, 1 + core)
    roots = []
    packed = root.shape[0] // 2
    mine_q = pl.ds(pl.multiple_of(core * packed, packed), packed)
    for d in range(n_shard):
        for c in range(2):
            if d == 0 and c == 1:
                continue
            peer = (to_core, z) if d == 0 else (base + c, lax.rem(z + d, n_shard))
            half = 1 - core if d == 0 else c
            cut = pl.ds(pl.multiple_of(half * packed, packed), packed)
            roots.append(remote(root.at[cut], qall_ref.at[block, member, cut], rs, rr.at[member], peer))

    @pl.when(is_home)
    def _():
        for d in range(n_shard):
            for k in range(3):
                source = remote(gram_out.at[0, 0], gram_in.at[d, k], as_.at[0, 0], ar.at[d, k], (to_core, z))
                local = (z == d) & ((core == k) if k < 2 else (core == 0))

                @pl.when(jnp.logical_not(local))
                def _():
                    source.wait_recv()

        blocks = []
        for k in range(3):
            value = gram_in[0, k]
            for d in range(1, n_shard):
                value = value + gram_in[d, k]
            blocks.append(value)
        top = jnp.concatenate([blocks[0], blocks[2]], axis=1)
        bottom = jnp.concatenate([blocks[2].T, blocks[1]], axis=1)
        result = gram_iteration(jnp.concatenate([top, bottom], axis=0), scale, gram_scr, root_scr)
        result = result.astype(bf16)
        root[:rows] = result[:rows, :rows]
        root[rows:packed] = result[: rows // 2, rows:]
        root[packed : packed + rows] = result[rows:, rows:]
        root[packed + rows :] = result[rows // 2 : rows, rows:]
        for c in roots:
            c.start()
        qall_ref[block, member, mine_q] = root[mine_q]

    walls = {}

    def at_w(d):
        return block_at(wall_ref.at[n_shard - d - 1], 1, rows)

    for d in (1, 3):
        sends[d].wait_recv()
        walls[d] = plane_gather_start(z, at_w(d), os_.at[d - 1], or_.at[d - 1])
    send_slice(2)
    lax.fori_loop(0, MATS, all_one, 0)
    for d in (1, 3):
        plane_gather_turn(z, at_w(d), os_.at[d - 1], or_.at[d - 1], walls[d])
    for i, (here, _, _) in enumerate(parts):
        arrival = remote(root.at[mine_q], qall_ref.at[block, i, mine_q], rs, rr.at[i], (to_core, z))

        @pl.when(jnp.logical_not(here))
        def _():
            arrival.wait_recv()

    at_q = block_at(qall_ref, 2, packed)
    gathers_q = plane_gather_start(z, at_q, hs, hr)
    sends[2].wait_recv()
    walls[2] = plane_gather_start(z, at_w(2), os_.at[1], or_.at[1])
    for d in (1, 3):
        plane_gather_finish(z, at_w(d), os_.at[d - 1], or_.at[d - 1], walls[d])
    plane_gather_turn(z, at_q, hs, hr, gathers_q)
    plane_gather_turn(z, at_w(2), os_.at[1], or_.at[1], walls[2])
    plane_gather_finish(z, at_q, hs, hr, gathers_q)
    plane_gather_finish(z, at_w(2), os_.at[1], or_.at[1], walls[2])
    most = pl.ds(0, 2 * rows - rows // 4)
    drain(gall.at[:, :, most], gs)
    drain(qall_ref.at[:, :, pl.ds(0, 2 * packed - packed // 4)], hs)
    for d in range(n_shard - 1):
        drain(wall_ref.at[d, :, most], os_.at[d])
    drain(held, ws)
    drain(sqall.at[pl.ds(0, everyone - 1)], ps)

    @pl.when(is_home)
    def _():
        drain(u_ref.at[pl.ds(0, len(roots)), pl.ds(0, packed * rows // cols)], rs)

    for here, part, cross in parts:

        @pl.when(jnp.logical_not(here))
        def _():
            part.wait_send()

            @pl.when(core == 0)
            def _():
                cross.wait_send()

    leave()


def finish_kernel(
    owner_ref, mout_ref, u_ref, wall_ref, qall_ref, mom_out, update_out, owned_out,
    ubuf, wbuf, qbuf, msem, usem, wsem,
):
    f32 = jnp.float32
    slots, _, width = wbuf.shape
    mats, _, cols = ubuf.shape
    n_shard = width // cols
    rows = qall_ref.shape[-1]
    z = lax.axis_index("shard")
    whole = pltpu.make_async_copy(mout_ref, mom_out, msem)
    whole.start()

    def put(buf, out, sem, m):
        return pltpu.make_async_copy(buf.at[m], out.at[m], sem.at[m])

    def update_one(m, carry):
        home, member = lodging(m)
        q = qall_ref[home, member]
        cross = jnp.concatenate([q[rows : 3 * rows // 2], q[5 * rows // 2 :]], axis=0)
        qbuf[m, :rows, :rows] = q[:rows]
        qbuf[m, :rows, rows:] = cross
        qbuf[m, rows:, :rows] = cross.T
        qbuf[m, rows:, rows:] = q[3 * rows // 2 : 5 * rows // 2]
        ubuf[m] = jnp.dot(qbuf[m], u_ref[m], preferred_element_type=f32)
        put(ubuf, update_out, usem, m).start()
        return carry

    lax.fori_loop(0, mats, update_one, 0)

    def owned_one(s, carry):
        matrix = jnp.int32(0)
        count = jnp.int32(0)
        for m in range(mats):
            yes = owner_ref[m] == z
            matrix = jnp.where(yes & (count == s), m, matrix)
            count = count + yes.astype(jnp.int32)
        keep = (count > s).astype(f32)
        q = qbuf[matrix]
        for d in range(n_shard):
            right = u_ref[matrix] if d == 0 else wall_ref[d - 1, s]
            value = jnp.dot(q, right, preferred_element_type=f32) * keep
            at = lax.rem(z + d, n_shard)
            wbuf[s, :, pl.ds(pl.multiple_of(at * cols, cols), cols)] = value.astype(wbuf.dtype)
        put(wbuf, owned_out, wsem, s).start()
        return carry

    lax.fori_loop(0, slots, owned_one, 0)

    def each(count, buf, out, sem):
        def step(m, carry):
            put(buf, out, sem, m).wait()
            return carry

        lax.fori_loop(0, count, step, 0)

    whole.wait()
    each(mats, ubuf, update_out, usem)
    each(slots, wbuf, owned_out, wsem)


def per_device_planes(activations, cotangents, momentum, owners, bucket_starts):
    n_shard = lax.axis_size("shard")
    n_rep = lax.axis_size("rep")
    layers, tok_rows, width = activations.shape
    token_total = tok_rows * n_shard * n_rep
    cols = width // n_shard
    rows = KV // 2
    lanes = math.gcd(cols, 128)
    groups = n_rep // 2
    members = MATS // groups
    slots = -(-MATS // n_shard) + 1
    update_scale = math.sqrt(max(KV, D))
    bf16, f32 = jnp.bfloat16, jnp.float32

    def params(limit, **rest):
        return pltpu.CompilerParams(vmem_limit_bytes=limit * 1024 * 1024, **rest)

    dma = pltpu.SemaphoreType.DMA
    tokens = 4 * tok_rows
    shares = (layers // 3, layers // 6)
    hbm = functools.partial(pltpu.with_memory_space_constraint, memory_space=pltpu.HBM)
    mout, turned, wall, qall = pl.pallas_call(
        functools.partial(muon_kernel, n_shard, 1.0 / math.sqrt(token_total), update_scale),
        out_shape=(
            pltpu.VMEM((MATS, KV, cols), f32),
            pltpu.VMEM((MATS, KV, cols), bf16),
            pltpu.VMEM((n_shard - 1, slots, KV, cols), bf16),
            pltpu.VMEM((groups, members, 3 * rows, rows), bf16),
        ),
        in_specs=[SMEM_SPEC, SMEM_SPEC, ANY_SPEC, ANY_SPEC, ANY_SPEC],
        out_specs=(VMEM_SPEC,) * 4,
        scratch_shapes=[
            pltpu.VMEM((MATS, KV, cols), f32),
            pltpu.VMEM((groups, members, KV, cols), bf16),
            pltpu.VMEM((n_rep * n_shard, members, 1, lanes), f32),
            pltpu.VMEM((16, lanes), f32),
            pltpu.VMEM((MATS, 1, cols), f32),
            pltpu.VMEM((members, KV, cols), bf16),
            pltpu.VMEM((n_shard - 1, rows, cols), bf16),
            pltpu.VMEM((members, 2, rows, rows), f32),
            pltpu.VMEM((n_shard, 3, rows, rows), f32),
            pltpu.VMEM((KV, KV), f32),
            pltpu.VMEM((KV, KV), f32),
            pltpu.VMEM((3 * rows, rows), bf16),
            [pltpu.VMEM((n_shard, n, tokens, cols), bf16) for n in shares],
            [pltpu.VMEM((n, tokens, 2 * KV), bf16) for n in shares],
            [pltpu.VMEM((n, 2, rows, tokens), bf16) for n in shares],
            [pltpu.VMEM((n_shard, 2, n, rows, cols), bf16) for n in shares],
            [pltpu.VMEM((n_shard, n, rows, cols), bf16) for n in shares],
            pltpu.VMEM((n_shard, members, rows, cols), bf16),
            pltpu.VMEM((n_shard + 1, members, rows, cols), bf16),
            [dma((3 * n_shard + 3,)) for _ in range(2)]
            + [dma((4,)) for _ in range(3)]
            + [dma((2,)), dma((2, n_shard)), dma((2,)), dma((n_shard + 1, 2))],
            dma(()),
            dma(()), dma(()),
            dma(()), dma((10,)),
            dma((members, 2)), dma((n_shard, 3)),
            dma(()), dma((n_shard - 1,)),
            dma((n_shard - 1,)), dma((n_shard - 1, 10)),
            dma(()), dma((members,)),
            dma(()), dma((10,)),
        ],
        compiler_params=params(48, has_side_effects=True, collective_id=0),
        name="muon",
    )(owners, bucket_starts, hbm(activations), hbm(cotangents), hbm(momentum))

    return pl.pallas_call(
        finish_kernel,
        out_shape=(
            jax.ShapeDtypeStruct(momentum.shape, f32),
            jax.ShapeDtypeStruct(momentum.shape, f32),
            jax.ShapeDtypeStruct((slots, KV, width), bf16),
        ),
        in_specs=[SMEM_SPEC] + [VMEM_SPEC] * 4,
        out_specs=(ANY_SPEC,) * 3,
        scratch_shapes=[
            pltpu.VMEM(momentum.shape, f32),
            pltpu.VMEM((slots, KV, width), bf16),
            pltpu.VMEM((MATS, KV, KV), bf16),
            dma(()), dma((MATS,)), dma((slots,)),
        ],
        compiler_params=params(20),
        name="finish",
    )(owners, mout, turned, wall, qall)


def solution(mesh):
    groups = mesh.shape["rep"] // 2
    slots = -(-MATS // mesh.shape["shard"]) + 1
    fits = mesh.shape["rep"] == 8 and mesh.shape["shard"] == 4 and slots <= groups
    placed = (
        P(None, ("rep", "shard"), None),
        P(None, ("rep", "shard"), None),
        P(None, None, "shard"),
        P(),
        P(),
    )
    return jax.shard_map(
        per_device_planes if fits else per_device_general,
        mesh=mesh,
        in_specs=placed,
        out_specs=(P(None, None, "shard"), P(None, None, "shard"), P("shard", None, None)),
        check_vma=False,
    )
```

```python
import functools
import math

import jax
import jax.numpy as jnp
from jax import lax
from jax.experimental import pallas as pl
from jax.experimental.pallas import tpu as pltpu
from jax.sharding import PartitionSpec as P

D = 2048
KV = 256
ITERS = 5
MATS = 12
MESH = pl.DeviceIdType.MESH
VMEM_SPEC = pl.BlockSpec(memory_space=pltpu.VMEM)
SMEM_SPEC = pl.BlockSpec(memory_space=pltpu.SMEM)
ANY_SPEC = pl.BlockSpec(memory_space=pl.ANY)
VMEM_LIMIT = 60 * 1024 * 1024

coef_a = 3.4445
coef_b = -4.775
coef_c = 2.0315
momentum_rate = 0.95
clip_level = 0.5
epsilon = 1e-06


def orthogonal_batch(matrices):
    values = matrices.astype(jnp.float32)
    frobenius = jnp.sqrt(jnp.sum(values * values, axis=(1, 2), keepdims=True))
    matrix = (values / (frobenius + epsilon)).astype(jnp.bfloat16)
    for iteration in range(ITERS):
        gram_matrix = jnp.einsum(
            "skd,sjd->skj", matrix, matrix, preferred_element_type=jnp.float32
        ).astype(jnp.bfloat16)
        square = jnp.einsum(
            "skj,sji->ski", gram_matrix, gram_matrix, preferred_element_type=jnp.float32
        )
        mixing = (coef_b * gram_matrix.astype(jnp.float32) + coef_c * square).astype(jnp.bfloat16)
        product = jnp.einsum("skj,sjd->skd", mixing, matrix, preferred_element_type=jnp.float32)
        matrix = (coef_a * matrix.astype(jnp.float32) + product).astype(jnp.bfloat16)
    return matrix


def clip_factors(square_sums, bucket_starts):
    indices = jnp.arange(MATS, dtype=jnp.int32)
    buckets = jnp.sum((indices[:, None] >= bucket_starts[None, :]).astype(jnp.int32), axis=1)
    together = (buckets[:, None] == buckets[None, :]).astype(jnp.float32)
    totals = jnp.sum(together * square_sums[None, :], axis=1)
    members = jnp.sum(together, axis=1)
    root_mean = jnp.sqrt(totals / (members * KV * D) + epsilon)
    return jnp.minimum(1.0, clip_level / root_mean)


def slot_numbers(owners):
    indices = jnp.arange(MATS, dtype=jnp.int32)
    earlier = (indices[None, :] < indices[:, None]) & (owners[None, :] == owners[:, None])
    return jnp.sum(earlier.astype(jnp.int32), axis=1)


def selector(owner_of, slot_of, shard_count, slot_count):
    holders = lax.broadcasted_iota(jnp.int32, (shard_count, slot_count, 1), 0)
    places = lax.broadcasted_iota(jnp.int32, (shard_count, slot_count, 1), 1)
    chosen = (holders == owner_of[None, None, :]) & (places == slot_of[None, None, :])
    return chosen.astype(jnp.bfloat16)


def pack_slots(shards, chooser):
    return jnp.einsum("psm,mkd->skpd", chooser, shards, preferred_element_type=jnp.float32).astype(
        jnp.bfloat16
    )


def unpack_slots(received, chooser):
    return jnp.einsum("psm,skpd->mkd", chooser, received, preferred_element_type=jnp.float32)


def per_device_general(activations, cotangents, momentum, owners, bucket_starts):
    shard_count = lax.axis_size("shard")
    replica_count = lax.axis_size("rep")
    layers, tok_rows, width = activations.shape
    token_total = tok_rows * shard_count * replica_count
    columns = width // shard_count
    slot_count = -(-MATS // shard_count) + 1
    update_scale = math.sqrt(max(KV, D))
    partial_terms = jnp.einsum(
        "ltk,ltd->lkd", cotangents, activations, preferred_element_type=jnp.float32
    ).reshape(MATS, KV, width)
    shard_part = lax.psum_scatter(
        partial_terms.astype(jnp.bfloat16), "shard", scatter_dimension=2, tiled=True
    )
    summed = lax.psum(shard_part, "rep").astype(jnp.float32)
    gradient = summed / jnp.sqrt(jnp.float32(token_total))
    square_sums = lax.psum(jnp.sum(gradient * gradient, axis=(1, 2)), "shard")
    factors = clip_factors(square_sums, bucket_starts)
    momentum_out = momentum_rate * momentum + factors[:, None, None] * gradient
    nesterov = (factors[:, None, None] * gradient + momentum_rate * momentum_out).astype(
        jnp.bfloat16
    )
    slot_of = slot_numbers(owners)
    chooser = selector(owners, slot_of, shard_count, slot_count)
    received = lax.all_to_all(
        pack_slots(nesterov, chooser), "shard", split_axis=2, concat_axis=2, tiled=True
    )
    item_count = received.shape[0]
    result = orthogonal_batch(received.reshape(item_count, KV, width))
    scaled = (update_scale * result.astype(jnp.float32)).astype(jnp.bfloat16)
    returned_part = lax.all_to_all(
        result.reshape(item_count, KV, shard_count, columns),
        "shard",
        split_axis=2,
        concat_axis=2,
        tiled=True,
    )
    update = update_scale * unpack_slots(returned_part, chooser)
    return (momentum_out, update, scaled)


def lodged(block, member):
    x = lax.rem(block, 2)
    y = lax.div(block, 2)
    whole = 2 * x + y
    paired = 4 + y
    return jnp.where(member < 2, whole, paired), jnp.where(member < 2, member, x)


def lodging(matrix):
    layer = lax.div(matrix, 2)
    side = lax.rem(matrix, 2)
    early = matrix < 8
    x = jnp.where(early, lax.div(layer, 2), side)
    y = jnp.where(early, lax.rem(layer, 2), layer - 4)
    return 2 * y + x, jnp.where(early, side, 2)


def place():
    me = lax.axis_index("rep")
    core = lax.rem(me, 2)
    x = lax.rem(lax.div(me, 2), 2)
    y = lax.div(me, 4)
    to_core = me + 1 - 2 * core
    to_x = me + 2 - 4 * x
    to_y = me + 4 - 8 * y
    to_xy = me + 6 - 4 * x - 8 * y
    return me, core, x, y, to_core, to_x, to_y, to_xy


def greet(peers, meanwhile):
    barrier = pltpu.get_barrier_semaphore()
    for peer in peers:
        pl.semaphore_signal(barrier, inc=1, device_id=peer, device_id_type=MESH)
    meanwhile()
    pl.semaphore_wait(barrier, len(peers))


def remote(src, dst, send, recv, peer):
    return pltpu.make_async_remote_copy(
        src_ref=src, dst_ref=dst, send_sem=send, recv_sem=recv, device_id=peer, device_id_type=MESH
    )


def plane_gather_start(z, at, send, recv):
    me, core, x, y, to_core, to_x, to_y, to_xy = place()
    plan = ((0, to_x, 0), (2, to_y, 1), (1, to_x, 1), (3, to_y, 0), (4, to_core, None))
    copies = {}
    for k, peer, half in plan:
        copies[k] = remote(at(me, half), at(me, half), send, recv.at[k], (peer, z))
        copies[k].start()
    return copies


def plane_gather_turn(z, at, send, recv, copies):
    me, core, x, y, to_core, to_x, to_y, to_xy = place()

    def forward(k, block, half, peer):
        copies[k] = remote(
            at(block, half), at(block, half), send, recv.at[k], (peer, z)
        )
        copies[k].start()

    copies[0].wait_recv()
    forward(5, to_x, 0, to_y)
    copies[2].wait_recv()
    forward(6, to_y, 1, to_x)
    copies[1].wait_recv()
    forward(7, to_x, None, to_core)
    copies[3].wait_recv()
    forward(8, to_y, None, to_core)


def plane_gather_finish(z, at, send, recv, copies, last=(4, 7, 8, 9)):
    me, core, x, y, to_core, to_x, to_y, to_xy = place()
    copies[5].wait_recv()
    copies[6].wait_recv()
    copies[9] = remote(
        at(to_xy, None), at(to_xy, None), send, recv.at[9], (to_core, z)
    )
    copies[9].start()
    for k in last:
        copies[k].wait_recv()


def drain(ref, semaphore):
    pltpu.make_async_copy(ref, ref, semaphore).wait()


def gather_reduce(
    n_shard, inverse, act_ref, cot_ref, gall, sqall, act, cot, turned, part, recv, plane, zrecv,
    in_sem, hop_r, swap_s, hop_s, pass_s, sum_s, sum_r, line_s, line_r,
):
    f32 = jnp.float32
    me, core, x, y, to_core, to_x, to_y, to_xy = place()
    z = lax.axis_index("shard")
    tokens = act_ref.shape[1]
    members, rows, cols = plane.shape[1:]
    near = z + 1 - 2 * lax.rem(z, 2)
    low = z < 2
    inner = (z == 1) | (z == 2)
    inward = jnp.where(low, z + 1, z - 1)
    targets = (jnp.where(low, 3, 0), jnp.where(low, 2, 1), near, z)
    cut = [pl.ds(pl.multiple_of(t * cols, cols), cols) for t in targets]
    counts = [c.shape[0] for c in cot]
    shared = counts[0] * 2
    mine = (counts[0] * x, shared + counts[1] * y)
    yours = (counts[0] * (1 - x), shared + counts[1] * (1 - y))
    peers = (to_x, to_y)
    layer_of = ((1 - y, y), (0,))
    keys = [(1, n_shard, 0), (0, n_shard, 0), (1, 0, 0), (0, 0, 0), (0, n_shard, 1), (0, 0, 1)]
    keys += [(kind, k, j) for k in range(1, n_shard) for kind, j in ((1, 0), (0, 0), (0, 1))]

    def index(kind, k, j):
        return 2 * k + j if kind == 0 else 2 * (n_shard + 1) + k

    def source(kind, k, layer):
        return cot_ref.at[layer] if k == n_shard else act_ref.at[layer, :, cut[k]]

    def slots(kind, k, j, first, count):
        layer = layer_of[kind][j]
        buffer = cot[kind].at[layer] if k == n_shard else act[kind].at[k, layer]
        return buffer.at[pl.ds(first * tokens, count * tokens)]

    own, swap, hop, onward = {}, {}, {}, {}
    for key in keys:
        kind, k, j = key
        at = in_sem.at[index(*key)]
        group = 2 * kind + (1 if k == n_shard else 0)
        layer = layer_of[kind][j]
        here = source(kind, k, mine[kind] + layer)
        own[key] = pltpu.make_async_copy(here, slots(*key, 0, 1), at)
        swap[key] = remote(here, slots(*key, 1, 1), swap_s.at[group], at, (to_core, z))
        hop[key] = remote(
            source(kind, k, yours[kind] + layer), slots(*key, 3, 1),
            hop_s.at[group], hop_r.at[index(*key)], (peers[kind], z),
        )
        onward[key] = remote(slots(*key, 3, 1), slots(*key, 2, 1), pass_s.at[group], at, (to_core, z))
    sums = [
        [
            remote(
                part[0].at[k, 1 - y], recv[0].at[k], sum_s.at[0], sum_r.at[0, k], (to_y, z)
            ),
            remote(
                part[1].at[k, 1 - x], recv[1].at[k], sum_s.at[1], sum_r.at[1, k], (to_x, z)
            ),
        ]
        for k in range(n_shard)
    ]
    spans = (pl.ds(0, members - 1), pl.ds(members - 1, 1))
    lines = [
        [
            remote(
                plane.at[k, spans[kind]],
                zrecv.at[k if k == 2 else k + 3 * inner.astype(jnp.int32), spans[kind]],
                line_s.at[kind],
                line_r.at[k if k == 2 else k + 3 * inner.astype(jnp.int32), kind],
                (me, near if k == 2 else inward),
            )
            for kind in range(2)
        ]
        for k in range(n_shard - 1)
    ]

    def arrived(s, kind):
        remote(
            plane.at[0, spans[kind]], zrecv.at[s, spans[kind]], line_s.at[kind], line_r.at[s, kind],
            (me, near),
        ).wait_recv()

    def enter():
        for key in keys:
            own[key].start()

    def begin():
        for key in keys[:9]:
            hop[key].start()
        for key in keys:
            swap[key].start()

    def take(kind, k, j=0):
        hop[kind, k, j].wait_recv()
        onward[kind, k, j].start()

    def ready(kind, k, j):
        drain(slots(kind, k, j, 0, 3), in_sem.at[index(kind, k, j)])

    def turn(kind, j=0):
        ready(kind, n_shard, j)
        layer = layer_of[kind][j]
        for side in range(2):
            at = pl.ds(pl.multiple_of((2 * side + core) * rows, rows), rows)
            turned[kind][layer, side] = cot[kind][layer, :, at].T

    def product(kind, k, j=0):
        ready(kind, k, j)
        layer = layer_of[kind][j]

        def one(side, carry):
            value = jnp.dot(turned[kind][layer, side], act[kind][k, layer], preferred_element_type=f32)
            if kind == 0:
                part[0][k, layer, side] = value.astype(part[0].dtype)
            else:
                part[1][k, side, 0] = value.astype(part[1].dtype)
            return carry

        lax.fori_loop(0, 2, one, 0)
        if j == 0:
            sums[k][kind].start()

    def gather(kind, k):
        sums[k][kind].wait_recv()
        for i in range(members - 1 if kind == 0 else 1):
            kept = part[0][k, y, i] if kind == 0 else part[1][k, x, i]
            value = kept.astype(f32) + recv[kind][k, i].astype(f32)
            plane[k, i if kind == 0 else members - 1] = value.astype(plane.dtype)

    def release(kind, k):
        @pl.when(jnp.logical_not(inner))
        def _():
            lines[k][kind].start()

    def forward(kind, k):
        s = 3 if k == 2 else k

        @pl.when(inner)
        def _():
            arrived(s, kind)
            for i in range(members - 1) if kind == 0 else (members - 1,):
                value = plane[k, i].astype(f32) + zrecv[s, i].astype(f32)
                plane[k, i] = value.astype(plane.dtype)
            lines[k][kind].start()

    def run():
        take(1, n_shard)
        take(0, n_shard, 0)
        turn(1)
        take(1, 0)
        take(0, 0, 0)
        turn(0, 0)
        product(1, 0)
        hop[0, 2, 0].start()
        product(0, 0, 0)
        hop[1, 2, 0].start()
        take(1, 1)
        take(0, n_shard, 1)
        product(1, 1)
        hop[0, 2, 1].start()
        hop[0, 3, 0].start()
        turn(0, 1)
        take(0, 0, 1)
        product(0, 0, 1)
        take(0, 1, 0)
        product(0, 1, 0)
        hop[1, 3, 0].start()
        gather(0, 0)
        release(0, 0)
        take(0, 1, 1)
        product(0, 1, 1)
        take(1, 2)
        product(1, 2)
        hop[0, 3, 1].start()
        gather(1, 0)
        release(1, 0)
        take(0, 2, 0)
        product(0, 2, 0)
        gather(0, 1)
        release(0, 1)
        forward(0, 0)
        gather(1, 1)
        release(1, 1)
        forward(1, 0)
        take(1, 3)
        product(1, 3)
        take(0, 2, 1)
        product(0, 2, 1)
        take(0, 3, 0)
        product(0, 3, 0)
        gather(0, 2)
        release(0, 2)
        forward(0, 1)
        forward(0, 2)
        gather(1, 2)
        release(1, 2)
        forward(1, 1)
        forward(1, 2)
        take(0, 3, 1)
        product(0, 3, 1)
        gather(1, 3)
        gather(0, 3)
        for kind in range(2):
            arrived(2, kind)
        home = lax.div(me, 2)
        half = pl.ds(pl.multiple_of(core * rows, rows), rows)

        def add_last(others, j):
            value = plane[n_shard - 1, j].astype(f32)
            for s in others:
                value = value + zrecv[s, j].astype(f32)
            value = (value * inverse).astype(gall.dtype)
            gall[home, j, half] = value
            value = value.astype(f32)
            line = jnp.sum(value * value, axis=0, keepdims=True)
            lanes = sqall.shape[-1]
            fold = line[:, :lanes]
            for i in range(1, cols // lanes):
                fold = fold + line[:, i * lanes : (i + 1) * lanes]
            sqall[me * n_shard + z, j] = fold

        @pl.when(inner)
        def _():
            for kind in range(2):
                arrived(4, kind)
            for j in range(members):
                add_last((2, 4), j)

        @pl.when(jnp.logical_not(inner))
        def _():
            for j in range(members):
                add_last((2,), j)

    def leave():
        for kind in range(2):
            for pool in (swap_s, hop_s, pass_s):
                drain(act[kind].at[:, :, pl.ds(0, tokens)], pool.at[2 * kind])
                drain(cot[kind].at[:, pl.ds(0, tokens)], pool.at[2 * kind + 1])
            drain(recv[kind], sum_s.at[kind])
            drain(plane.at[pl.ds(0, n_shard - 1), spans[kind]], line_s.at[kind])

    return enter, begin, run, leave


HOMES = ((1, 0), (2, 0), (2, 1))


def block_at(ref, axis, rows):
    def at(r, half):
        count = rows if half is None else rows // 2
        start = lax.rem(r, 2) * rows + (0 if half is None else half * count)
        cut = pl.ds(pl.multiple_of(start, count), count)
        block = lax.div(r, 2)
        return ref.at[block, cut] if axis == 1 else ref.at[block, :, cut]

    return at


def split(value):
    high = value.astype(jnp.bfloat16)
    return high, (value - high.astype(jnp.float32)).astype(jnp.bfloat16)


def times(left, right):
    dot = functools.partial(jnp.dot, preferred_element_type=jnp.float32)
    return dot(left[0], right[0]) + (dot(left[0], right[1]) + dot(left[1], right[0]))


def gram_iteration(gram, scale, gram_scr, root_scr):
    n = gram.shape[0]
    row = lax.broadcasted_iota(jnp.int32, (n, n), 0)
    col = lax.broadcasted_iota(jnp.int32, (n, n), 1)
    eye = (row == col).astype(jnp.float32)
    trace = jnp.sum(jnp.sum(gram * eye, axis=0, keepdims=True), axis=1, keepdims=True)
    inverse = 1.0 / (jnp.sqrt(trace) + epsilon)
    gram_scr[...] = gram * inverse * inverse
    for iteration in range(ITERS):
        a = split(gram_scr[...])
        mixing = coef_b * gram_scr[...] + coef_c * times(a, a)
        b = split(mixing)
        if iteration == 0:
            root_scr[...] = coef_a * eye + mixing
        else:
            root_scr[...] = coef_a * root_scr[...] + times(b, split(root_scr[...]))
        if iteration < ITERS - 1:
            half = coef_a * gram_scr[...] + times(b, a)
            gram_scr[...] = coef_a * half + times(b, split(half))
    return root_scr[...] * (inverse * scale)


def muon_kernel(
    n_shard, inverse, scale, owner_ref, start_ref, act_ref, cot_ref, momentum_hbm,
    mout_ref, u_ref, wall_ref, qall_ref,
    momentum, gall, sqall, table, factor, uown, held, gram_out, gram_in, gram_scr, root_scr, root,
    act, cot, turned, part, recv, plane, zrecv, reduce_sems,
    load, ps, pr, gs, gr, as_, ar, ws, wr, os_, or_, rs, rr, hs, hr,
):
    f32, bf16 = jnp.float32, jnp.bfloat16
    me, core, x, y, to_core, to_x, to_y, to_xy = place()
    z = lax.axis_index("shard")
    base = me - core
    block = lax.div(me, 2)
    members = gall.shape[1]
    rows, cols = held.shape[1:]
    lanes = sqall.shape[-1]
    mine = pl.ds(pl.multiple_of(core * rows, rows), rows)

    fetch = pltpu.make_async_copy(momentum_hbm, momentum, load)
    enter, begin, run, leave = gather_reduce(
        n_shard, inverse, act_ref, cot_ref, gall, sqall, act, cot, turned, part, recv,
        plane, zrecv, *reduce_sems,
    )
    everyone = n_shard * 2 * gall.shape[0]
    here = me * n_shard + z
    others = [lax.rem(here + t, everyone) for t in range(1, everyone)]
    others = [(lax.div(to, n_shard), lax.rem(to, n_shard)) for to in others]
    greet(others, enter)

    begin()
    fetch.start()
    run()

    for peer in others:
        remote(sqall.at[here], sqall.at[here], ps, pr, peer).start()
    at_g = block_at(gall, 2, rows)
    gathers = plane_gather_start(z, at_g, gs, gr)
    fetch.wait()
    drain(sqall.at[pl.ds(0, everyone - 1)], pr)

    table[...] = jnp.zeros_like(table)
    for m in range(MATS):
        layer, side = divmod(m, 2)
        bx, by = divmod(layer, 2) if m < 8 else (side, layer - 4)
        j, i = 2 * by + bx, side if m < 8 else 2
        line = sqall[2 * j * n_shard, i]
        for d in range(1, 2 * n_shard):
            line = line + sqall[2 * j * n_shard + d, i]
        table[pl.ds(m, 1)] = line
    index = lax.broadcasted_iota(jnp.int32, table.shape, 0)
    bucket = jnp.zeros(table.shape, jnp.int32)
    for k in range(start_ref.shape[0]):
        bucket = bucket + (index >= start_ref[k]).astype(jnp.int32)
    sums = table[...]
    clip = jnp.zeros(table.shape, f32)
    for k in range(start_ref.shape[0] + 1):
        inside = (bucket == k) & (index < MATS)
        total = jnp.sum(jnp.where(inside, sums, 0.0), axis=(0, 1), keepdims=True)
        count = jnp.sum(inside.astype(f32), axis=(0, 1), keepdims=True) / lanes
        mean = total / (jnp.maximum(count, 1.0) * (2 * rows) * (n_shard * cols))
        clip = jnp.where(inside, jnp.minimum(1.0, clip_level / jnp.sqrt(mean + epsilon)), clip)
    for m in range(MATS):
        factor[m] = jnp.concatenate([clip[m : m + 1, :]] * (cols // lanes), axis=1)

    def advance(matrix, gradient, past):
        step = factor[matrix] * gradient.astype(f32)
        new = momentum_rate * past + step
        return new, (step + momentum_rate * new).astype(bf16)

    gathers[4].wait_recv()
    for i in range(members):
        layer, side = lodged(block, i)
        matrix = 2 * layer + side
        uown[i] = advance(matrix, gall[block, i], momentum[matrix])[1]
    over = (((1,), (1,)), ((), ()))
    parts = []
    for i, (hz, hc) in enumerate(HOMES):
        here = (z == hz) & (core == hc)
        owner = (base + hc, hz)
        low = uown[i, :rows]
        high = uown[i, rows:]
        own = jnp.where(core == 0, low, high)
        diag = lax.dot_general(own, own, over, preferred_element_type=f32)
        gram_out[i, 0] = diag
        part = remote(gram_out.at[i, 0], gram_in.at[z, core], as_.at[i, 0], ar.at[z, core], owner)
        cross = remote(gram_out.at[i, 1], gram_in.at[z, 2], as_.at[i, 1], ar.at[z, 2], owner)
        parts.append((here, part, cross))

        @pl.when(here)
        def _():
            gram_in[z, core] = diag

        @pl.when(jnp.logical_not(here))
        def _():
            part.start()

        @pl.when(core == 0)
        def _():
            off = lax.dot_general(low, high, over, preferred_element_type=f32)
            gram_out[i, 1] = off

            @pl.when(here)
            def _():
                gram_in[z, 2] = off

            @pl.when(jnp.logical_not(here))
            def _():
                cross.start()

    plane_gather_turn(z, at_g, gs, gr, gathers)
    plane_gather_finish(z, at_g, gs, gr, gathers, last=(7, 8, 9))

    def slot_matrix(shard, slot):
        found = jnp.int32(0)
        count = jnp.int32(0)
        for m in range(MATS):
            yes = owner_ref[m] == shard
            found = jnp.where(yes & (count == slot), m, found)
            count = count + yes.astype(jnp.int32)
        return found

    partners = {
        1: z + 1 - 2 * lax.rem(z, 2),
        2: z + 2 - 4 * lax.div(z, 2),
        3: n_shard - 1 - z,
    }
    sends = {}
    walls = {}
    for e in (1, 3, 2):
        matrix = slot_matrix(partners[e], block)
        home, member = lodging(matrix)
        held[e - 1] = advance(matrix, gall[home, member, mine], momentum[matrix, mine])[1]
        sends[e] = remote(
            held.at[e - 1], wall_ref.at[e - 1, block, mine], ws, wr.at[e - 1], (me, partners[e])
        )
        sends[e].start()

    def all_one(m, carry):
        home, member = lodging(m)
        new, turned = advance(m, gall[home, member], momentum[m])
        mout_ref[m] = new
        u_ref[m] = turned
        return carry

    def wall_at(e):
        return block_at(wall_ref.at[e - 1], 1, rows)

    def wall_start(e):
        sends[e].wait_recv()
        walls[e] = plane_gather_start(z, wall_at(e), os_.at[e - 1], or_.at[e - 1])

    def wall_turn(e):
        plane_gather_turn(z, wall_at(e), os_.at[e - 1], or_.at[e - 1], walls[e])

    def wall_finish(e):
        plane_gather_finish(z, wall_at(e), os_.at[e - 1], or_.at[e - 1], walls[e])

    is_home = functools.reduce(jnp.logical_or, [here for here, _, _ in parts])
    member = jnp.where(z == HOMES[0][0], 0, 1 + core)
    roots = []
    packed = root.shape[0] // 2
    mine_q = pl.ds(pl.multiple_of(core * packed, packed), packed)
    for d in range(n_shard):
        for c in range(2):
            if d == 0 and c == 1:
                continue
            peer = (to_core, z) if d == 0 else (base + c, lax.rem(z + d, n_shard))
            half = 1 - core if d == 0 else c
            cut = pl.ds(pl.multiple_of(half * packed, packed), packed)
            roots.append(remote(root.at[cut], qall_ref.at[block, member, cut], rs, rr.at[member], peer))

    @pl.when(jnp.logical_not(is_home))
    def _():
        lax.fori_loop(0, MATS, all_one, 0)

    wall_start(1)

    @pl.when(is_home)
    def _():
        for d in range(n_shard):
            for k in range(3):
                source = remote(gram_out.at[0, 0], gram_in.at[d, k], as_.at[0, 0], ar.at[d, k], (to_core, z))
                local = (z == d) & ((core == k) if k < 2 else (core == 0))

                @pl.when(jnp.logical_not(local))
                def _():
                    source.wait_recv()

        blocks = []
        for k in range(3):
            value = gram_in[0, k]
            for d in range(1, n_shard):
                value = value + gram_in[d, k]
            blocks.append(value)
        top = jnp.concatenate([blocks[0], blocks[2]], axis=1)
        bottom = jnp.concatenate([blocks[2].T, blocks[1]], axis=1)
        result = gram_iteration(jnp.concatenate([top, bottom], axis=0), scale, gram_scr, root_scr)
        result = result.astype(bf16)
        root[:rows] = result[:rows, :rows]
        root[rows:packed] = result[: rows // 2, rows:]
        root[packed : packed + rows] = result[rows:, rows:]
        root[packed + rows :] = result[rows // 2 : rows, rows:]
        for c in roots:
            c.start()
        qall_ref[block, member, mine_q] = root[mine_q]

    wall_start(3)
    wall_turn(1)

    @pl.when(is_home)
    def _():
        lax.fori_loop(0, MATS, all_one, 0)

    wall_start(2)
    wall_turn(3)
    wall_finish(1)
    wall_turn(2)
    for i, (here, _, _) in enumerate(parts):
        arrival = remote(root.at[mine_q], qall_ref.at[block, i, mine_q], rs, rr.at[i], (to_core, z))

        @pl.when(jnp.logical_not(here))
        def _():
            arrival.wait_recv()

    at_q = block_at(qall_ref, 2, packed)
    gathers_q = plane_gather_start(z, at_q, hs, hr)
    wall_finish(3)
    wall_finish(2)
    plane_gather_turn(z, at_q, hs, hr, gathers_q)
    plane_gather_finish(z, at_q, hs, hr, gathers_q)
    most = pl.ds(0, 2 * rows - rows // 4)
    drain(gall.at[:, :, most], gs)
    drain(qall_ref.at[:, :, pl.ds(0, 2 * packed - packed // 4)], hs)
    for d in range(n_shard - 1):
        drain(wall_ref.at[d, :, most], os_.at[d])
    drain(held, ws)
    drain(sqall.at[pl.ds(0, everyone - 1)], ps)

    @pl.when(is_home)
    def _():
        drain(u_ref.at[pl.ds(0, len(roots)), pl.ds(0, packed * rows // cols)], rs)

    for here, part, cross in parts:

        @pl.when(jnp.logical_not(here))
        def _():
            part.wait_send()

            @pl.when(core == 0)
            def _():
                cross.wait_send()

    leave()


def finish_kernel(
    owner_ref, mout_ref, u_ref, wall_ref, qall_ref, mom_out, update_out, owned_out,
    ubuf, wbuf, qbuf, msem, usem, wsem,
):
    f32 = jnp.float32
    slots, _, width = wbuf.shape
    mats, _, cols = ubuf.shape
    n_shard = width // cols
    rows = qall_ref.shape[-1]
    z = lax.axis_index("shard")
    whole = pltpu.make_async_copy(mout_ref, mom_out, msem)
    whole.start()

    def put(buf, out, sem, m):
        return pltpu.make_async_copy(buf.at[m], out.at[m], sem.at[m])

    def update_one(m, carry):
        home, member = lodging(m)
        q = qall_ref[home, member]
        cross = jnp.concatenate([q[rows : 3 * rows // 2], q[5 * rows // 2 :]], axis=0)
        qbuf[m, :rows, :rows] = q[:rows]
        qbuf[m, :rows, rows:] = cross
        qbuf[m, rows:, :rows] = cross.T
        qbuf[m, rows:, rows:] = q[3 * rows // 2 : 5 * rows // 2]
        ubuf[m] = jnp.dot(qbuf[m], u_ref[m], preferred_element_type=f32)
        put(ubuf, update_out, usem, m).start()
        return carry

    lax.fori_loop(0, mats, update_one, 0)

    def owned_one(s, carry):
        matrix = jnp.int32(0)
        count = jnp.int32(0)
        for m in range(mats):
            yes = owner_ref[m] == z
            matrix = jnp.where(yes & (count == s), m, matrix)
            count = count + yes.astype(jnp.int32)
        keep = (count > s).astype(f32)
        q = qbuf[matrix]
        for d in range(n_shard):
            right = u_ref[matrix] if d == 0 else wall_ref[d - 1, s]
            value = jnp.dot(q, right, preferred_element_type=f32) * keep
            at = (z, z + 1 - 2 * lax.rem(z, 2), z + 2 - 4 * lax.div(z, 2), n_shard - 1 - z)[d]
            wbuf[s, :, pl.ds(pl.multiple_of(at * cols, cols), cols)] = value.astype(wbuf.dtype)
        put(wbuf, owned_out, wsem, s).start()
        return carry

    lax.fori_loop(0, slots, owned_one, 0)

    def each(count, buf, out, sem):
        def step(m, carry):
            put(buf, out, sem, m).wait()
            return carry

        lax.fori_loop(0, count, step, 0)

    whole.wait()
    each(mats, ubuf, update_out, usem)
    each(slots, wbuf, owned_out, wsem)


def per_device_planes(activations, cotangents, momentum, owners, bucket_starts):
    n_shard = lax.axis_size("shard")
    n_rep = lax.axis_size("rep")
    layers, tok_rows, width = activations.shape
    token_total = tok_rows * n_shard * n_rep
    cols = width // n_shard
    rows = KV // 2
    lanes = math.gcd(cols, 128)
    groups = n_rep // 2
    members = MATS // groups
    slots = -(-MATS // n_shard) + 1
    update_scale = math.sqrt(max(KV, D))
    bf16, f32 = jnp.bfloat16, jnp.float32

    def params(limit, **rest):
        return pltpu.CompilerParams(vmem_limit_bytes=limit * 1024 * 1024, **rest)

    dma = pltpu.SemaphoreType.DMA
    tokens = 4 * tok_rows
    shares = (layers // 3, layers // 6)
    hbm = functools.partial(pltpu.with_memory_space_constraint, memory_space=pltpu.HBM)
    mout, turned, wall, qall = pl.pallas_call(
        functools.partial(muon_kernel, n_shard, 1.0 / math.sqrt(token_total), update_scale),
        out_shape=(
            pltpu.VMEM((MATS, KV, cols), f32),
            pltpu.VMEM((MATS, KV, cols), bf16),
            pltpu.VMEM((n_shard - 1, slots, KV, cols), bf16),
            pltpu.VMEM((groups, members, 3 * rows, rows), bf16),
        ),
        in_specs=[SMEM_SPEC, SMEM_SPEC, ANY_SPEC, ANY_SPEC, ANY_SPEC],
        out_specs=(VMEM_SPEC,) * 4,
        scratch_shapes=[
            pltpu.VMEM((MATS, KV, cols), f32),
            pltpu.VMEM((groups, members, KV, cols), bf16),
            pltpu.VMEM((n_rep * n_shard, members, 1, lanes), f32),
            pltpu.VMEM((16, lanes), f32),
            pltpu.VMEM((MATS, 1, cols), f32),
            pltpu.VMEM((members, KV, cols), bf16),
            pltpu.VMEM((n_shard - 1, rows, cols), bf16),
            pltpu.VMEM((members, 2, rows, rows), f32),
            pltpu.VMEM((n_shard, 3, rows, rows), f32),
            pltpu.VMEM((KV, KV), f32),
            pltpu.VMEM((KV, KV), f32),
            pltpu.VMEM((3 * rows, rows), bf16),
            [pltpu.VMEM((n_shard, n, tokens, cols), bf16) for n in shares],
            [pltpu.VMEM((n, tokens, 2 * KV), bf16) for n in shares],
            [pltpu.VMEM((n, 2, rows, tokens), bf16) for n in shares],
            [pltpu.VMEM((n_shard, 2, n, rows, cols), bf16) for n in shares],
            [pltpu.VMEM((n_shard, n, rows, cols), bf16) for n in shares],
            pltpu.VMEM((n_shard, members, rows, cols), bf16),
            pltpu.VMEM((n_shard + 1, members, rows, cols), bf16),
            [dma((3 * n_shard + 3,)) for _ in range(2)]
            + [dma((4,)) for _ in range(3)]
            + [dma((2,)), dma((2, n_shard)), dma((2,)), dma((n_shard + 1, 2))],
            dma(()),
            dma(()), dma(()),
            dma(()), dma((10,)),
            dma((members, 2)), dma((n_shard, 3)),
            dma(()), dma((n_shard - 1,)),
            dma((n_shard - 1,)), dma((n_shard - 1, 10)),
            dma(()), dma((members,)),
            dma(()), dma((10,)),
        ],
        compiler_params=params(48, has_side_effects=True, collective_id=0),
        name="muon",
    )(owners, bucket_starts, hbm(activations), hbm(cotangents), hbm(momentum))

    return pl.pallas_call(
        finish_kernel,
        out_shape=(
            jax.ShapeDtypeStruct(momentum.shape, f32),
            jax.ShapeDtypeStruct(momentum.shape, f32),
            jax.ShapeDtypeStruct((slots, KV, width), bf16),
        ),
        in_specs=[SMEM_SPEC] + [VMEM_SPEC] * 4,
        out_specs=(ANY_SPEC,) * 3,
        scratch_shapes=[
            pltpu.VMEM(momentum.shape, f32),
            pltpu.VMEM((slots, KV, width), bf16),
            pltpu.VMEM((MATS, KV, KV), bf16),
            dma(()), dma((MATS,)), dma((slots,)),
        ],
        compiler_params=params(20),
        name="finish",
    )(owners, mout, turned, wall, qall)


def solution(mesh):
    groups = mesh.shape["rep"] // 2
    slots = -(-MATS // mesh.shape["shard"]) + 1
    fits = mesh.shape["rep"] == 8 and mesh.shape["shard"] == 4 and slots <= groups
    placed = (
        P(None, ("rep", "shard"), None),
        P(None, ("rep", "shard"), None),
        P(None, None, "shard"),
        P(),
        P(),
    )
    return jax.shard_map(
        per_device_planes if fits else per_device_general,
        mesh=mesh,
        in_specs=placed,
        out_specs=(P(None, None, "shard"), P(None, None, "shard"), P("shard", None, None)),
        check_vma=False,
    )
```

```python
import functools
import math

import jax
import jax.numpy as jnp
from jax import lax
from jax.experimental import pallas as pl
from jax.experimental.pallas import tpu as pltpu
from jax.sharding import PartitionSpec as P

D = 2048
KV = 256
ITERS = 5
MATS = 12
MESH = pl.DeviceIdType.MESH
VMEM_SPEC = pl.BlockSpec(memory_space=pltpu.VMEM)
SMEM_SPEC = pl.BlockSpec(memory_space=pltpu.SMEM)
ANY_SPEC = pl.BlockSpec(memory_space=pl.ANY)
VMEM_LIMIT = 60 * 1024 * 1024

coef_a = 3.4445
coef_b = -4.775
coef_c = 2.0315
momentum_rate = 0.95
clip_level = 0.5
epsilon = 1e-06


def orthogonal_batch(matrices):
    values = matrices.astype(jnp.float32)
    frobenius = jnp.sqrt(jnp.sum(values * values, axis=(1, 2), keepdims=True))
    matrix = (values / (frobenius + epsilon)).astype(jnp.bfloat16)
    for iteration in range(ITERS):
        gram_matrix = jnp.einsum(
            "skd,sjd->skj", matrix, matrix, preferred_element_type=jnp.float32
        ).astype(jnp.bfloat16)
        square = jnp.einsum(
            "skj,sji->ski", gram_matrix, gram_matrix, preferred_element_type=jnp.float32
        )
        mixing = (coef_b * gram_matrix.astype(jnp.float32) + coef_c * square).astype(jnp.bfloat16)
        product = jnp.einsum("skj,sjd->skd", mixing, matrix, preferred_element_type=jnp.float32)
        matrix = (coef_a * matrix.astype(jnp.float32) + product).astype(jnp.bfloat16)
    return matrix


def clip_factors(square_sums, bucket_starts):
    indices = jnp.arange(MATS, dtype=jnp.int32)
    buckets = jnp.sum((indices[:, None] >= bucket_starts[None, :]).astype(jnp.int32), axis=1)
    together = (buckets[:, None] == buckets[None, :]).astype(jnp.float32)
    totals = jnp.sum(together * square_sums[None, :], axis=1)
    members = jnp.sum(together, axis=1)
    root_mean = jnp.sqrt(totals / (members * KV * D) + epsilon)
    return jnp.minimum(1.0, clip_level / root_mean)


def slot_numbers(owners):
    indices = jnp.arange(MATS, dtype=jnp.int32)
    earlier = (indices[None, :] < indices[:, None]) & (owners[None, :] == owners[:, None])
    return jnp.sum(earlier.astype(jnp.int32), axis=1)


def selector(owner_of, slot_of, shard_count, slot_count):
    holders = lax.broadcasted_iota(jnp.int32, (shard_count, slot_count, 1), 0)
    places = lax.broadcasted_iota(jnp.int32, (shard_count, slot_count, 1), 1)
    chosen = (holders == owner_of[None, None, :]) & (places == slot_of[None, None, :])
    return chosen.astype(jnp.bfloat16)


def pack_slots(shards, chooser):
    return jnp.einsum("psm,mkd->skpd", chooser, shards, preferred_element_type=jnp.float32).astype(
        jnp.bfloat16
    )


def unpack_slots(received, chooser):
    return jnp.einsum("psm,skpd->mkd", chooser, received, preferred_element_type=jnp.float32)


def per_device_general(activations, cotangents, momentum, owners, bucket_starts):
    shard_count = lax.axis_size("shard")
    replica_count = lax.axis_size("rep")
    layers, tok_rows, width = activations.shape
    token_total = tok_rows * shard_count * replica_count
    columns = width // shard_count
    slot_count = -(-MATS // shard_count) + 1
    update_scale = math.sqrt(max(KV, D))
    partial_terms = jnp.einsum(
        "ltk,ltd->lkd", cotangents, activations, preferred_element_type=jnp.float32
    ).reshape(MATS, KV, width)
    shard_part = lax.psum_scatter(
        partial_terms.astype(jnp.bfloat16), "shard", scatter_dimension=2, tiled=True
    )
    summed = lax.psum(shard_part, "rep").astype(jnp.float32)
    gradient = summed / jnp.sqrt(jnp.float32(token_total))
    square_sums = lax.psum(jnp.sum(gradient * gradient, axis=(1, 2)), "shard")
    factors = clip_factors(square_sums, bucket_starts)
    momentum_out = momentum_rate * momentum + factors[:, None, None] * gradient
    nesterov = (factors[:, None, None] * gradient + momentum_rate * momentum_out).astype(
        jnp.bfloat16
    )
    slot_of = slot_numbers(owners)
    chooser = selector(owners, slot_of, shard_count, slot_count)
    received = lax.all_to_all(
        pack_slots(nesterov, chooser), "shard", split_axis=2, concat_axis=2, tiled=True
    )
    item_count = received.shape[0]
    result = orthogonal_batch(received.reshape(item_count, KV, width))
    scaled = (update_scale * result.astype(jnp.float32)).astype(jnp.bfloat16)
    returned_part = lax.all_to_all(
        result.reshape(item_count, KV, shard_count, columns),
        "shard",
        split_axis=2,
        concat_axis=2,
        tiled=True,
    )
    update = update_scale * unpack_slots(returned_part, chooser)
    return (momentum_out, update, scaled)


def lodged(block, member):
    x = lax.rem(block, 2)
    y = lax.div(block, 2)
    whole = 2 * x + y
    paired = 4 + y
    return jnp.where(member < 2, whole, paired), jnp.where(member < 2, member, x)


def lodging(matrix):
    layer = lax.div(matrix, 2)
    side = lax.rem(matrix, 2)
    early = matrix < 8
    x = jnp.where(early, lax.div(layer, 2), side)
    y = jnp.where(early, lax.rem(layer, 2), layer - 4)
    return 2 * y + x, jnp.where(early, side, 2)


def place():
    me = lax.axis_index("rep")
    core = lax.rem(me, 2)
    x = lax.rem(lax.div(me, 2), 2)
    y = lax.div(me, 4)
    to_core = me + 1 - 2 * core
    to_x = me + 2 - 4 * x
    to_y = me + 4 - 8 * y
    to_xy = me + 6 - 4 * x - 8 * y
    return me, core, x, y, to_core, to_x, to_y, to_xy


def greet(peers, meanwhile):
    barrier = pltpu.get_barrier_semaphore()
    for peer in peers:
        pl.semaphore_signal(barrier, inc=1, device_id=peer, device_id_type=MESH)
    meanwhile()
    pl.semaphore_wait(barrier, len(peers))


def remote(src, dst, send, recv, peer):
    return pltpu.make_async_remote_copy(
        src_ref=src, dst_ref=dst, send_sem=send, recv_sem=recv, device_id=peer, device_id_type=MESH
    )


class PlaneGather:
    def __init__(self, z, at, send, recv):
        self.z, self.at, self.send, self.recv = z, at, send, recv
        self.copies = {}

    def go(self, k, block, half, peer):
        ref = self.at(block, half)
        self.copies[k] = remote(ref, ref, self.send, self.recv.at[k], (peer, self.z))
        self.copies[k].start()

    def wait(self, *ks):
        for k in ks:
            self.copies[k].wait_recv()

    def begin(self):
        me, core, x, y, to_core, to_x, to_y, to_xy = place()
        for k, peer, half in ((0, to_x, 0), (2, to_y, 1), (1, to_x, 1), (3, to_y, 0), (4, to_core, None)):
            self.go(k, me, half, peer)

    def turn(self):
        me, core, x, y, to_core, to_x, to_y, to_xy = place()
        self.wait(0)
        self.go(5, to_x, 0, to_y)
        self.wait(2)
        self.go(6, to_y, 1, to_x)

    def share(self):
        me, core, x, y, to_core, to_x, to_y, to_xy = place()
        self.wait(1)
        self.go(7, to_x, None, to_core)
        self.wait(3)
        self.go(8, to_y, None, to_core)

    def corner(self):
        me, core, x, y, to_core, to_x, to_y, to_xy = place()
        self.wait(5, 6)
        self.go(9, to_xy, None, to_core)


def drain(ref, semaphore):
    pltpu.make_async_copy(ref, ref, semaphore).wait()


def gather_reduce(
    n_shard, inverse, act_ref, cot_ref, gall, sqall, act, cot, turned, part, recv, plane, zrecv,
    in_sem, hop_r, swap_s, hop_s, pass_s, sum_s, sum_r, line_s, line_r,
):
    f32 = jnp.float32
    me, core, x, y, to_core, to_x, to_y, to_xy = place()
    z = lax.axis_index("shard")
    tokens = act_ref.shape[1]
    members, rows, cols = plane.shape[1:]
    near = z + 1 - 2 * lax.rem(z, 2)
    low = z < 2
    inner = (z == 1) | (z == 2)
    inward = jnp.where(low, z + 1, z - 1)
    targets = (jnp.where(low, 3, 0), jnp.where(low, 2, 1), near, z)
    cut = [pl.ds(pl.multiple_of(t * cols, cols), cols) for t in targets]
    counts = [c.shape[0] for c in cot]
    shared = counts[0] * 2
    mine = (counts[0] * x, shared + counts[1] * y)
    yours = (counts[0] * (1 - x), shared + counts[1] * (1 - y))
    peers = (to_x, to_y)
    layer_of = ((1 - y, y), (0,))
    keys = [(1, n_shard, 0), (0, n_shard, 0), (1, 0, 0), (0, 0, 0), (0, n_shard, 1), (0, 0, 1)]
    keys += [(kind, k, j) for k in range(1, n_shard) for kind, j in ((1, 0), (0, 0), (0, 1))]

    def index(kind, k, j):
        return 2 * k + j if kind == 0 else 2 * (n_shard + 1) + k

    def source(kind, k, layer):
        return cot_ref.at[layer] if k == n_shard else act_ref.at[layer, :, cut[k]]

    def slots(kind, k, j, first, count):
        layer = layer_of[kind][j]
        buffer = cot[kind].at[layer] if k == n_shard else act[kind].at[k, layer]
        return buffer.at[pl.ds(first * tokens, count * tokens)]

    own, swap, hop, onward = {}, {}, {}, {}
    for key in keys:
        kind, k, j = key
        at = in_sem.at[index(*key)]
        group = 2 * kind + (1 if k == n_shard else 0)
        layer = layer_of[kind][j]
        here = source(kind, k, mine[kind] + layer)
        own[key] = pltpu.make_async_copy(here, slots(*key, 0, 1), at)
        swap[key] = remote(here, slots(*key, 1, 1), swap_s.at[group], at, (to_core, z))
        hop[key] = remote(
            source(kind, k, yours[kind] + layer), slots(*key, 3, 1),
            hop_s.at[group], hop_r.at[index(*key)], (peers[kind], z),
        )
        onward[key] = remote(slots(*key, 3, 1), slots(*key, 2, 1), pass_s.at[group], at, (to_core, z))
    sums = [
        [
            remote(
                part[0].at[k, 1 - y], recv[0].at[k], sum_s.at[0], sum_r.at[0, k], (to_y, z)
            ),
            remote(
                part[1].at[k, 1 - x], recv[1].at[k], sum_s.at[1], sum_r.at[1, k], (to_x, z)
            ),
        ]
        for k in range(n_shard)
    ]
    spans = (pl.ds(0, members - 1), pl.ds(members - 1, 1))
    lines = [
        [
            remote(
                plane.at[k, spans[kind]],
                zrecv.at[k if k == 2 else k + 3 * inner.astype(jnp.int32), spans[kind]],
                line_s.at[kind],
                line_r.at[k if k == 2 else k + 3 * inner.astype(jnp.int32), kind],
                (me, near if k == 2 else inward),
            )
            for kind in range(2)
        ]
        for k in range(n_shard - 1)
    ]

    def arrived(s, kind):
        remote(
            plane.at[0, spans[kind]], zrecv.at[s, spans[kind]], line_s.at[kind], line_r.at[s, kind],
            (me, near),
        ).wait_recv()

    def enter():
        for key in keys:
            own[key].start()

    def begin():
        for key in keys[:9]:
            hop[key].start()
        for key in keys:
            swap[key].start()

    def take(kind, k, j=0):
        hop[kind, k, j].wait_recv()
        onward[kind, k, j].start()

    def ready(kind, k, j):
        drain(slots(kind, k, j, 0, 3), in_sem.at[index(kind, k, j)])

    def turn(kind, j=0):
        ready(kind, n_shard, j)
        layer = layer_of[kind][j]
        for side in range(2):
            at = pl.ds(pl.multiple_of((2 * side + core) * rows, rows), rows)
            turned[kind][layer, side] = cot[kind][layer, :, at].T

    def product(kind, k, j=0):
        ready(kind, k, j)
        layer = layer_of[kind][j]

        def one(side, carry):
            value = jnp.dot(turned[kind][layer, side], act[kind][k, layer], preferred_element_type=f32)
            if kind == 0:
                part[0][k, layer, side] = value.astype(part[0].dtype)
            else:
                part[1][k, side, 0] = value.astype(part[1].dtype)
            return carry

        lax.fori_loop(0, 2, one, 0)
        if j == 0:
            sums[k][kind].start()

    def gather(kind, k):
        sums[k][kind].wait_recv()
        for i in range(members - 1 if kind == 0 else 1):
            kept = part[0][k, y, i] if kind == 0 else part[1][k, x, i]
            value = kept.astype(f32) + recv[kind][k, i].astype(f32)
            plane[k, i if kind == 0 else members - 1] = value.astype(plane.dtype)

    def release(kind, k):
        @pl.when(jnp.logical_not(inner))
        def _():
            lines[k][kind].start()

    def forward(kind, k):
        s = 3 if k == 2 else k

        @pl.when(inner)
        def _():
            arrived(s, kind)
            for i in range(members - 1) if kind == 0 else (members - 1,):
                value = plane[k, i].astype(f32) + zrecv[s, i].astype(f32)
                plane[k, i] = value.astype(plane.dtype)
            lines[k][kind].start()

    def run():
        take(1, n_shard)
        take(0, n_shard, 0)
        turn(1)
        take(1, 0)
        take(0, 0, 0)
        turn(0, 0)
        product(1, 0)
        hop[0, 2, 0].start()
        product(0, 0, 0)
        hop[1, 2, 0].start()
        take(1, 1)
        take(0, n_shard, 1)
        product(1, 1)
        hop[0, 2, 1].start()
        hop[0, 3, 0].start()
        turn(0, 1)
        take(0, 0, 1)
        product(0, 0, 1)
        take(0, 1, 0)
        product(0, 1, 0)
        hop[1, 3, 0].start()
        gather(0, 0)
        release(0, 0)
        take(0, 1, 1)
        product(0, 1, 1)
        take(1, 2)
        product(1, 2)
        hop[0, 3, 1].start()
        gather(1, 0)
        release(1, 0)
        take(0, 2, 0)
        product(0, 2, 0)
        gather(0, 1)
        release(0, 1)
        forward(0, 0)
        gather(1, 1)
        release(1, 1)
        forward(1, 0)
        take(1, 3)
        product(1, 3)
        take(0, 2, 1)
        product(0, 2, 1)
        take(0, 3, 0)
        product(0, 3, 0)
        gather(0, 2)
        release(0, 2)
        forward(0, 1)
        forward(0, 2)
        gather(1, 2)
        release(1, 2)
        forward(1, 1)
        forward(1, 2)
        take(0, 3, 1)
        product(0, 3, 1)
        gather(1, 3)
        gather(0, 3)
        for kind in range(2):
            arrived(2, kind)
        home = lax.div(me, 2)
        half = pl.ds(pl.multiple_of(core * rows, rows), rows)

        def add_last(others, j):
            value = plane[n_shard - 1, j].astype(f32)
            for s in others:
                value = value + zrecv[s, j].astype(f32)
            value = (value * inverse).astype(gall.dtype)
            gall[home, j, half] = value
            value = value.astype(f32)
            line = jnp.sum(value * value, axis=0, keepdims=True)
            lanes = sqall.shape[-1]
            fold = line[:, :lanes]
            for i in range(1, cols // lanes):
                fold = fold + line[:, i * lanes : (i + 1) * lanes]
            sqall[me * n_shard + z, j] = fold

        @pl.when(inner)
        def _():
            for kind in range(2):
                arrived(4, kind)
            for j in range(members):
                add_last((2, 4), j)

        @pl.when(jnp.logical_not(inner))
        def _():
            for j in range(members):
                add_last((2,), j)

    def leave():
        for kind in range(2):
            for pool in (swap_s, hop_s, pass_s):
                drain(act[kind].at[:, :, pl.ds(0, tokens)], pool.at[2 * kind])
                drain(cot[kind].at[:, pl.ds(0, tokens)], pool.at[2 * kind + 1])
            drain(recv[kind], sum_s.at[kind])
            drain(plane.at[pl.ds(0, n_shard - 1), spans[kind]], line_s.at[kind])

    return enter, begin, run, leave


HOMES = ((1, 0), (2, 0), (2, 1))


def block_at(ref, axis, rows):
    def at(r, half):
        count = rows if half is None else rows // 2
        start = lax.rem(r, 2) * rows + (0 if half is None else half * count)
        cut = pl.ds(pl.multiple_of(start, count), count)
        block = lax.div(r, 2)
        return ref.at[block, cut] if axis == 1 else ref.at[block, :, cut]

    return at


def split(value):
    high = value.astype(jnp.bfloat16)
    return high, (value - high.astype(jnp.float32)).astype(jnp.bfloat16)


def times(left, right):
    dot = functools.partial(jnp.dot, preferred_element_type=jnp.float32)
    return dot(left[0], right[0]) + (dot(left[0], right[1]) + dot(left[1], right[0]))


def gram_iteration(gram, scale, gram_scr, root_scr):
    n = gram.shape[0]
    row = lax.broadcasted_iota(jnp.int32, (n, n), 0)
    col = lax.broadcasted_iota(jnp.int32, (n, n), 1)
    eye = (row == col).astype(jnp.float32)
    trace = jnp.sum(jnp.sum(gram * eye, axis=0, keepdims=True), axis=1, keepdims=True)
    inverse = 1.0 / (jnp.sqrt(trace) + epsilon)
    gram_scr[...] = gram * inverse * inverse
    for iteration in range(ITERS):
        a = split(gram_scr[...])
        mixing = coef_b * gram_scr[...] + coef_c * times(a, a)
        b = split(mixing)
        if iteration == 0:
            root_scr[...] = coef_a * eye + mixing
        else:
            root_scr[...] = coef_a * root_scr[...] + times(b, split(root_scr[...]))
        if iteration < ITERS - 1:
            half = coef_a * gram_scr[...] + times(b, a)
            gram_scr[...] = coef_a * half + times(b, split(half))
    return root_scr[...] * (inverse * scale)


def muon_kernel(
    n_shard, inverse, scale, owner_ref, start_ref, act_ref, cot_ref, momentum_hbm,
    mout_ref, u_ref, wall_ref, qall_ref,
    momentum, gall, sqall, table, factor, uown, held, gram_out, gram_in, gram_scr, root_scr, root,
    act, cot, turned, part, recv, plane, zrecv, reduce_sems,
    load, ps, pr, gs, gr, as_, ar, ws, wr, os_, or_, rs, rr, hs, hr,
):
    f32, bf16 = jnp.float32, jnp.bfloat16
    me, core, x, y, to_core, to_x, to_y, to_xy = place()
    z = lax.axis_index("shard")
    base = me - core
    block = lax.div(me, 2)
    members = gall.shape[1]
    rows, cols = held.shape[1:]
    lanes = sqall.shape[-1]
    mine = pl.ds(pl.multiple_of(core * rows, rows), rows)

    fetch = pltpu.make_async_copy(momentum_hbm, momentum, load)
    enter, begin, run, leave = gather_reduce(
        n_shard, inverse, act_ref, cot_ref, gall, sqall, act, cot, turned, part, recv,
        plane, zrecv, *reduce_sems,
    )
    everyone = n_shard * 2 * gall.shape[0]
    here = me * n_shard + z
    others = [lax.rem(here + t, everyone) for t in range(1, everyone)]
    others = [(lax.div(to, n_shard), lax.rem(to, n_shard)) for to in others]
    greet(others, enter)

    begin()
    fetch.start()
    run()

    for peer in others:
        remote(sqall.at[here], sqall.at[here], ps, pr, peer).start()
    at_g = block_at(gall, 2, rows)
    gather_g = PlaneGather(z, at_g, gs, gr)
    gather_g.begin()
    fetch.wait()
    drain(sqall.at[pl.ds(0, everyone - 1)], pr)

    table[...] = jnp.zeros_like(table)
    for m in range(MATS):
        layer, side = divmod(m, 2)
        bx, by = divmod(layer, 2) if m < 8 else (side, layer - 4)
        j, i = 2 * by + bx, side if m < 8 else 2
        line = sqall[2 * j * n_shard, i]
        for d in range(1, 2 * n_shard):
            line = line + sqall[2 * j * n_shard + d, i]
        table[pl.ds(m, 1)] = line
    index = lax.broadcasted_iota(jnp.int32, table.shape, 0)
    bucket = jnp.zeros(table.shape, jnp.int32)
    for k in range(start_ref.shape[0]):
        bucket = bucket + (index >= start_ref[k]).astype(jnp.int32)
    sums = table[...]
    clip = jnp.zeros(table.shape, f32)
    for k in range(start_ref.shape[0] + 1):
        inside = (bucket == k) & (index < MATS)
        total = jnp.sum(jnp.where(inside, sums, 0.0), axis=(0, 1), keepdims=True)
        count = jnp.sum(inside.astype(f32), axis=(0, 1), keepdims=True) / lanes
        mean = total / (jnp.maximum(count, 1.0) * (2 * rows) * (n_shard * cols))
        clip = jnp.where(inside, jnp.minimum(1.0, clip_level / jnp.sqrt(mean + epsilon)), clip)
    for m in range(MATS):
        factor[m] = jnp.concatenate([clip[m : m + 1, :]] * (cols // lanes), axis=1)

    def advance(matrix, gradient, past):
        step = factor[matrix] * gradient.astype(f32)
        new = momentum_rate * past + step
        return new, (step + momentum_rate * new).astype(bf16)

    gather_g.turn()
    gather_g.wait(4)
    for i in range(members):
        layer, side = lodged(block, i)
        matrix = 2 * layer + side
        uown[i] = advance(matrix, gall[block, i], momentum[matrix])[1]
    over = (((1,), (1,)), ((), ()))
    parts = []
    for i, (hz, hc) in enumerate(HOMES):
        here = (z == hz) & (core == hc)
        owner = (base + hc, hz)
        low = uown[i, :rows]
        high = uown[i, rows:]
        own = jnp.where(core == 0, low, high)
        diag = lax.dot_general(own, own, over, preferred_element_type=f32)
        gram_out[i, 0] = diag
        part = remote(gram_out.at[i, 0], gram_in.at[z, core], as_.at[i, 0], ar.at[z, core], owner)
        cross = remote(gram_out.at[i, 1], gram_in.at[z, 2], as_.at[i, 1], ar.at[z, 2], owner)
        parts.append((here, part, cross))

        @pl.when(here)
        def _():
            gram_in[z, core] = diag

        @pl.when(jnp.logical_not(here))
        def _():
            part.start()

        @pl.when(core == 0)
        def _():
            off = lax.dot_general(low, high, over, preferred_element_type=f32)
            gram_out[i, 1] = off

            @pl.when(here)
            def _():
                gram_in[z, 2] = off

            @pl.when(jnp.logical_not(here))
            def _():
                cross.start()

    gather_g.share()
    gather_g.corner()
    gather_g.wait(7, 8, 9)

    def slot_matrix(shard, slot):
        found = jnp.int32(0)
        count = jnp.int32(0)
        for m in range(MATS):
            yes = owner_ref[m] == shard
            found = jnp.where(yes & (count == slot), m, found)
            count = count + yes.astype(jnp.int32)
        return found

    partners = {
        1: z + 1 - 2 * lax.rem(z, 2),
        2: z + 2 - 4 * lax.div(z, 2),
        3: n_shard - 1 - z,
    }
    sends = {}
    walls = {}

    def send_slice(e):
        matrix = slot_matrix(partners[e], block)
        home, member = lodging(matrix)
        held[e - 1] = advance(matrix, gall[home, member, mine], momentum[matrix, mine])[1]
        sends[e] = remote(
            held.at[e - 1], wall_ref.at[e - 1, block, mine], ws, wr.at[e - 1], (me, partners[e])
        )
        sends[e].start()

    send_slice(1)
    send_slice(3)

    def all_one(m, carry):
        home, member = lodging(m)
        new, turned = advance(m, gall[home, member], momentum[m])
        mout_ref[m] = new
        u_ref[m] = turned
        return carry

    def wall_begin(e):
        sends[e].wait_recv()
        at = block_at(wall_ref.at[e - 1], 1, rows)
        walls[e] = PlaneGather(z, at, os_.at[e - 1], or_.at[e - 1])
        walls[e].begin()

    is_home = functools.reduce(jnp.logical_or, [here for here, _, _ in parts])
    member = jnp.where(z == HOMES[0][0], 0, 1 + core)
    roots = []
    packed = root.shape[0] // 2
    mine_q = pl.ds(pl.multiple_of(core * packed, packed), packed)
    for d in range(n_shard):
        for c in range(2):
            if d == 0 and c == 1:
                continue
            peer = (to_core, z) if d == 0 else (base + c, lax.rem(z + d, n_shard))
            half = 1 - core if d == 0 else c
            cut = pl.ds(pl.multiple_of(half * packed, packed), packed)
            roots.append(remote(root.at[cut], qall_ref.at[block, member, cut], rs, rr.at[member], peer))

    @pl.when(jnp.logical_not(is_home))
    def _():
        lax.fori_loop(0, MATS, all_one, 0)

    @pl.when(is_home)
    def _():
        for d in range(n_shard):
            for k in range(3):
                source = remote(gram_out.at[0, 0], gram_in.at[d, k], as_.at[0, 0], ar.at[d, k], (to_core, z))
                local = (z == d) & ((core == k) if k < 2 else (core == 0))

                @pl.when(jnp.logical_not(local))
                def _():
                    source.wait_recv()

        blocks = []
        for k in range(3):
            value = gram_in[0, k]
            for d in range(1, n_shard):
                value = value + gram_in[d, k]
            blocks.append(value)
        top = jnp.concatenate([blocks[0], blocks[2]], axis=1)
        bottom = jnp.concatenate([blocks[2].T, blocks[1]], axis=1)
        result = gram_iteration(jnp.concatenate([top, bottom], axis=0), scale, gram_scr, root_scr)
        result = result.astype(bf16)
        root[:rows] = result[:rows, :rows]
        root[rows:packed] = result[: rows // 2, rows:]
        root[packed : packed + rows] = result[rows:, rows:]
        root[packed + rows :] = result[rows // 2 : rows, rows:]
        for c in roots:
            c.start()
        qall_ref[block, member, mine_q] = root[mine_q]

    wall_begin(1)
    wall_begin(3)
    send_slice(2)
    walls[1].turn()
    walls[1].share()
    walls[3].turn()
    walls[1].corner()
    for i, (here, _, _) in enumerate(parts):
        arrival = remote(root.at[mine_q], qall_ref.at[block, i, mine_q], rs, rr.at[i], (to_core, z))

        @pl.when(jnp.logical_not(here))
        def _():
            arrival.wait_recv()

    gather_q = PlaneGather(z, block_at(qall_ref, 2, packed), hs, hr)
    gather_q.begin()
    walls[3].share()
    wall_begin(2)
    walls[3].corner()
    gather_q.turn()
    gather_q.share()
    walls[2].turn()

    @pl.when(is_home)
    def _():
        lax.fori_loop(0, MATS, all_one, 0)

    gather_q.corner()
    walls[2].share()
    walls[2].corner()
    for gather in (walls[1], walls[3], gather_q, walls[2]):
        gather.wait(4, 7, 8, 9)
    most = pl.ds(0, 2 * rows - rows // 4)
    drain(gall.at[:, :, most], gs)
    drain(qall_ref.at[:, :, pl.ds(0, 2 * packed - packed // 4)], hs)
    for d in range(n_shard - 1):
        drain(wall_ref.at[d, :, most], os_.at[d])
    drain(held, ws)
    drain(sqall.at[pl.ds(0, everyone - 1)], ps)

    @pl.when(is_home)
    def _():
        drain(u_ref.at[pl.ds(0, len(roots)), pl.ds(0, packed * rows // cols)], rs)

    for here, part, cross in parts:

        @pl.when(jnp.logical_not(here))
        def _():
            part.wait_send()

            @pl.when(core == 0)
            def _():
                cross.wait_send()

    leave()


def finish_kernel(
    owner_ref, mout_ref, u_ref, wall_ref, qall_ref, mom_out, update_out, owned_out,
    ubuf, wbuf, qbuf, msem, usem, wsem,
):
    f32 = jnp.float32
    slots, _, width = wbuf.shape
    mats, _, cols = ubuf.shape
    n_shard = width // cols
    rows = qall_ref.shape[-1]
    z = lax.axis_index("shard")
    whole = pltpu.make_async_copy(mout_ref, mom_out, msem)
    whole.start()

    def put(buf, out, sem, m):
        return pltpu.make_async_copy(buf.at[m], out.at[m], sem.at[m])

    def update_one(m, carry):
        home, member = lodging(m)
        q = qall_ref[home, member]
        cross = jnp.concatenate([q[rows : 3 * rows // 2], q[5 * rows // 2 :]], axis=0)
        qbuf[m, :rows, :rows] = q[:rows]
        qbuf[m, :rows, rows:] = cross
        qbuf[m, rows:, :rows] = cross.T
        qbuf[m, rows:, rows:] = q[3 * rows // 2 : 5 * rows // 2]
        ubuf[m] = jnp.dot(qbuf[m], u_ref[m], preferred_element_type=f32)
        put(ubuf, update_out, usem, m).start()
        return carry

    lax.fori_loop(0, mats, update_one, 0, unroll=3)

    def owned_one(s, carry):
        matrix = jnp.int32(0)
        count = jnp.int32(0)
        for m in range(mats):
            yes = owner_ref[m] == z
            matrix = jnp.where(yes & (count == s), m, matrix)
            count = count + yes.astype(jnp.int32)
        keep = (count > s).astype(f32)
        q = qbuf[matrix]
        for d in range(n_shard):
            right = u_ref[matrix] if d == 0 else wall_ref[d - 1, s]
            value = jnp.dot(q, right, preferred_element_type=f32) * keep
            at = (z, z + 1 - 2 * lax.rem(z, 2), z + 2 - 4 * lax.div(z, 2), n_shard - 1 - z)[d]
            wbuf[s, :, pl.ds(pl.multiple_of(at * cols, cols), cols)] = value.astype(wbuf.dtype)
        put(wbuf, owned_out, wsem, s).start()
        return carry

    lax.fori_loop(0, slots, owned_one, 0, unroll=2)

    def each(count, buf, out, sem):
        def step(m, carry):
            put(buf, out, sem, m).wait()
            return carry

        lax.fori_loop(0, count, step, 0)

    whole.wait()
    each(mats, ubuf, update_out, usem)
    each(slots, wbuf, owned_out, wsem)


def per_device_planes(activations, cotangents, momentum, owners, bucket_starts):
    n_shard = lax.axis_size("shard")
    n_rep = lax.axis_size("rep")
    layers, tok_rows, width = activations.shape
    token_total = tok_rows * n_shard * n_rep
    cols = width // n_shard
    rows = KV // 2
    lanes = math.gcd(cols, 128)
    groups = n_rep // 2
    members = MATS // groups
    slots = -(-MATS // n_shard) + 1
    update_scale = math.sqrt(max(KV, D))
    bf16, f32 = jnp.bfloat16, jnp.float32

    def params(limit, **rest):
        return pltpu.CompilerParams(vmem_limit_bytes=limit * 1024 * 1024, **rest)

    dma = pltpu.SemaphoreType.DMA
    tokens = 4 * tok_rows
    shares = (layers // 3, layers // 6)
    hbm = functools.partial(pltpu.with_memory_space_constraint, memory_space=pltpu.HBM)
    mout, turned, wall, qall = pl.pallas_call(
        functools.partial(muon_kernel, n_shard, 1.0 / math.sqrt(token_total), update_scale),
        out_shape=(
            pltpu.VMEM((MATS, KV, cols), f32),
            pltpu.VMEM((MATS, KV, cols), bf16),
            pltpu.VMEM((n_shard - 1, slots, KV, cols), bf16),
            pltpu.VMEM((groups, members, 3 * rows, rows), bf16),
        ),
        in_specs=[SMEM_SPEC, SMEM_SPEC, ANY_SPEC, ANY_SPEC, ANY_SPEC],
        out_specs=(VMEM_SPEC,) * 4,
        scratch_shapes=[
            pltpu.VMEM((MATS, KV, cols), f32),
            pltpu.VMEM((groups, members, KV, cols), bf16),
            pltpu.VMEM((n_rep * n_shard, members, 1, lanes), f32),
            pltpu.VMEM((16, lanes), f32),
            pltpu.VMEM((MATS, 1, cols), f32),
            pltpu.VMEM((members, KV, cols), bf16),
            pltpu.VMEM((n_shard - 1, rows, cols), bf16),
            pltpu.VMEM((members, 2, rows, rows), f32),
            pltpu.VMEM((n_shard, 3, rows, rows), f32),
            pltpu.VMEM((KV, KV), f32),
            pltpu.VMEM((KV, KV), f32),
            pltpu.VMEM((3 * rows, rows), bf16),
            [pltpu.VMEM((n_shard, n, tokens, cols), bf16) for n in shares],
            [pltpu.VMEM((n, tokens, 2 * KV), bf16) for n in shares],
            [pltpu.VMEM((n, 2, rows, tokens), bf16) for n in shares],
            [pltpu.VMEM((n_shard, 2, n, rows, cols), bf16) for n in shares],
            [pltpu.VMEM((n_shard, n, rows, cols), bf16) for n in shares],
            pltpu.VMEM((n_shard, members, rows, cols), bf16),
            pltpu.VMEM((n_shard + 1, members, rows, cols), bf16),
            [dma((3 * n_shard + 3,)) for _ in range(2)]
            + [dma((4,)) for _ in range(3)]
            + [dma((2,)), dma((2, n_shard)), dma((2,)), dma((n_shard + 1, 2))],
            dma(()),
            dma(()), dma(()),
            dma(()), dma((10,)),
            dma((members, 2)), dma((n_shard, 3)),
            dma(()), dma((n_shard - 1,)),
            dma((n_shard - 1,)), dma((n_shard - 1, 10)),
            dma(()), dma((members,)),
            dma(()), dma((10,)),
        ],
        compiler_params=params(48, has_side_effects=True, collective_id=0),
        name="muon",
    )(owners, bucket_starts, hbm(activations), hbm(cotangents), hbm(momentum))

    return pl.pallas_call(
        finish_kernel,
        out_shape=(
            jax.ShapeDtypeStruct(momentum.shape, f32),
            jax.ShapeDtypeStruct(momentum.shape, f32),
            jax.ShapeDtypeStruct((slots, KV, width), bf16),
        ),
        in_specs=[SMEM_SPEC] + [VMEM_SPEC] * 4,
        out_specs=(ANY_SPEC,) * 3,
        scratch_shapes=[
            pltpu.VMEM(momentum.shape, f32),
            pltpu.VMEM((slots, KV, width), bf16),
            pltpu.VMEM((MATS, KV, KV), bf16),
            dma(()), dma((MATS,)), dma((slots,)),
        ],
        compiler_params=params(20),
        name="finish",
    )(owners, mout, turned, wall, qall)


def solution(mesh):
    groups = mesh.shape["rep"] // 2
    slots = -(-MATS // mesh.shape["shard"]) + 1
    fits = mesh.shape["rep"] == 8 and mesh.shape["shard"] == 4 and slots <= groups
    placed = (
        P(None, ("rep", "shard"), None),
        P(None, ("rep", "shard"), None),
        P(None, None, "shard"),
        P(),
        P(),
    )
    return jax.shard_map(
        per_device_planes if fits else per_device_general,
        mesh=mesh,
        in_specs=placed,
        out_specs=(P(None, None, "shard"), P(None, None, "shard"), P("shard", None, None)),
        check_vma=False,
    )
```

```python
import functools
import math

import jax
import jax.numpy as jnp
from jax import lax
from jax.experimental import pallas as pl
from jax.experimental.pallas import tpu as pltpu
from jax.sharding import PartitionSpec as P

D = 2048
KV = 256
ITERS = 5
MATS = 12
MESH = pl.DeviceIdType.MESH
VMEM_SPEC = pl.BlockSpec(memory_space=pltpu.VMEM)
SMEM_SPEC = pl.BlockSpec(memory_space=pltpu.SMEM)
ANY_SPEC = pl.BlockSpec(memory_space=pl.ANY)
VMEM_LIMIT = 60 * 1024 * 1024

coef_a = 3.4445
coef_b = -4.775
coef_c = 2.0315
momentum_rate = 0.95
clip_level = 0.5
epsilon = 1e-06


def orthogonal_batch(matrices):
    values = matrices.astype(jnp.float32)
    frobenius = jnp.sqrt(jnp.sum(values * values, axis=(1, 2), keepdims=True))
    matrix = (values / (frobenius + epsilon)).astype(jnp.bfloat16)
    for iteration in range(ITERS):
        gram_matrix = jnp.einsum(
            "skd,sjd->skj", matrix, matrix, preferred_element_type=jnp.float32
        ).astype(jnp.bfloat16)
        square = jnp.einsum(
            "skj,sji->ski", gram_matrix, gram_matrix, preferred_element_type=jnp.float32
        )
        mixing = (coef_b * gram_matrix.astype(jnp.float32) + coef_c * square).astype(jnp.bfloat16)
        product = jnp.einsum("skj,sjd->skd", mixing, matrix, preferred_element_type=jnp.float32)
        matrix = (coef_a * matrix.astype(jnp.float32) + product).astype(jnp.bfloat16)
    return matrix


def clip_factors(square_sums, bucket_starts):
    indices = jnp.arange(MATS, dtype=jnp.int32)
    buckets = jnp.sum((indices[:, None] >= bucket_starts[None, :]).astype(jnp.int32), axis=1)
    together = (buckets[:, None] == buckets[None, :]).astype(jnp.float32)
    totals = jnp.sum(together * square_sums[None, :], axis=1)
    members = jnp.sum(together, axis=1)
    root_mean = jnp.sqrt(totals / (members * KV * D) + epsilon)
    return jnp.minimum(1.0, clip_level / root_mean)


def slot_numbers(owners):
    indices = jnp.arange(MATS, dtype=jnp.int32)
    earlier = (indices[None, :] < indices[:, None]) & (owners[None, :] == owners[:, None])
    return jnp.sum(earlier.astype(jnp.int32), axis=1)


def selector(owner_of, slot_of, shard_count, slot_count):
    holders = lax.broadcasted_iota(jnp.int32, (shard_count, slot_count, 1), 0)
    places = lax.broadcasted_iota(jnp.int32, (shard_count, slot_count, 1), 1)
    chosen = (holders == owner_of[None, None, :]) & (places == slot_of[None, None, :])
    return chosen.astype(jnp.bfloat16)


def pack_slots(shards, chooser):
    return jnp.einsum("psm,mkd->skpd", chooser, shards, preferred_element_type=jnp.float32).astype(
        jnp.bfloat16
    )


def unpack_slots(received, chooser):
    return jnp.einsum("psm,skpd->mkd", chooser, received, preferred_element_type=jnp.float32)


def per_device_general(activations, cotangents, momentum, owners, bucket_starts):
    shard_count = lax.axis_size("shard")
    replica_count = lax.axis_size("rep")
    layers, tok_rows, width = activations.shape
    token_total = tok_rows * shard_count * replica_count
    columns = width // shard_count
    slot_count = -(-MATS // shard_count) + 1
    update_scale = math.sqrt(max(KV, D))
    partial_terms = jnp.einsum(
        "ltk,ltd->lkd", cotangents, activations, preferred_element_type=jnp.float32
    ).reshape(MATS, KV, width)
    shard_part = lax.psum_scatter(
        partial_terms.astype(jnp.bfloat16), "shard", scatter_dimension=2, tiled=True
    )
    summed = lax.psum(shard_part, "rep").astype(jnp.float32)
    gradient = summed / jnp.sqrt(jnp.float32(token_total))
    square_sums = lax.psum(jnp.sum(gradient * gradient, axis=(1, 2)), "shard")
    factors = clip_factors(square_sums, bucket_starts)
    momentum_out = momentum_rate * momentum + factors[:, None, None] * gradient
    nesterov = (factors[:, None, None] * gradient + momentum_rate * momentum_out).astype(
        jnp.bfloat16
    )
    slot_of = slot_numbers(owners)
    chooser = selector(owners, slot_of, shard_count, slot_count)
    received = lax.all_to_all(
        pack_slots(nesterov, chooser), "shard", split_axis=2, concat_axis=2, tiled=True
    )
    item_count = received.shape[0]
    result = orthogonal_batch(received.reshape(item_count, KV, width))
    scaled = (update_scale * result.astype(jnp.float32)).astype(jnp.bfloat16)
    returned_part = lax.all_to_all(
        result.reshape(item_count, KV, shard_count, columns),
        "shard",
        split_axis=2,
        concat_axis=2,
        tiled=True,
    )
    update = update_scale * unpack_slots(returned_part, chooser)
    return (momentum_out, update, scaled)


def lodged(block, member):
    x = lax.rem(block, 2)
    y = lax.div(block, 2)
    whole = 2 * x + y
    paired = 4 + y
    return jnp.where(member < 2, whole, paired), jnp.where(member < 2, member, x)


def lodging(matrix):
    layer = lax.div(matrix, 2)
    side = lax.rem(matrix, 2)
    early = matrix < 8
    x = jnp.where(early, lax.div(layer, 2), side)
    y = jnp.where(early, lax.rem(layer, 2), layer - 4)
    return 2 * y + x, jnp.where(early, side, 2)


def place():
    me = lax.axis_index("rep")
    core = lax.rem(me, 2)
    x = lax.rem(lax.div(me, 2), 2)
    y = lax.div(me, 4)
    to_core = me + 1 - 2 * core
    to_x = me + 2 - 4 * x
    to_y = me + 4 - 8 * y
    to_xy = me + 6 - 4 * x - 8 * y
    return me, core, x, y, to_core, to_x, to_y, to_xy


def greet(peers, meanwhile):
    barrier = pltpu.get_barrier_semaphore()
    for peer in peers:
        pl.semaphore_signal(barrier, inc=1, device_id=peer, device_id_type=MESH)
    meanwhile()
    pl.semaphore_wait(barrier, len(peers))


def remote(src, dst, send, recv, peer):
    return pltpu.make_async_remote_copy(
        src_ref=src, dst_ref=dst, send_sem=send, recv_sem=recv, device_id=peer, device_id_type=MESH
    )


def plane_gather_start(z, at, send, recv):
    me, core, x, y, to_core, to_x, to_y, to_xy = place()
    plan = ((0, to_x, 0), (2, to_y, 1), (1, to_x, 1), (3, to_y, 0), (4, to_core, None))
    copies = {}
    for k, peer, half in plan:
        copies[k] = remote(at(me, half), at(me, half), send, recv.at[k], (peer, z))
        copies[k].start()
    return copies


def plane_gather_turn(z, at, send, recv, copies):
    me, core, x, y, to_core, to_x, to_y, to_xy = place()

    def forward(k, block, half, peer):
        copies[k] = remote(
            at(block, half), at(block, half), send, recv.at[k], (peer, z)
        )
        copies[k].start()

    copies[0].wait_recv()
    forward(5, to_x, 0, to_y)
    copies[2].wait_recv()
    forward(6, to_y, 1, to_x)
    copies[1].wait_recv()
    forward(7, to_x, None, to_core)
    copies[3].wait_recv()
    forward(8, to_y, None, to_core)


def plane_gather_finish(z, at, send, recv, copies, last=(4, 7, 8, 9)):
    me, core, x, y, to_core, to_x, to_y, to_xy = place()
    copies[5].wait_recv()
    copies[6].wait_recv()
    copies[9] = remote(
        at(to_xy, None), at(to_xy, None), send, recv.at[9], (to_core, z)
    )
    copies[9].start()
    for k in last:
        copies[k].wait_recv()


def drain(ref, semaphore):
    pltpu.make_async_copy(ref, ref, semaphore).wait()


def gather_reduce(
    n_shard, inverse, act_ref, cot_ref, gall, sqall, act, cot, turned, part, recv, plane, zrecv,
    in_sem, hop_r, swap_s, hop_s, pass_s, sum_s, sum_r, line_s, line_r,
):
    f32 = jnp.float32
    me, core, x, y, to_core, to_x, to_y, to_xy = place()
    z = lax.axis_index("shard")
    tokens = act_ref.shape[1]
    members, rows, cols = plane.shape[1:]
    near = z + 1 - 2 * lax.rem(z, 2)
    low = z < 2
    inner = (z == 1) | (z == 2)
    inward = jnp.where(low, z + 1, z - 1)
    targets = (jnp.where(low, 3, 0), jnp.where(low, 2, 1), near, z)
    cut = [pl.ds(pl.multiple_of(t * cols, cols), cols) for t in targets]
    counts = [c.shape[0] for c in cot]
    shared = counts[0] * 2
    mine = (counts[0] * x, shared + counts[1] * y)
    yours = (counts[0] * (1 - x), shared + counts[1] * (1 - y))
    peers = (to_x, to_y)
    layer_of = ((1 - y, y), (0,))
    keys = [(1, n_shard, 0), (0, n_shard, 0), (1, 0, 0), (0, 0, 0), (0, n_shard, 1), (0, 0, 1)]
    keys += [(kind, k, j) for k in range(1, n_shard) for kind, j in ((1, 0), (0, 0), (0, 1))]

    def index(kind, k, j):
        return 2 * k + j if kind == 0 else 2 * (n_shard + 1) + k

    def source(kind, k, layer):
        return cot_ref.at[layer] if k == n_shard else act_ref.at[layer, :, cut[k]]

    def slots(kind, k, j, first, count):
        layer = layer_of[kind][j]
        buffer = cot[kind].at[layer] if k == n_shard else act[kind].at[k, layer]
        return buffer.at[pl.ds(first * tokens, count * tokens)]

    own, swap, hop, onward = {}, {}, {}, {}
    for key in keys:
        kind, k, j = key
        at = in_sem.at[index(*key)]
        group = 2 * kind + (1 if k == n_shard else 0)
        layer = layer_of[kind][j]
        here = source(kind, k, mine[kind] + layer)
        own[key] = pltpu.make_async_copy(here, slots(*key, 0, 1), at)
        swap[key] = remote(here, slots(*key, 1, 1), swap_s.at[group], at, (to_core, z))
        hop[key] = remote(
            source(kind, k, yours[kind] + layer), slots(*key, 3, 1),
            hop_s.at[group], hop_r.at[index(*key)], (peers[kind], z),
        )
        onward[key] = remote(slots(*key, 3, 1), slots(*key, 2, 1), pass_s.at[group], at, (to_core, z))
    sums = [
        [
            remote(
                part[0].at[k, 1 - y], recv[0].at[k], sum_s.at[0], sum_r.at[0, k], (to_y, z)
            ),
            remote(
                part[1].at[k, 1 - x], recv[1].at[k], sum_s.at[1], sum_r.at[1, k], (to_x, z)
            ),
        ]
        for k in range(n_shard)
    ]
    spans = (pl.ds(0, members - 1), pl.ds(members - 1, 1))
    lines = [
        [
            remote(
                plane.at[k, spans[kind]],
                zrecv.at[k if k == 2 else k + 3 * inner.astype(jnp.int32), spans[kind]],
                line_s.at[kind],
                line_r.at[k if k == 2 else k + 3 * inner.astype(jnp.int32), kind],
                (me, near if k == 2 else inward),
            )
            for kind in range(2)
        ]
        for k in range(n_shard - 1)
    ]

    def arrived(s, kind):
        remote(
            plane.at[0, spans[kind]], zrecv.at[s, spans[kind]], line_s.at[kind], line_r.at[s, kind],
            (me, near),
        ).wait_recv()

    def enter():
        for key in keys:
            own[key].start()

    def begin():
        for key in keys[:9]:
            hop[key].start()
        for key in keys:
            swap[key].start()

    def take(kind, k, j=0):
        hop[kind, k, j].wait_recv()
        onward[kind, k, j].start()

    def ready(kind, k, j):
        drain(slots(kind, k, j, 0, 3), in_sem.at[index(kind, k, j)])

    def turn(kind, j=0):
        ready(kind, n_shard, j)
        layer = layer_of[kind][j]
        for side in range(2):
            at = pl.ds(pl.multiple_of((2 * side + core) * rows, rows), rows)
            turned[kind][layer, side] = cot[kind][layer, :, at].T

    def product(kind, k, j=0):
        ready(kind, k, j)
        layer = layer_of[kind][j]

        def one(side, carry):
            value = jnp.dot(turned[kind][layer, side], act[kind][k, layer], preferred_element_type=f32)
            if kind == 0:
                part[0][k, layer, side] = value.astype(part[0].dtype)
            else:
                part[1][k, side, 0] = value.astype(part[1].dtype)
            return carry

        lax.fori_loop(0, 2, one, 0)
        if j == 0:
            sums[k][kind].start()

    def gather(kind, k):
        sums[k][kind].wait_recv()
        for i in range(members - 1 if kind == 0 else 1):
            kept = part[0][k, y, i] if kind == 0 else part[1][k, x, i]
            value = kept.astype(f32) + recv[kind][k, i].astype(f32)
            plane[k, i if kind == 0 else members - 1] = value.astype(plane.dtype)

    def release(kind, k):
        @pl.when(jnp.logical_not(inner))
        def _():
            lines[k][kind].start()

    def forward(kind, k):
        s = 3 if k == 2 else k

        @pl.when(inner)
        def _():
            arrived(s, kind)
            for i in range(members - 1) if kind == 0 else (members - 1,):
                value = plane[k, i].astype(f32) + zrecv[s, i].astype(f32)
                plane[k, i] = value.astype(plane.dtype)
            lines[k][kind].start()

    def run():
        take(1, n_shard)
        take(0, n_shard, 0)
        turn(1)
        take(1, 0)
        take(0, 0, 0)
        turn(0, 0)
        product(1, 0)
        hop[0, 2, 0].start()
        product(0, 0, 0)
        hop[1, 2, 0].start()
        take(1, 1)
        take(0, n_shard, 1)
        product(1, 1)
        hop[0, 2, 1].start()
        hop[0, 3, 0].start()
        turn(0, 1)
        take(0, 0, 1)
        product(0, 0, 1)
        take(0, 1, 0)
        product(0, 1, 0)
        hop[1, 3, 0].start()
        gather(0, 0)
        release(0, 0)
        take(0, 1, 1)
        product(0, 1, 1)
        take(1, 2)
        product(1, 2)
        hop[0, 3, 1].start()
        gather(1, 0)
        release(1, 0)
        take(0, 2, 0)
        product(0, 2, 0)
        gather(0, 1)
        release(0, 1)
        forward(0, 0)
        gather(1, 1)
        release(1, 1)
        forward(1, 0)
        take(1, 3)
        product(1, 3)
        take(0, 2, 1)
        product(0, 2, 1)
        take(0, 3, 0)
        product(0, 3, 0)
        gather(0, 2)
        release(0, 2)
        forward(0, 1)
        forward(0, 2)
        gather(1, 2)
        release(1, 2)
        forward(1, 1)
        forward(1, 2)
        take(0, 3, 1)
        product(0, 3, 1)
        gather(1, 3)
        gather(0, 3)
        for kind in range(2):
            arrived(2, kind)
        home = lax.div(me, 2)
        half = pl.ds(pl.multiple_of(core * rows, rows), rows)

        def add_last(others, j):
            value = plane[n_shard - 1, j].astype(f32)
            for s in others:
                value = value + zrecv[s, j].astype(f32)
            value = (value * inverse).astype(gall.dtype)
            gall[home, j, half] = value
            value = value.astype(f32)
            line = jnp.sum(value * value, axis=0, keepdims=True)
            lanes = sqall.shape[-1]
            fold = line[:, :lanes]
            for i in range(1, cols // lanes):
                fold = fold + line[:, i * lanes : (i + 1) * lanes]
            sqall[me * n_shard + z, j] = fold

        @pl.when(inner)
        def _():
            for kind in range(2):
                arrived(4, kind)
            for j in range(members):
                add_last((2, 4), j)

        @pl.when(jnp.logical_not(inner))
        def _():
            for j in range(members):
                add_last((2,), j)

    def leave():
        for kind in range(2):
            for pool in (swap_s, hop_s, pass_s):
                drain(act[kind].at[:, :, pl.ds(0, tokens)], pool.at[2 * kind])
                drain(cot[kind].at[:, pl.ds(0, tokens)], pool.at[2 * kind + 1])
            drain(recv[kind], sum_s.at[kind])
            drain(plane.at[pl.ds(0, n_shard - 1), spans[kind]], line_s.at[kind])

    return enter, begin, run, leave


HOMES = ((2, 0), (1, 0), (1, 1))


def block_at(ref, axis, rows):
    def at(r, half):
        count = rows if half is None else rows // 2
        start = lax.rem(r, 2) * rows + (0 if half is None else half * count)
        cut = pl.ds(pl.multiple_of(start, count), count)
        block = lax.div(r, 2)
        return ref.at[block, cut] if axis == 1 else ref.at[block, :, cut]

    return at


def split(value):
    high = value.astype(jnp.bfloat16)
    return high, (value - high.astype(jnp.float32)).astype(jnp.bfloat16)


def times(left, right):
    dot = functools.partial(jnp.dot, preferred_element_type=jnp.float32)
    return dot(left[0], right[0]) + (dot(left[0], right[1]) + dot(left[1], right[0]))


def gram_iteration(gram, scale, gram_scr, root_scr):
    n = gram.shape[0]
    row = lax.broadcasted_iota(jnp.int32, (n, n), 0)
    col = lax.broadcasted_iota(jnp.int32, (n, n), 1)
    eye = (row == col).astype(jnp.float32)
    trace = jnp.sum(jnp.sum(gram * eye, axis=0, keepdims=True), axis=1, keepdims=True)
    inverse = 1.0 / (jnp.sqrt(trace) + epsilon)
    gram_scr[...] = gram * inverse * inverse
    for iteration in range(ITERS):
        a = split(gram_scr[...])
        mixing = coef_b * gram_scr[...] + coef_c * times(a, a)
        b = split(mixing)
        if iteration == 0:
            root_scr[...] = coef_a * eye + mixing
        else:
            root_scr[...] = coef_a * root_scr[...] + times(b, split(root_scr[...]))
        if iteration < ITERS - 1:
            half = coef_a * gram_scr[...] + times(b, a)
            gram_scr[...] = coef_a * half + times(b, split(half))
    return root_scr[...] * (inverse * scale)


def muon_kernel(
    n_shard, inverse, scale, owner_ref, start_ref, act_ref, cot_ref, momentum_hbm,
    mout_ref, u_ref, wall_ref, qall_ref,
    momentum, gall, sqall, table, factor, uown, held, gram_out, gram_in, gram_scr, root_scr, root,
    act, cot, turned, part, recv, plane, zrecv, reduce_sems,
    load, ps, pr, gs, gr, as_, ar, ws, wr, os_, or_, rs, rr, hs, hr,
):
    f32, bf16 = jnp.float32, jnp.bfloat16
    me, core, x, y, to_core, to_x, to_y, to_xy = place()
    z = lax.axis_index("shard")
    base = me - core
    block = lax.div(me, 2)
    members = gall.shape[1]
    rows, cols = held.shape[1:]
    lanes = sqall.shape[-1]
    mine = pl.ds(pl.multiple_of(core * rows, rows), rows)

    fetch = pltpu.make_async_copy(momentum_hbm, momentum, load)
    enter, begin, run, leave = gather_reduce(
        n_shard, inverse, act_ref, cot_ref, gall, sqall, act, cot, turned, part, recv,
        plane, zrecv, *reduce_sems,
    )
    everyone = n_shard * 2 * gall.shape[0]
    here = me * n_shard + z
    others = [lax.rem(here + t, everyone) for t in range(1, everyone)]
    others = [(lax.div(to, n_shard), lax.rem(to, n_shard)) for to in others]
    greet(others, enter)

    begin()
    fetch.start()
    run()

    for peer in others:
        remote(sqall.at[here], sqall.at[here], ps, pr, peer).start()
    at_g = block_at(gall, 2, rows)
    gathers = plane_gather_start(z, at_g, gs, gr)
    fetch.wait()
    drain(sqall.at[pl.ds(0, everyone - 1)], pr)

    table[...] = jnp.zeros_like(table)
    for m in range(MATS):
        layer, side = divmod(m, 2)
        bx, by = divmod(layer, 2) if m < 8 else (side, layer - 4)
        j, i = 2 * by + bx, side if m < 8 else 2
        line = sqall[2 * j * n_shard, i]
        for d in range(1, 2 * n_shard):
            line = line + sqall[2 * j * n_shard + d, i]
        table[pl.ds(m, 1)] = line
    index = lax.broadcasted_iota(jnp.int32, table.shape, 0)
    bucket = jnp.zeros(table.shape, jnp.int32)
    for k in range(start_ref.shape[0]):
        bucket = bucket + (index >= start_ref[k]).astype(jnp.int32)
    sums = table[...]
    clip = jnp.zeros(table.shape, f32)
    for k in range(start_ref.shape[0] + 1):
        inside = (bucket == k) & (index < MATS)
        total = jnp.sum(jnp.where(inside, sums, 0.0), axis=(0, 1), keepdims=True)
        count = jnp.sum(inside.astype(f32), axis=(0, 1), keepdims=True) / lanes
        mean = total / (jnp.maximum(count, 1.0) * (2 * rows) * (n_shard * cols))
        clip = jnp.where(inside, jnp.minimum(1.0, clip_level / jnp.sqrt(mean + epsilon)), clip)
    for m in range(MATS):
        factor[m] = jnp.concatenate([clip[m : m + 1, :]] * (cols // lanes), axis=1)

    def advance(matrix, gradient, past):
        step = factor[matrix] * gradient.astype(f32)
        new = momentum_rate * past + step
        return new, (step + momentum_rate * new).astype(bf16)

    gathers[4].wait_recv()
    for i in range(members):
        layer, side = lodged(block, i)
        matrix = 2 * layer + side
        uown[i] = advance(matrix, gall[block, i], momentum[matrix])[1]
    over = (((1,), (1,)), ((), ()))
    parts = []
    for i, (hz, hc) in enumerate(HOMES):
        here = (z == hz) & (core == hc)
        owner = (base + hc, hz)
        low = uown[i, :rows]
        high = uown[i, rows:]
        own = jnp.where(core == 0, low, high)
        diag = lax.dot_general(own, own, over, preferred_element_type=f32)
        gram_out[i, 0] = diag
        part = remote(gram_out.at[i, 0], gram_in.at[z, core], as_.at[i, 0], ar.at[z, core], owner)
        cross = remote(gram_out.at[i, 1], gram_in.at[z, 2], as_.at[i, 1], ar.at[z, 2], owner)
        parts.append((here, part, cross))

        @pl.when(here)
        def _():
            gram_in[z, core] = diag

        @pl.when(jnp.logical_not(here))
        def _():
            part.start()

        @pl.when(core == 0)
        def _():
            off = lax.dot_general(low, high, over, preferred_element_type=f32)
            gram_out[i, 1] = off

            @pl.when(here)
            def _():
                gram_in[z, 2] = off

            @pl.when(jnp.logical_not(here))
            def _():
                cross.start()

    plane_gather_turn(z, at_g, gs, gr, gathers)
    plane_gather_finish(z, at_g, gs, gr, gathers, last=(7, 8, 9))

    def slot_matrix(shard, slot):
        found = jnp.int32(0)
        count = jnp.int32(0)
        for m in range(MATS):
            yes = owner_ref[m] == shard
            found = jnp.where(yes & (count == slot), m, found)
            count = count + yes.astype(jnp.int32)
        return found

    sends = {}

    def send_slice(d):
        shard = lax.rem(z + d, n_shard)
        matrix = slot_matrix(shard, block)
        home, member = lodging(matrix)
        held[d - 1] = advance(matrix, gall[home, member, mine], momentum[matrix, mine])[1]
        sends[d] = remote(
            held.at[d - 1], wall_ref.at[n_shard - d - 1, block, mine], ws, wr.at[d - 1], (me, shard)
        )
        sends[d].start()

    send_slice(1)
    send_slice(3)

    def all_one(m, carry):
        home, member = lodging(m)
        new, turned = advance(m, gall[home, member], momentum[m])
        mout_ref[m] = new
        u_ref[m] = turned
        return carry

    is_home = functools.reduce(jnp.logical_or, [here for here, _, _ in parts])
    member = jnp.where(z == HOMES[0][0], 0, 1 + core)
    roots = []
    packed = root.shape[0] // 2
    mine_q = pl.ds(pl.multiple_of(core * packed, packed), packed)
    for d in range(n_shard):
        for c in range(2):
            if d == 0 and c == 1:
                continue
            peer = (to_core, z) if d == 0 else (base + c, lax.rem(z + d, n_shard))
            half = 1 - core if d == 0 else c
            cut = pl.ds(pl.multiple_of(half * packed, packed), packed)
            roots.append(remote(root.at[cut], qall_ref.at[block, member, cut], rs, rr.at[member], peer))

    @pl.when(is_home)
    def _():
        for d in range(n_shard):
            for k in range(3):
                source = remote(gram_out.at[0, 0], gram_in.at[d, k], as_.at[0, 0], ar.at[d, k], (to_core, z))
                local = (z == d) & ((core == k) if k < 2 else (core == 0))

                @pl.when(jnp.logical_not(local))
                def _():
                    source.wait_recv()

        blocks = []
        for k in range(3):
            value = gram_in[0, k]
            for d in range(1, n_shard):
                value = value + gram_in[d, k]
            blocks.append(value)
        top = jnp.concatenate([blocks[0], blocks[2]], axis=1)
        bottom = jnp.concatenate([blocks[2].T, blocks[1]], axis=1)
        result = gram_iteration(jnp.concatenate([top, bottom], axis=0), scale, gram_scr, root_scr)
        result = result.astype(bf16)
        root[:rows] = result[:rows, :rows]
        root[rows:packed] = result[: rows // 2, rows:]
        root[packed : packed + rows] = result[rows:, rows:]
        root[packed + rows :] = result[rows // 2 : rows, rows:]
        for c in roots:
            c.start()
        qall_ref[block, member, mine_q] = root[mine_q]

    walls = {}

    def at_w(d):
        return block_at(wall_ref.at[n_shard - d - 1], 1, rows)

    for d in (1, 3):
        sends[d].wait_recv()
        walls[d] = plane_gather_start(z, at_w(d), os_.at[d - 1], or_.at[d - 1])
    send_slice(2)
    lax.fori_loop(0, MATS, all_one, 0)
    for d in (1, 3):
        plane_gather_turn(z, at_w(d), os_.at[d - 1], or_.at[d - 1], walls[d])
    for i, (here, _, _) in enumerate(parts):
        arrival = remote(root.at[mine_q], qall_ref.at[block, i, mine_q], rs, rr.at[i], (to_core, z))

        @pl.when(jnp.logical_not(here))
        def _():
            arrival.wait_recv()

    at_q = block_at(qall_ref, 2, packed)
    gathers_q = plane_gather_start(z, at_q, hs, hr)
    sends[2].wait_recv()
    walls[2] = plane_gather_start(z, at_w(2), os_.at[1], or_.at[1])
    for d in (1, 3):
        plane_gather_finish(z, at_w(d), os_.at[d - 1], or_.at[d - 1], walls[d])
    plane_gather_turn(z, at_q, hs, hr, gathers_q)
    plane_gather_turn(z, at_w(2), os_.at[1], or_.at[1], walls[2])
    plane_gather_finish(z, at_q, hs, hr, gathers_q)
    plane_gather_finish(z, at_w(2), os_.at[1], or_.at[1], walls[2])
    most = pl.ds(0, 2 * rows - rows // 4)
    drain(gall.at[:, :, most], gs)
    drain(qall_ref.at[:, :, pl.ds(0, 2 * packed - packed // 4)], hs)
    for d in range(n_shard - 1):
        drain(wall_ref.at[d, :, most], os_.at[d])
    drain(held, ws)
    drain(sqall.at[pl.ds(0, everyone - 1)], ps)

    @pl.when(is_home)
    def _():
        drain(u_ref.at[pl.ds(0, len(roots)), pl.ds(0, packed * rows // cols)], rs)

    for here, part, cross in parts:

        @pl.when(jnp.logical_not(here))
        def _():
            part.wait_send()

            @pl.when(core == 0)
            def _():
                cross.wait_send()

    leave()


def finish_kernel(
    owner_ref, mout_ref, u_ref, wall_ref, qall_ref, mom_out, update_out, owned_out,
    ubuf, wbuf, qbuf, msem, usem, wsem,
):
    f32 = jnp.float32
    slots, _, width = wbuf.shape
    mats, _, cols = ubuf.shape
    n_shard = width // cols
    rows = qall_ref.shape[-1]
    z = lax.axis_index("shard")

    def put(buf, out, sem, m):
        return pltpu.make_async_copy(buf.at[m], out.at[m], sem)

    for m in range(mats):
        put(mout_ref, mom_out, msem, m).start()

    def update_one(m, carry):
        home, member = lodging(m)
        q = qall_ref[home, member]
        cross = jnp.concatenate([q[rows : 3 * rows // 2], q[5 * rows // 2 :]], axis=0)
        qbuf[m, :rows, :rows] = q[:rows]
        qbuf[m, :rows, rows:] = cross
        qbuf[m, rows:, :rows] = cross.T
        qbuf[m, rows:, rows:] = q[3 * rows // 2 : 5 * rows // 2]
        ubuf[m] = jnp.dot(qbuf[m], u_ref[m], preferred_element_type=f32)
        put(ubuf, update_out, usem, m).start()
        return carry

    lax.fori_loop(0, mats, update_one, 0, unroll=3)

    def owned_one(s, carry):
        matrix = jnp.int32(0)
        count = jnp.int32(0)
        for m in range(mats):
            yes = owner_ref[m] == z
            matrix = jnp.where(yes & (count == s), m, matrix)
            count = count + yes.astype(jnp.int32)
        keep = (count > s).astype(f32)
        q = qbuf[matrix]
        for d in range(n_shard):
            right = u_ref[matrix] if d == 0 else wall_ref[d - 1, s]
            value = jnp.dot(q, right, preferred_element_type=f32) * keep
            at = lax.rem(z + d, n_shard)
            wbuf[s, :, pl.ds(pl.multiple_of(at * cols, cols), cols)] = value.astype(wbuf.dtype)
        put(wbuf, owned_out, wsem, s).start()
        return carry

    lax.fori_loop(0, slots, owned_one, 0, unroll=2)

    drain(mout_ref, msem)
    drain(ubuf, usem)
    drain(wbuf, wsem)


def per_device_planes(activations, cotangents, momentum, owners, bucket_starts):
    n_shard = lax.axis_size("shard")
    n_rep = lax.axis_size("rep")
    layers, tok_rows, width = activations.shape
    token_total = tok_rows * n_shard * n_rep
    cols = width // n_shard
    rows = KV // 2
    lanes = math.gcd(cols, 128)
    groups = n_rep // 2
    members = MATS // groups
    slots = -(-MATS // n_shard) + 1
    update_scale = math.sqrt(max(KV, D))
    bf16, f32 = jnp.bfloat16, jnp.float32

    def params(limit, **rest):
        return pltpu.CompilerParams(vmem_limit_bytes=limit * 1024 * 1024, **rest)

    dma = pltpu.SemaphoreType.DMA
    tokens = 4 * tok_rows
    shares = (layers // 3, layers // 6)
    hbm = functools.partial(pltpu.with_memory_space_constraint, memory_space=pltpu.HBM)
    mout, turned, wall, qall = pl.pallas_call(
        functools.partial(muon_kernel, n_shard, 1.0 / math.sqrt(token_total), update_scale),
        out_shape=(
            pltpu.VMEM((MATS, KV, cols), f32),
            pltpu.VMEM((MATS, KV, cols), bf16),
            pltpu.VMEM((n_shard - 1, slots, KV, cols), bf16),
            pltpu.VMEM((groups, members, 3 * rows, rows), bf16),
        ),
        in_specs=[SMEM_SPEC, SMEM_SPEC, ANY_SPEC, ANY_SPEC, ANY_SPEC],
        out_specs=(VMEM_SPEC,) * 4,
        scratch_shapes=[
            pltpu.VMEM((MATS, KV, cols), f32),
            pltpu.VMEM((groups, members, KV, cols), bf16),
            pltpu.VMEM((n_rep * n_shard, members, 1, lanes), f32),
            pltpu.VMEM((16, lanes), f32),
            pltpu.VMEM((MATS, 1, cols), f32),
            pltpu.VMEM((members, KV, cols), bf16),
            pltpu.VMEM((n_shard - 1, rows, cols), bf16),
            pltpu.VMEM((members, 2, rows, rows), f32),
            pltpu.VMEM((n_shard, 3, rows, rows), f32),
            pltpu.VMEM((KV, KV), f32),
            pltpu.VMEM((KV, KV), f32),
            pltpu.VMEM((3 * rows, rows), bf16),
            [pltpu.VMEM((n_shard, n, tokens, cols), bf16) for n in shares],
            [pltpu.VMEM((n, tokens, 2 * KV), bf16) for n in shares],
            [pltpu.VMEM((n, 2, rows, tokens), bf16) for n in shares],
            [pltpu.VMEM((n_shard, 2, n, rows, cols), bf16) for n in shares],
            [pltpu.VMEM((n_shard, n, rows, cols), bf16) for n in shares],
            pltpu.VMEM((n_shard, members, rows, cols), bf16),
            pltpu.VMEM((n_shard + 1, members, rows, cols), bf16),
            [dma((3 * n_shard + 3,)) for _ in range(2)]
            + [dma((4,)) for _ in range(3)]
            + [dma((2,)), dma((2, n_shard)), dma((2,)), dma((n_shard + 1, 2))],
            dma(()),
            dma(()), dma(()),
            dma(()), dma((10,)),
            dma((members, 2)), dma((n_shard, 3)),
            dma(()), dma((n_shard - 1,)),
            dma((n_shard - 1,)), dma((n_shard - 1, 10)),
            dma(()), dma((members,)),
            dma(()), dma((10,)),
        ],
        compiler_params=params(48, has_side_effects=True, collective_id=0),
        name="muon",
    )(owners, bucket_starts, hbm(activations), hbm(cotangents), hbm(momentum))

    return pl.pallas_call(
        finish_kernel,
        out_shape=(
            jax.ShapeDtypeStruct(momentum.shape, f32),
            jax.ShapeDtypeStruct(momentum.shape, f32),
            jax.ShapeDtypeStruct((slots, KV, width), bf16),
        ),
        in_specs=[SMEM_SPEC] + [VMEM_SPEC] * 4,
        out_specs=(ANY_SPEC,) * 3,
        scratch_shapes=[
            pltpu.VMEM(momentum.shape, f32),
            pltpu.VMEM((slots, KV, width), bf16),
            pltpu.VMEM((MATS, KV, KV), bf16),
            dma(()), dma(()), dma(()),
        ],
        compiler_params=params(20),
        name="finish",
    )(owners, mout, turned, wall, qall)


def solution(mesh):
    groups = mesh.shape["rep"] // 2
    slots = -(-MATS // mesh.shape["shard"]) + 1
    fits = mesh.shape["rep"] == 8 and mesh.shape["shard"] == 4 and slots <= groups
    placed = (
        P(None, ("rep", "shard"), None),
        P(None, ("rep", "shard"), None),
        P(None, None, "shard"),
        P(),
        P(),
    )
    return jax.shard_map(
        per_device_planes if fits else per_device_general,
        mesh=mesh,
        in_specs=placed,
        out_specs=(P(None, None, "shard"), P(None, None, "shard"), P("shard", None, None)),
        check_vma=False,
    )
```

```python
import functools
import math

import jax
import jax.numpy as jnp
from jax import lax
from jax.experimental import pallas as pl
from jax.experimental.pallas import tpu as pltpu
from jax.sharding import PartitionSpec as P

D = 2048
KV = 256
ITERS = 5
MATS = 12
MESH = pl.DeviceIdType.MESH
VMEM_SPEC = pl.BlockSpec(memory_space=pltpu.VMEM)
SMEM_SPEC = pl.BlockSpec(memory_space=pltpu.SMEM)
ANY_SPEC = pl.BlockSpec(memory_space=pl.ANY)
VMEM_LIMIT = 60 * 1024 * 1024

coef_a = 3.4445
coef_b = -4.775
coef_c = 2.0315
momentum_rate = 0.95
clip_level = 0.5
epsilon = 1e-06


def orthogonal_batch(matrices):
    values = matrices.astype(jnp.float32)
    frobenius = jnp.sqrt(jnp.sum(values * values, axis=(1, 2), keepdims=True))
    matrix = (values / (frobenius + epsilon)).astype(jnp.bfloat16)
    for iteration in range(ITERS):
        gram_matrix = jnp.einsum(
            "skd,sjd->skj", matrix, matrix, preferred_element_type=jnp.float32
        ).astype(jnp.bfloat16)
        square = jnp.einsum(
            "skj,sji->ski", gram_matrix, gram_matrix, preferred_element_type=jnp.float32
        )
        mixing = (coef_b * gram_matrix.astype(jnp.float32) + coef_c * square).astype(jnp.bfloat16)
        product = jnp.einsum("skj,sjd->skd", mixing, matrix, preferred_element_type=jnp.float32)
        matrix = (coef_a * matrix.astype(jnp.float32) + product).astype(jnp.bfloat16)
    return matrix


def clip_factors(square_sums, bucket_starts):
    indices = jnp.arange(MATS, dtype=jnp.int32)
    buckets = jnp.sum((indices[:, None] >= bucket_starts[None, :]).astype(jnp.int32), axis=1)
    together = (buckets[:, None] == buckets[None, :]).astype(jnp.float32)
    totals = jnp.sum(together * square_sums[None, :], axis=1)
    members = jnp.sum(together, axis=1)
    root_mean = jnp.sqrt(totals / (members * KV * D) + epsilon)
    return jnp.minimum(1.0, clip_level / root_mean)


def slot_numbers(owners):
    indices = jnp.arange(MATS, dtype=jnp.int32)
    earlier = (indices[None, :] < indices[:, None]) & (owners[None, :] == owners[:, None])
    return jnp.sum(earlier.astype(jnp.int32), axis=1)


def selector(owner_of, slot_of, shard_count, slot_count):
    holders = lax.broadcasted_iota(jnp.int32, (shard_count, slot_count, 1), 0)
    places = lax.broadcasted_iota(jnp.int32, (shard_count, slot_count, 1), 1)
    chosen = (holders == owner_of[None, None, :]) & (places == slot_of[None, None, :])
    return chosen.astype(jnp.bfloat16)


def pack_slots(shards, chooser):
    return jnp.einsum("psm,mkd->skpd", chooser, shards, preferred_element_type=jnp.float32).astype(
        jnp.bfloat16
    )


def unpack_slots(received, chooser):
    return jnp.einsum("psm,skpd->mkd", chooser, received, preferred_element_type=jnp.float32)


def per_device_general(activations, cotangents, momentum, owners, bucket_starts):
    shard_count = lax.axis_size("shard")
    replica_count = lax.axis_size("rep")
    layers, tok_rows, width = activations.shape
    token_total = tok_rows * shard_count * replica_count
    columns = width // shard_count
    slot_count = -(-MATS // shard_count) + 1
    update_scale = math.sqrt(max(KV, D))
    partial_terms = jnp.einsum(
        "ltk,ltd->lkd", cotangents, activations, preferred_element_type=jnp.float32
    ).reshape(MATS, KV, width)
    shard_part = lax.psum_scatter(
        partial_terms.astype(jnp.bfloat16), "shard", scatter_dimension=2, tiled=True
    )
    summed = lax.psum(shard_part, "rep").astype(jnp.float32)
    gradient = summed / jnp.sqrt(jnp.float32(token_total))
    square_sums = lax.psum(jnp.sum(gradient * gradient, axis=(1, 2)), "shard")
    factors = clip_factors(square_sums, bucket_starts)
    momentum_out = momentum_rate * momentum + factors[:, None, None] * gradient
    nesterov = (factors[:, None, None] * gradient + momentum_rate * momentum_out).astype(
        jnp.bfloat16
    )
    slot_of = slot_numbers(owners)
    chooser = selector(owners, slot_of, shard_count, slot_count)
    received = lax.all_to_all(
        pack_slots(nesterov, chooser), "shard", split_axis=2, concat_axis=2, tiled=True
    )
    item_count = received.shape[0]
    result = orthogonal_batch(received.reshape(item_count, KV, width))
    scaled = (update_scale * result.astype(jnp.float32)).astype(jnp.bfloat16)
    returned_part = lax.all_to_all(
        result.reshape(item_count, KV, shard_count, columns),
        "shard",
        split_axis=2,
        concat_axis=2,
        tiled=True,
    )
    update = update_scale * unpack_slots(returned_part, chooser)
    return (momentum_out, update, scaled)


def lodged(block, member):
    x = lax.rem(block, 2)
    y = lax.div(block, 2)
    whole = 2 * x + y
    paired = 4 + y
    return jnp.where(member < 2, whole, paired), jnp.where(member < 2, member, x)


def lodging(matrix):
    layer = lax.div(matrix, 2)
    side = lax.rem(matrix, 2)
    early = matrix < 8
    x = jnp.where(early, lax.div(layer, 2), side)
    y = jnp.where(early, lax.rem(layer, 2), layer - 4)
    return 2 * y + x, jnp.where(early, side, 2)


def place():
    me = lax.axis_index("rep")
    core = lax.rem(me, 2)
    x = lax.rem(lax.div(me, 2), 2)
    y = lax.div(me, 4)
    to_core = me + 1 - 2 * core
    to_x = me + 2 - 4 * x
    to_y = me + 4 - 8 * y
    to_xy = me + 6 - 4 * x - 8 * y
    return me, core, x, y, to_core, to_x, to_y, to_xy


def greet(peers, meanwhile):
    barrier = pltpu.get_barrier_semaphore()
    for peer in peers:
        pl.semaphore_signal(barrier, inc=1, device_id=peer, device_id_type=MESH)
    meanwhile()
    pl.semaphore_wait(barrier, len(peers))


def remote(src, dst, send, recv, peer):
    return pltpu.make_async_remote_copy(
        src_ref=src, dst_ref=dst, send_sem=send, recv_sem=recv, device_id=peer, device_id_type=MESH
    )


def plane_gather_start(z, at, send, recv):
    me, core, x, y, to_core, to_x, to_y, to_xy = place()
    plan = ((0, to_x, 0), (2, to_y, 1), (1, to_x, 1), (3, to_y, 0), (4, to_core, None))
    copies = {}
    for k, peer, half in plan:
        copies[k] = remote(at(me, half), at(me, half), send, recv.at[k], (peer, z))
        copies[k].start()
    return copies


def plane_gather_turn(z, at, send, recv, copies):
    me, core, x, y, to_core, to_x, to_y, to_xy = place()

    def forward(k, block, half, peer):
        copies[k] = remote(
            at(block, half), at(block, half), send, recv.at[k], (peer, z)
        )
        copies[k].start()

    copies[0].wait_recv()
    forward(5, to_x, 0, to_y)
    copies[2].wait_recv()
    forward(6, to_y, 1, to_x)
    copies[1].wait_recv()
    forward(7, to_x, None, to_core)
    copies[3].wait_recv()
    forward(8, to_y, None, to_core)


def plane_gather_finish(z, at, send, recv, copies, last=(4, 7, 8, 9)):
    me, core, x, y, to_core, to_x, to_y, to_xy = place()
    copies[5].wait_recv()
    copies[6].wait_recv()
    copies[9] = remote(
        at(to_xy, None), at(to_xy, None), send, recv.at[9], (to_core, z)
    )
    copies[9].start()
    for k in last:
        copies[k].wait_recv()


def drain(ref, semaphore):
    pltpu.make_async_copy(ref, ref, semaphore).wait()


def gather_reduce(
    n_shard, inverse, act_ref, cot_ref, gall, sqall, act, cot, turned, part, recv, plane, zrecv,
    in_sem, hop_r, swap_s, hop_s, pass_s, sum_s, sum_r, line_s, line_r,
):
    f32 = jnp.float32
    me, core, x, y, to_core, to_x, to_y, to_xy = place()
    z = lax.axis_index("shard")
    tokens = act_ref.shape[1]
    members, rows, cols = plane.shape[1:]
    near = z + 1 - 2 * lax.rem(z, 2)
    low = z < 2
    inner = (z == 1) | (z == 2)
    inward = jnp.where(low, z + 1, z - 1)
    targets = (jnp.where(low, 3, 0), jnp.where(low, 2, 1), near, z)
    cut = [pl.ds(pl.multiple_of(t * cols, cols), cols) for t in targets]
    counts = [c.shape[0] for c in cot]
    shared = counts[0] * 2
    mine = (counts[0] * x, shared + counts[1] * y)
    yours = (counts[0] * (1 - x), shared + counts[1] * (1 - y))
    peers = (to_x, to_y)
    layer_of = ((1 - y, y), (0,))
    keys = [(1, n_shard, 0), (0, n_shard, 0), (1, 0, 0), (0, 0, 0), (0, n_shard, 1), (0, 0, 1)]
    keys += [(kind, k, j) for k in range(1, n_shard) for kind, j in ((1, 0), (0, 0), (0, 1))]

    def index(kind, k, j):
        return 2 * k + j if kind == 0 else 2 * (n_shard + 1) + k

    def source(kind, k, layer):
        return cot_ref.at[layer] if k == n_shard else act_ref.at[layer, :, cut[k]]

    def slots(kind, k, j, first, count):
        layer = layer_of[kind][j]
        buffer = cot[kind].at[layer] if k == n_shard else act[kind].at[k, layer]
        return buffer.at[pl.ds(first * tokens, count * tokens)]

    own, swap, hop, onward = {}, {}, {}, {}
    for key in keys:
        kind, k, j = key
        at = in_sem.at[index(*key)]
        group = 2 * kind + (1 if k == n_shard else 0)
        layer = layer_of[kind][j]
        here = source(kind, k, mine[kind] + layer)
        own[key] = pltpu.make_async_copy(here, slots(*key, 0, 1), at)
        swap[key] = remote(here, slots(*key, 1, 1), swap_s.at[group], at, (to_core, z))
        hop[key] = remote(
            source(kind, k, yours[kind] + layer), slots(*key, 3, 1),
            hop_s.at[group], hop_r.at[index(*key)], (peers[kind], z),
        )
        onward[key] = remote(slots(*key, 3, 1), slots(*key, 2, 1), pass_s.at[group], at, (to_core, z))
    sums = [
        [
            remote(
                part[0].at[k, 1 - y], recv[0].at[k], sum_s.at[0], sum_r.at[0, k], (to_y, z)
            ),
            remote(
                part[1].at[k, 1 - x], recv[1].at[k], sum_s.at[1], sum_r.at[1, k], (to_x, z)
            ),
        ]
        for k in range(n_shard)
    ]
    spans = (pl.ds(0, members - 1), pl.ds(members - 1, 1))
    lines = [
        [
            remote(
                plane.at[k, spans[kind]],
                zrecv.at[k if k == 2 else k + 3 * inner.astype(jnp.int32), spans[kind]],
                line_s.at[kind],
                line_r.at[k if k == 2 else k + 3 * inner.astype(jnp.int32), kind],
                (me, near if k == 2 else inward),
            )
            for kind in range(2)
        ]
        for k in range(n_shard - 1)
    ]

    def arrived(s, kind):
        remote(
            plane.at[0, spans[kind]], zrecv.at[s, spans[kind]], line_s.at[kind], line_r.at[s, kind],
            (me, near),
        ).wait_recv()

    def enter():
        for key in keys:
            own[key].start()

    def begin():
        for key in keys[:9]:
            hop[key].start()
        for key in keys:
            swap[key].start()

    def take(kind, k, j=0):
        hop[kind, k, j].wait_recv()
        onward[kind, k, j].start()

    def ready(kind, k, j):
        drain(slots(kind, k, j, 0, 3), in_sem.at[index(kind, k, j)])

    def turn(kind, j=0):
        ready(kind, n_shard, j)
        layer = layer_of[kind][j]
        for side in range(2):
            at = pl.ds(pl.multiple_of((2 * side + core) * rows, rows), rows)
            turned[kind][layer, side] = cot[kind][layer, :, at].T

    def product(kind, k, j=0):
        ready(kind, k, j)
        layer = layer_of[kind][j]

        def one(side, carry):
            value = jnp.dot(turned[kind][layer, side], act[kind][k, layer], preferred_element_type=f32)
            if kind == 0:
                part[0][k, layer, side] = value.astype(part[0].dtype)
            else:
                part[1][k, side, 0] = value.astype(part[1].dtype)
            return carry

        lax.fori_loop(0, 2, one, 0)
        if j == 0:
            sums[k][kind].start()

    def gather(kind, k):
        sums[k][kind].wait_recv()
        for i in range(members - 1 if kind == 0 else 1):
            kept = part[0][k, y, i] if kind == 0 else part[1][k, x, i]
            value = kept.astype(f32) + recv[kind][k, i].astype(f32)
            plane[k, i if kind == 0 else members - 1] = value.astype(plane.dtype)

    def release(kind, k):
        @pl.when(jnp.logical_not(inner))
        def _():
            lines[k][kind].start()

    def forward(kind, k):
        s = 3 if k == 2 else k

        @pl.when(inner)
        def _():
            arrived(s, kind)
            for i in range(members - 1) if kind == 0 else (members - 1,):
                value = plane[k, i].astype(f32) + zrecv[s, i].astype(f32)
                plane[k, i] = value.astype(plane.dtype)
            lines[k][kind].start()

    def run():
        take(1, n_shard)
        take(0, n_shard, 0)
        turn(1)
        take(1, 0)
        take(0, 0, 0)
        turn(0, 0)
        product(1, 0)
        hop[0, 2, 0].start()
        product(0, 0, 0)
        hop[1, 2, 0].start()
        take(1, 1)
        take(0, n_shard, 1)
        product(1, 1)
        hop[0, 2, 1].start()
        hop[0, 3, 0].start()
        turn(0, 1)
        take(0, 0, 1)
        product(0, 0, 1)
        take(0, 1, 0)
        product(0, 1, 0)
        hop[1, 3, 0].start()
        gather(0, 0)
        release(0, 0)
        take(0, 1, 1)
        product(0, 1, 1)
        take(1, 2)
        product(1, 2)
        hop[0, 3, 1].start()
        gather(1, 0)
        release(1, 0)
        take(0, 2, 0)
        product(0, 2, 0)
        gather(0, 1)
        release(0, 1)
        forward(0, 0)
        gather(1, 1)
        release(1, 1)
        forward(1, 0)
        take(1, 3)
        product(1, 3)
        take(0, 2, 1)
        product(0, 2, 1)
        take(0, 3, 0)
        product(0, 3, 0)
        gather(0, 2)
        release(0, 2)
        forward(0, 1)
        forward(0, 2)
        gather(1, 2)
        release(1, 2)
        forward(1, 1)
        forward(1, 2)
        take(0, 3, 1)
        product(0, 3, 1)
        gather(1, 3)
        gather(0, 3)
        for kind in range(2):
            arrived(2, kind)
        home = lax.div(me, 2)
        half = pl.ds(pl.multiple_of(core * rows, rows), rows)

        def add_last(others, j):
            value = plane[n_shard - 1, j].astype(f32)
            for s in others:
                value = value + zrecv[s, j].astype(f32)
            value = (value * inverse).astype(gall.dtype)
            gall[home, j, half] = value
            value = value.astype(f32)
            line = jnp.sum(value * value, axis=0, keepdims=True)
            lanes = sqall.shape[-1]
            fold = line[:, :lanes]
            for i in range(1, cols // lanes):
                fold = fold + line[:, i * lanes : (i + 1) * lanes]
            sqall[me * n_shard + z, j] = fold

        @pl.when(inner)
        def _():
            for kind in range(2):
                arrived(4, kind)
            for j in range(members):
                add_last((2, 4), j)

        @pl.when(jnp.logical_not(inner))
        def _():
            for j in range(members):
                add_last((2,), j)

    def leave():
        for kind in range(2):
            for pool in (swap_s, hop_s, pass_s):
                drain(act[kind].at[:, :, pl.ds(0, tokens)], pool.at[2 * kind])
                drain(cot[kind].at[:, pl.ds(0, tokens)], pool.at[2 * kind + 1])
            drain(recv[kind], sum_s.at[kind])
            drain(plane.at[pl.ds(0, n_shard - 1), spans[kind]], line_s.at[kind])

    return enter, begin, run, leave


HOMES = ((2, 0), (1, 0), (1, 1))


def block_at(ref, axis, rows):
    def at(r, half):
        count = rows if half is None else rows // 2
        start = lax.rem(r, 2) * rows + (0 if half is None else half * count)
        cut = pl.ds(pl.multiple_of(start, count), count)
        block = lax.div(r, 2)
        return ref.at[block, cut] if axis == 1 else ref.at[block, :, cut]

    return at


def split(value):
    high = value.astype(jnp.bfloat16)
    return high, (value - high.astype(jnp.float32)).astype(jnp.bfloat16)


def times(left, right):
    dot = functools.partial(jnp.dot, preferred_element_type=jnp.float32)
    return dot(left[0], right[0]) + (dot(left[0], right[1]) + dot(left[1], right[0]))


def gram_iteration(gram, scale, gram_scr, root_scr):
    n = gram.shape[0]
    row = lax.broadcasted_iota(jnp.int32, (n, n), 0)
    col = lax.broadcasted_iota(jnp.int32, (n, n), 1)
    eye = (row == col).astype(jnp.float32)
    trace = jnp.sum(jnp.sum(gram * eye, axis=0, keepdims=True), axis=1, keepdims=True)
    inverse = 1.0 / (jnp.sqrt(trace) + epsilon)
    gram_scr[...] = gram * inverse * inverse
    for iteration in range(ITERS):
        a = split(gram_scr[...])
        mixing = coef_b * gram_scr[...] + coef_c * times(a, a)
        b = split(mixing)
        if iteration == 0:
            root_scr[...] = coef_a * eye + mixing
        else:
            root_scr[...] = coef_a * root_scr[...] + times(b, split(root_scr[...]))
        if iteration < ITERS - 1:
            half = coef_a * gram_scr[...] + times(b, a)
            gram_scr[...] = coef_a * half + times(b, split(half))
    return root_scr[...] * (inverse * scale)


def muon_kernel(
    n_shard, inverse, scale, owner_ref, start_ref, act_ref, cot_ref, momentum_hbm,
    mout_ref, u_ref, wall_ref, qall_ref,
    momentum, gall, sqall, table, factor, uown, held, gram_out, gram_in, gram_scr, root_scr, root,
    act, cot, turned, part, recv, plane, zrecv, reduce_sems,
    load, ps, pr, gs, gr, as_, ar, ws, wr, os_, or_, rs, rr, hs, hr,
):
    f32, bf16 = jnp.float32, jnp.bfloat16
    me, core, x, y, to_core, to_x, to_y, to_xy = place()
    z = lax.axis_index("shard")
    base = me - core
    block = lax.div(me, 2)
    members = gall.shape[1]
    rows, cols = held.shape[1:]
    lanes = sqall.shape[-1]
    mine = pl.ds(pl.multiple_of(core * rows, rows), rows)

    fetch = pltpu.make_async_copy(momentum_hbm, momentum, load)
    enter, begin, run, leave = gather_reduce(
        n_shard, inverse, act_ref, cot_ref, gall, sqall, act, cot, turned, part, recv,
        plane, zrecv, *reduce_sems,
    )
    everyone = n_shard * 2 * gall.shape[0]
    here = me * n_shard + z
    others = [lax.rem(here + t, everyone) for t in range(1, everyone)]
    others = [(lax.div(to, n_shard), lax.rem(to, n_shard)) for to in others]
    greet(others, enter)

    begin()
    fetch.start()
    run()

    for peer in others:
        remote(sqall.at[here], sqall.at[here], ps, pr, peer).start()
    at_g = block_at(gall, 2, rows)
    gathers = plane_gather_start(z, at_g, gs, gr)
    fetch.wait()
    drain(sqall.at[pl.ds(0, everyone - 1)], pr)

    table[...] = jnp.zeros_like(table)
    for m in range(MATS):
        layer, side = divmod(m, 2)
        bx, by = divmod(layer, 2) if m < 8 else (side, layer - 4)
        j, i = 2 * by + bx, side if m < 8 else 2
        line = sqall[2 * j * n_shard, i]
        for d in range(1, 2 * n_shard):
            line = line + sqall[2 * j * n_shard + d, i]
        table[pl.ds(m, 1)] = line
    index = lax.broadcasted_iota(jnp.int32, table.shape, 0)
    bucket = jnp.zeros(table.shape, jnp.int32)
    for k in range(start_ref.shape[0]):
        bucket = bucket + (index >= start_ref[k]).astype(jnp.int32)
    sums = table[...]
    clip = jnp.zeros(table.shape, f32)
    for k in range(start_ref.shape[0] + 1):
        inside = (bucket == k) & (index < MATS)
        total = jnp.sum(jnp.where(inside, sums, 0.0), axis=(0, 1), keepdims=True)
        count = jnp.sum(inside.astype(f32), axis=(0, 1), keepdims=True) / lanes
        mean = total / (jnp.maximum(count, 1.0) * (2 * rows) * (n_shard * cols))
        clip = jnp.where(inside, jnp.minimum(1.0, clip_level / jnp.sqrt(mean + epsilon)), clip)
    for m in range(MATS):
        factor[m] = jnp.concatenate([clip[m : m + 1, :]] * (cols // lanes), axis=1)

    def advance(matrix, gradient, past):
        step = factor[matrix] * gradient.astype(f32)
        new = momentum_rate * past + step
        return new, (step + momentum_rate * new).astype(bf16)

    gathers[4].wait_recv()
    for i in range(members):
        layer, side = lodged(block, i)
        matrix = 2 * layer + side
        uown[i] = advance(matrix, gall[block, i], momentum[matrix])[1]
    over = (((1,), (1,)), ((), ()))
    parts = []
    for i, (hz, hc) in enumerate(HOMES):
        here = (z == hz) & (core == hc)
        owner = (base + hc, hz)
        low = uown[i, :rows]
        high = uown[i, rows:]
        own = jnp.where(core == 0, low, high)
        diag = lax.dot_general(own, own, over, preferred_element_type=f32)
        gram_out[i, 0] = diag
        part = remote(gram_out.at[i, 0], gram_in.at[z, core], as_.at[i, 0], ar.at[z, core], owner)
        cross = remote(gram_out.at[i, 1], gram_in.at[z, 2], as_.at[i, 1], ar.at[z, 2], owner)
        parts.append((here, part, cross))

        @pl.when(here)
        def _():
            gram_in[z, core] = diag

        @pl.when(jnp.logical_not(here))
        def _():
            part.start()

        @pl.when(core == 0)
        def _():
            off = lax.dot_general(low, high, over, preferred_element_type=f32)
            gram_out[i, 1] = off

            @pl.when(here)
            def _():
                gram_in[z, 2] = off

            @pl.when(jnp.logical_not(here))
            def _():
                cross.start()

    plane_gather_turn(z, at_g, gs, gr, gathers)
    plane_gather_finish(z, at_g, gs, gr, gathers, last=(7, 8, 9))

    def slot_matrix(shard, slot):
        found = jnp.int32(0)
        count = jnp.int32(0)
        for m in range(MATS):
            yes = owner_ref[m] == shard
            found = jnp.where(yes & (count == slot), m, found)
            count = count + yes.astype(jnp.int32)
        return found

    sends = {}

    def make_slice(d):
        shard = lax.rem(z + d, n_shard)
        matrix = slot_matrix(shard, block)
        home, member = lodging(matrix)
        held[d - 1] = advance(matrix, gall[home, member, mine], momentum[matrix, mine])[1]
        sends[d] = remote(
            held.at[d - 1], wall_ref.at[n_shard - d - 1, block, mine], ws, wr.at[d - 1], (me, shard)
        )

    for d in (1, 3):
        make_slice(d)
        sends[d].start()
    make_slice(2)
    early = z == 2

    @pl.when(early)
    def _():
        sends[2].start()

    def all_one(m, carry):
        home, member = lodging(m)
        new, turned = advance(m, gall[home, member], momentum[m])
        mout_ref[m] = new
        u_ref[m] = turned
        return carry

    is_home = functools.reduce(jnp.logical_or, [here for here, _, _ in parts])
    member = jnp.where(z == HOMES[0][0], 0, 1 + core)
    roots = []
    packed = root.shape[0] // 2
    mine_q = pl.ds(pl.multiple_of(core * packed, packed), packed)
    for d in range(n_shard):
        for c in range(2):
            if d == 0 and c == 1:
                continue
            peer = (to_core, z) if d == 0 else (base + c, lax.rem(z + d, n_shard))
            half = 1 - core if d == 0 else c
            cut = pl.ds(pl.multiple_of(half * packed, packed), packed)
            roots.append(remote(root.at[cut], qall_ref.at[block, member, cut], rs, rr.at[member], peer))

    @pl.when(jnp.logical_not(is_home))
    def _():
        lax.fori_loop(0, MATS, all_one, 0)

    @pl.when(is_home)
    def _():
        for d in range(n_shard):
            for k in range(3):
                source = remote(gram_out.at[0, 0], gram_in.at[d, k], as_.at[0, 0], ar.at[d, k], (to_core, z))
                local = (z == d) & ((core == k) if k < 2 else (core == 0))

                @pl.when(jnp.logical_not(local))
                def _():
                    source.wait_recv()

        blocks = []
        for k in range(3):
            value = gram_in[0, k]
            for d in range(1, n_shard):
                value = value + gram_in[d, k]
            blocks.append(value)
        top = jnp.concatenate([blocks[0], blocks[2]], axis=1)
        bottom = jnp.concatenate([blocks[2].T, blocks[1]], axis=1)
        result = gram_iteration(jnp.concatenate([top, bottom], axis=0), scale, gram_scr, root_scr)
        result = result.astype(bf16)
        root[:rows] = result[:rows, :rows]
        root[rows:packed] = result[: rows // 2, rows:]
        root[packed : packed + rows] = result[rows:, rows:]
        root[packed + rows :] = result[rows // 2 : rows, rows:]
        for c in roots:
            c.start()
        qall_ref[block, member, mine_q] = root[mine_q]

    walls = {}

    def at_w(d):
        return block_at(wall_ref.at[n_shard - d - 1], 1, rows)

    for d in (1, 3):
        sends[d].wait_recv()
        walls[d] = plane_gather_start(z, at_w(d), os_.at[d - 1], or_.at[d - 1])

    @pl.when(jnp.logical_not(early))
    def _():
        sends[2].start()

    @pl.when(is_home)
    def _():
        lax.fori_loop(0, MATS, all_one, 0)

    for d in (1, 3):
        plane_gather_turn(z, at_w(d), os_.at[d - 1], or_.at[d - 1], walls[d])
    for i, (here, _, _) in enumerate(parts):
        arrival = remote(root.at[mine_q], qall_ref.at[block, i, mine_q], rs, rr.at[i], (to_core, z))

        @pl.when(jnp.logical_not(here))
        def _():
            arrival.wait_recv()

    at_q = block_at(qall_ref, 2, packed)
    gathers_q = plane_gather_start(z, at_q, hs, hr)
    sends[2].wait_recv()
    walls[2] = plane_gather_start(z, at_w(2), os_.at[1], or_.at[1])
    for d in (1, 3):
        plane_gather_finish(z, at_w(d), os_.at[d - 1], or_.at[d - 1], walls[d])
    plane_gather_turn(z, at_q, hs, hr, gathers_q)
    plane_gather_turn(z, at_w(2), os_.at[1], or_.at[1], walls[2])
    plane_gather_finish(z, at_q, hs, hr, gathers_q)
    plane_gather_finish(z, at_w(2), os_.at[1], or_.at[1], walls[2])
    most = pl.ds(0, 2 * rows - rows // 4)
    drain(gall.at[:, :, most], gs)
    drain(qall_ref.at[:, :, pl.ds(0, 2 * packed - packed // 4)], hs)
    for d in range(n_shard - 1):
        drain(wall_ref.at[d, :, most], os_.at[d])
    drain(held, ws)
    drain(sqall.at[pl.ds(0, everyone - 1)], ps)

    @pl.when(is_home)
    def _():
        drain(u_ref.at[pl.ds(0, len(roots)), pl.ds(0, packed * rows // cols)], rs)

    for here, part, cross in parts:

        @pl.when(jnp.logical_not(here))
        def _():
            part.wait_send()

            @pl.when(core == 0)
            def _():
                cross.wait_send()

    leave()


def finish_kernel(
    owner_ref, mout_ref, u_ref, wall_ref, qall_ref, mom_out, update_out, owned_out,
    ubuf, wbuf, qbuf, msem, usem, wsem,
):
    f32 = jnp.float32
    slots, _, width = wbuf.shape
    mats, _, cols = ubuf.shape
    n_shard = width // cols
    rows = qall_ref.shape[-1]
    z = lax.axis_index("shard")

    def put(buf, out, sem, m):
        return pltpu.make_async_copy(buf.at[m], out.at[m], sem)

    for m in range(mats):
        put(mout_ref, mom_out, msem, m).start()

    def update_one(m, carry):
        home, member = lodging(m)
        q = qall_ref[home, member]
        cross = jnp.concatenate([q[rows : 3 * rows // 2], q[5 * rows // 2 :]], axis=0)
        qbuf[m, :rows, :rows] = q[:rows]
        qbuf[m, :rows, rows:] = cross
        qbuf[m, rows:, :rows] = cross.T
        qbuf[m, rows:, rows:] = q[3 * rows // 2 : 5 * rows // 2]
        ubuf[m] = jnp.dot(qbuf[m], u_ref[m], preferred_element_type=f32)
        put(ubuf, update_out, usem, m).start()
        return carry

    lax.fori_loop(0, mats, update_one, 0, unroll=3)

    def owned_one(s, carry):
        matrix = jnp.int32(0)
        count = jnp.int32(0)
        for m in range(mats):
            yes = owner_ref[m] == z
            matrix = jnp.where(yes & (count == s), m, matrix)
            count = count + yes.astype(jnp.int32)
        keep = (count > s).astype(f32)
        q = qbuf[matrix]
        for d in range(n_shard):
            right = u_ref[matrix] if d == 0 else wall_ref[d - 1, s]
            value = jnp.dot(q, right, preferred_element_type=f32) * keep
            at = lax.rem(z + d, n_shard)
            wbuf[s, :, pl.ds(pl.multiple_of(at * cols, cols), cols)] = value.astype(wbuf.dtype)
        put(wbuf, owned_out, wsem, s).start()
        return carry

    lax.fori_loop(0, slots, owned_one, 0, unroll=2)

    drain(mout_ref, msem)
    drain(ubuf, usem)
    drain(wbuf, wsem)


def per_device_planes(activations, cotangents, momentum, owners, bucket_starts):
    n_shard = lax.axis_size("shard")
    n_rep = lax.axis_size("rep")
    layers, tok_rows, width = activations.shape
    token_total = tok_rows * n_shard * n_rep
    cols = width // n_shard
    rows = KV // 2
    lanes = math.gcd(cols, 128)
    groups = n_rep // 2
    members = MATS // groups
    slots = -(-MATS // n_shard) + 1
    update_scale = math.sqrt(max(KV, D))
    bf16, f32 = jnp.bfloat16, jnp.float32

    def params(limit, **rest):
        return pltpu.CompilerParams(vmem_limit_bytes=limit * 1024 * 1024, **rest)

    dma = pltpu.SemaphoreType.DMA
    tokens = 4 * tok_rows
    shares = (layers // 3, layers // 6)
    hbm = functools.partial(pltpu.with_memory_space_constraint, memory_space=pltpu.HBM)
    mout, turned, wall, qall = pl.pallas_call(
        functools.partial(muon_kernel, n_shard, 1.0 / math.sqrt(token_total), update_scale),
        out_shape=(
            pltpu.VMEM((MATS, KV, cols), f32),
            pltpu.VMEM((MATS, KV, cols), bf16),
            pltpu.VMEM((n_shard - 1, slots, KV, cols), bf16),
            pltpu.VMEM((groups, members, 3 * rows, rows), bf16),
        ),
        in_specs=[SMEM_SPEC, SMEM_SPEC, ANY_SPEC, ANY_SPEC, ANY_SPEC],
        out_specs=(VMEM_SPEC,) * 4,
        scratch_shapes=[
            pltpu.VMEM((MATS, KV, cols), f32),
            pltpu.VMEM((groups, members, KV, cols), bf16),
            pltpu.VMEM((n_rep * n_shard, members, 1, lanes), f32),
            pltpu.VMEM((16, lanes), f32),
            pltpu.VMEM((MATS, 1, cols), f32),
            pltpu.VMEM((members, KV, cols), bf16),
            pltpu.VMEM((n_shard - 1, rows, cols), bf16),
            pltpu.VMEM((members, 2, rows, rows), f32),
            pltpu.VMEM((n_shard, 3, rows, rows), f32),
            pltpu.VMEM((KV, KV), f32),
            pltpu.VMEM((KV, KV), f32),
            pltpu.VMEM((3 * rows, rows), bf16),
            [pltpu.VMEM((n_shard, n, tokens, cols), bf16) for n in shares],
            [pltpu.VMEM((n, tokens, 2 * KV), bf16) for n in shares],
            [pltpu.VMEM((n, 2, rows, tokens), bf16) for n in shares],
            [pltpu.VMEM((n_shard, 2, n, rows, cols), bf16) for n in shares],
            [pltpu.VMEM((n_shard, n, rows, cols), bf16) for n in shares],
            pltpu.VMEM((n_shard, members, rows, cols), bf16),
            pltpu.VMEM((n_shard + 1, members, rows, cols), bf16),
            [dma((3 * n_shard + 3,)) for _ in range(2)]
            + [dma((4,)) for _ in range(3)]
            + [dma((2,)), dma((2, n_shard)), dma((2,)), dma((n_shard + 1, 2))],
            dma(()),
            dma(()), dma(()),
            dma(()), dma((10,)),
            dma((members, 2)), dma((n_shard, 3)),
            dma(()), dma((n_shard - 1,)),
            dma((n_shard - 1,)), dma((n_shard - 1, 10)),
            dma(()), dma((members,)),
            dma(()), dma((10,)),
        ],
        compiler_params=params(48, has_side_effects=True, collective_id=0),
        name="muon",
    )(owners, bucket_starts, hbm(activations), hbm(cotangents), hbm(momentum))

    return pl.pallas_call(
        finish_kernel,
        out_shape=(
            jax.ShapeDtypeStruct(momentum.shape, f32),
            jax.ShapeDtypeStruct(momentum.shape, f32),
            jax.ShapeDtypeStruct((slots, KV, width), bf16),
        ),
        in_specs=[SMEM_SPEC] + [VMEM_SPEC] * 4,
        out_specs=(ANY_SPEC,) * 3,
        scratch_shapes=[
            pltpu.VMEM(momentum.shape, f32),
            pltpu.VMEM((slots, KV, width), bf16),
            pltpu.VMEM((MATS, KV, KV), bf16),
            dma(()), dma(()), dma(()),
        ],
        compiler_params=params(20),
        name="finish",
    )(owners, mout, turned, wall, qall)


def solution(mesh):
    groups = mesh.shape["rep"] // 2
    slots = -(-MATS // mesh.shape["shard"]) + 1
    fits = mesh.shape["rep"] == 8 and mesh.shape["shard"] == 4 and slots <= groups
    placed = (
        P(None, ("rep", "shard"), None),
        P(None, ("rep", "shard"), None),
        P(None, None, "shard"),
        P(),
        P(),
    )
    return jax.shard_map(
        per_device_planes if fits else per_device_general,
        mesh=mesh,
        in_specs=placed,
        out_specs=(P(None, None, "shard"), P(None, None, "shard"), P("shard", None, None)),
        check_vma=False,
    )
```
